256 devices in a mesh: grp: 4 (over y), gx: 16 (over z, core), gy: 4 (over x).
Axes of the slice: x: 4, y: 4, z: 8, core: 2. Of those that a mesh axis runs over, the one named last changes fastest.
Arguments:
- pressure: float32 [4, 64, 64, 128], P('grp', 'gx', 'gy'), may hold values from -6 to 6
- source: float32 [4, 64, 64, 128], P('grp', 'gx', 'gy'), may hold values from -6 to 6
- storage: float32 [4, 64, 64, 128], P('grp', 'gx', 'gy'), may hold values from 0.05 to 2
- well_mask: int32 [4, 64, 64, 128], P('grp', 'gx', 'gy'), may hold values 0 or 1
- block_id: int32 [4, 64, 64, 128], P('grp', 'gx', 'gy'), may hold values from 0 to 63
- basis_weight: float32 [4, 8, 64, 64, 128], P('grp', None, 'gx', 'gy'), may hold values from 0 to 1
- host_elem: int32 [4, 64, 64, 128], P('grp', 'gx', 'gy'), may hold values from 0 to 8191
- displacement: float32 [4, 3, 64, 64, 128], P('grp', None, 'gx', 'gy'), may hold values from -4 to 4
- body_force: float32 [4, 3, 64, 64, 128], P('grp', None, 'gx', 'gy'), may hold values from -6 to 6
- modulus: float32 [4, 64, 64, 128], P('grp', 'gx', 'gy'), may hold values from 0.5 to 4
- elem_mask: int32 [4, 64, 64, 128], P('grp', 'gx', 'gy'), may hold values 0 or 1
- stiffness: float32 [24, 24], replicated, as said below
Outputs:
- pressure_out: float32 [4, 64, 64, 128], P('grp', 'gx', 'gy')
- displacement_out: float32 [4, 3, 64, 64, 128], P('grp', None, 'gx', 'gy')
The draws below stay inside these ranges and needn't reach their ends.
Inputs may be any that keep to these rules, and one draw needn't show every extreme that they name: stiffness is symmetric and each diagonal entry exceeds the sum of the magnitudes of the other entries in its row by one.
All inputs are finite; a program needn't handle non-finite values. No bound on the sum of `well_mask` or of `elem_mask` on one device may be relied on, other than what follows from the above.
Results may differ from the reference program's by a relative error of at most 0.0003.
Values sent between devices are 32-bit elements; how exact they have to be, the bound alone decides.
A program may use at most 64 MiB of HBM per device.

```python
import math
import jax
import jax.numpy as jnp
from jax import lax

FX = 4
FY = 16
FZ = 128
NBLK = 64
SWEEPS = 2
ITERS = 2
NXF = 64
NYF = 64
N_GRP = 4
N_GX = 16
N_GY = 4


def draw_stiffness(key, part):
    random_part = jax.random.normal(jax.random.fold_in(key, 11), (24, 24), jnp.float32) * 0.3
    paired = (random_part + random_part.T) * 0.7071
    identity = jnp.eye(24, dtype=jnp.float32)
    offdiag = paired * (1.0 - identity)
    dominant = jnp.sum(jnp.abs(offdiag), axis=1) + 1.0
    return offdiag + identity * dominant[:, None]


def with_ends(drawn, stream_key, low, largest):
    longest = drawn.shape.index(max(drawn.shape))
    spots = []
    for shift in (0, 1):
        where = [jax.random.randint(jax.random.fold_in(stream_key, axis), (), 0, length) for axis, length in enumerate(drawn.shape)]
        where[longest] = (where[longest] + shift) % drawn.shape[longest]
        spots.append(tuple(where))
    return drawn.at[spots[0]].set(low).at[spots[1]].set(largest)


def steps_of(stream_key, shape, shards, low, high):
    def one(dim, blocks):
        heights = jax.random.uniform(jax.random.fold_in(jax.random.fold_in(stream_key, 6), dim), (blocks,), jnp.float32, low / len(shards), high / len(shards))
        return jnp.repeat(jnp.exp(heights), shape[dim] // blocks).reshape((-1,) + (1,) * (len(shape) - dim - 1))

    loudness = one(*shards[0])
    for cut in shards[1:]:
        loudness = loudness * one(*cut)
    return loudness


def centred(own_key, dims, deviation, limit, split=(), kind=jnp.bfloat16):
    drawn = jax.random.normal(own_key, dims, jnp.float32) * deviation
    if len(split) > 0:
        drawn = steps_of(own_key, dims, split, -0.22, 0.18) * drawn
    return jnp.clip(drawn, min=-limit, max=limit).astype(kind)


def setup_inputs(seed: int = 0) -> dict:
    seeds = jax.random.split(jax.random.key(seed), 13)
    pressure = centred(seeds[0], (N_GRP, NXF, NYF, FZ), 1.0, 6.0, ((0, 4), (1, 16), (2, 4)), jnp.float32)
    source = centred(seeds[1], (N_GRP, NXF, NYF, FZ), 1.0, 6.0, ((0, 4), (1, 16), (2, 4)), jnp.float32)
    storage = jnp.clip(jnp.exp(math.log(2.0) - 3.6888794 * jax.random.uniform(seeds[2], (N_GRP, NXF, NYF, FZ), jnp.float32) ** steps_of(seeds[2], (N_GRP, NXF, NYF, FZ), ((0, 4), (1, 16), (2, 4)), -0.2, 0.2)), 0.05, 2.0)
    well_mask = with_ends((jax.random.randint(seeds[3], (N_GRP, NXF, NYF, FZ), 0, 16) < 1).astype(jnp.int32), jax.random.fold_in(seeds[3], 1), 0, 1)
    block_id = with_ends(jax.random.randint(seeds[4], (N_GRP, NXF, NYF, FZ), 0, NBLK), jax.random.fold_in(seeds[4], 1), 0, NBLK - 1).astype(jnp.int32)
    basis_weight = jnp.clip(1.0 * jax.random.uniform(seeds[5], (N_GRP, 8, NXF, NYF, FZ), jnp.float32) ** steps_of(seeds[5], (N_GRP, 8, NXF, NYF, FZ), ((0, 4), (2, 16), (3, 4)), -0.2, 0.2), 0.0, 1.0)
    host_elem = with_ends(jax.random.randint(seeds[6], (N_GRP, NXF, NYF, FZ), 0, FX * FY * FZ), jax.random.fold_in(seeds[6], 1), 0, (FX * FY * FZ) - 1).astype(jnp.int32)
    displacement = centred(seeds[7], (N_GRP, 3, NXF, NYF, FZ), 0.3, 4.0, ((0, 4), (2, 16), (3, 4)), jnp.float32)
    body_force = centred(seeds[8], (N_GRP, 3, NXF, NYF, FZ), 1.0, 6.0, ((0, 4), (2, 16), (3, 4)), jnp.float32)
    modulus = jnp.clip(jnp.exp(math.log(4.0) - 2.0794415 * jax.random.uniform(seeds[9], (N_GRP, NXF, NYF, FZ), jnp.float32) ** steps_of(seeds[9], (N_GRP, NXF, NYF, FZ), ((0, 4), (1, 16), (2, 4)), -0.2, 0.2)), 0.5, 4.0)
    elem_mask = with_ends((jax.random.randint(seeds[10], (N_GRP, NXF, NYF, FZ), 0, 8) < 7).astype(jnp.int32), jax.random.fold_in(seeds[10], 1), 0, 1)
    stiffness = draw_stiffness(jax.random.fold_in(seeds[12], 71), 0)
    return dict(pressure=pressure, source=source, storage=storage, well_mask=well_mask, block_id=block_id, basis_weight=basis_weight, host_elem=host_elem, displacement=displacement, body_force=body_force, modulus=modulus, elem_mask=elem_mask, stiffness=stiffness)


biot_coef = 1.5
relaxation = 0.8
spring_coef = 0.5
well_index = 4.0
highest = lax.Precision.HIGHEST


def coupling_vector():
    index = jnp.arange(24, dtype=jnp.int32)
    corner = index // 3
    component = index % 3
    bitval = (corner >> (2 - component)) & 1
    return (bitval.astype(jnp.float32) * 2.0 - 1.0) * 0.25


def corner_list():
    return [((corner >> 2) & 1, (corner >> 1) & 1, corner & 1) for corner in range(8)]


def reference(pressure, source, storage, well_mask, block_id, basis_weight, host_elem, displacement, body_force, modulus, elem_mask, stiffness):
    layers = N_GRP - 1
    elements = FX * FY * FZ

    def to_grid(field):
        return jnp.moveaxis(field, 0, 2).reshape(NXF, NYF, layers * FZ)

    def from_grid(field):
        return jnp.moveaxis(field.reshape(NXF, NYF, layers, FZ), 2, 0)

    def to_tiles(field):
        return field.reshape(layers, N_GX, FX, N_GY, FY, FZ).transpose(0, 1, 3, 2, 4, 5).reshape(-1)

    def from_tiles(flat):
        return flat.reshape(layers, N_GX, N_GY, FX, FY, FZ).transpose(0, 1, 3, 2, 4, 5).reshape(layers, NXF, NYF, FZ)

    def to_blocks(field):
        return field.reshape(N_GX, FX, N_GY, FY, FZ).transpose(0, 2, 1, 3, 4).reshape(-1)

    def from_blocks(flat):
        return flat.reshape(N_GX, N_GY, FX, FY, FZ).transpose(0, 2, 1, 3, 4).reshape(NXF, NYF, FZ)

    columns = (jnp.arange(N_GX, dtype=jnp.int32)[:, None] * N_GY + jnp.arange(N_GY, dtype=jnp.int32)[None, :]).astype(jnp.int32)
    host_tiles = to_tiles(host_elem[:layers]).reshape(layers, N_GX, N_GY, elements)
    host_seg = (columns[None, :, :, None] * elements + host_tiles).astype(jnp.int32).reshape(-1)
    tile_ids = jnp.arange(layers * N_GX * N_GY, dtype=jnp.int32).reshape(layers, N_GX, N_GY, 1)
    block_tiles = to_tiles(block_id[:layers]).reshape(layers, N_GX, N_GY, elements)
    block_seg = (tile_ids * NBLK + block_tiles).astype(jnp.int32).reshape(-1)
    coarse_count = layers * N_GX * N_GY * NBLK

    coupling = coupling_vector()
    mech_mask = elem_mask[layers].astype(jnp.float32).reshape(-1)
    weights = modulus[layers].reshape(-1) * mech_mask

    def spread(nodes):
        padded = jnp.pad(nodes, ((0, 0), (0, 1), (0, 1), (0, 1)))
        pieces = [padded[:, shift_x:shift_x + NXF, shift_y:shift_y + NYF, shift_z:shift_z + FZ] for shift_x, shift_y, shift_z in corner_list()]
        return jnp.stack(pieces).reshape(24, -1)

    def assemble(values):
        parts = values.reshape(8, 3, NXF, NYF, FZ)
        total = jnp.zeros((3, NXF + 1, NYF + 1, FZ + 1), jnp.float32)
        for corner, (shift_x, shift_y, shift_z) in enumerate(corner_list()):
            total = total + jnp.pad(parts[corner], ((0, 0), (shift_x, 1 - shift_x), (shift_y, 1 - shift_y), (shift_z, 1 - shift_z)))
        return total[:, :NXF, :NYF, :FZ]

    def apply(vector):
        return assemble(jnp.dot(stiffness, spread(vector), precision=highest) * weights[None, :]) + spring_coef * vector

    initial = displacement[layers]
    strain = mech_mask * jnp.dot(coupling, spread(initial), precision=highest)
    strain_cells = to_grid(from_tiles(to_blocks(strain.reshape(NXF, NYF, FZ))[host_seg]))

    start = to_grid(pressure[:layers])
    diagonal = 6.0 + to_grid(storage[:layers]) + well_index * to_grid(well_mask[:layers].astype(jnp.float32))
    forcing = to_grid(source[:layers]) - biot_coef * strain_cells

    def neighbours(field):
        padded = jnp.pad(field, 1)
        total = padded[2:, 1:-1, 1:-1] + padded[:-2, 1:-1, 1:-1]
        total = total + padded[1:-1, 2:, 1:-1] + padded[1:-1, :-2, 1:-1]
        return total + padded[1:-1, 1:-1, 2:] + padded[1:-1, 1:-1, :-2]

    def residual(field):
        return forcing - (diagonal * field - neighbours(field))

    current = start
    for sweep_index in range(SWEEPS):
        current = current + relaxation * residual(current) / diagonal
    remainder = to_tiles(from_grid(residual(current)))
    weight_flat = jnp.stack([to_tiles(basis_weight[:layers, index]) for index in range(8)])
    diag_flat = to_tiles(from_grid(diagonal))
    coarse = jax.ops.segment_sum((weight_flat * remainder).T, block_seg, num_segments=coarse_count)
    scale = 1.0 + jax.ops.segment_sum((weight_flat * weight_flat * diag_flat).T, block_seg, num_segments=coarse_count)
    correction = coarse / scale
    delta = jnp.sum(weight_flat.T * correction[block_seg], axis=1)
    updated = current + to_grid(from_tiles(delta))

    change = to_tiles(from_grid(updated - start))
    sums = jax.ops.segment_sum(change, host_seg, num_segments=N_GX * N_GY * elements)
    counts = jax.ops.segment_sum(jnp.ones_like(change), host_seg, num_segments=N_GX * N_GY * elements)
    element_pressure = from_blocks(sums / jnp.maximum(counts, 1.0)).reshape(-1)
    force = body_force[layers] + biot_coef * assemble(coupling[:, None] * (mech_mask * element_pressure)[None, :])

    solution = initial
    remain = force - apply(solution)
    search = remain
    norm_now = jnp.sum(remain * remain)
    for iteration in range(ITERS):
        image = apply(search)
        step_size = norm_now / jnp.sum(search * image)
        solution = solution + step_size * search
        remain = remain - step_size * image
        norm_next = jnp.sum(remain * remain)
        search = remain + (norm_next / norm_now) * search
        norm_now = norm_next
    pressure_out = jnp.concatenate([from_grid(updated), jnp.zeros((1, NXF, NYF, FZ), jnp.float32)], 0)
    displacement_out = jnp.concatenate([jnp.zeros((layers, 3, NXF, NYF, FZ), jnp.float32), solution[None]], 0)
    return pressure_out, displacement_out
```

```python
import functools

import jax
import jax.numpy as jnp
from jax import lax
from jax.experimental import pallas as pl
from jax.experimental.pallas import tpu as pltpu
from jax.sharding import PartitionSpec as P

F32 = jnp.float32
BF16 = jnp.bfloat16
I32 = jnp.int32
MESH = pl.DeviceIdType.MESH
NBLK = 64
LANES = 128
ROWS = 64
BIOT = 1.5
RELAX = 0.8
SPRING = 0.5
WELL = 4.0
AROUND = [(dx, dy) for dx in (-1, 0, 1) for dy in (-1, 0, 1) if (dx, dy) != (0, 0)]

SEND = dict(ux=3, strain=3, ue=8, ce=8, mw=8, gr=8, sums=1, counts=1, halo=18, ary=4, arx=16)
RECV = dict(ux=3, strain=1, ue=8, ce=8, mw=8, gr=8, sums=3, counts=3, halo=18, ary=4, arx=16)


def offsets(table):
    at, out = 0, {}
    for name, count in table.items():
        out[name] = at
        at += count
    return out, at


SEND_AT, N_SEND = offsets(SEND)
RECV_AT, N_RECV = offsets(RECV)

SCRATCH = dict(
    pres=((64, 128), F32), srcs=((64, 128), F32), stor=((64, 128), F32), well=((64, 128), I32),
    blk=((64, 128), I32), bas=((512, 128), F32), host=((64, 128), I32),
    disp=((3, 64, 128), F32), body=((192, 128), F32), modl=((64, 128), F32), mask=((64, 128), I32),
    stif=((24, 24), F32),
    p1=((64, 128), F32), p2=((64, 128), F32), diag=((64, 128), F32), frc=((64, 128), F32),
    xh=((6, 16, 128), F32), yh=((6, 8, 128), F32), zh=((6, 8, 128), F32),
    ys=((6, 8, 128), F32), zs=((6, 8, 128), F32),
    sti=((64, 128), F32), ol=((128, 8192), BF16), oh=((64, 8192), BF16), ob=((64, 8192), BF16),
    wt=((64, 8, 128), F32), wr=((16, 8192), BF16), ar=((128, 8192), BF16), scale=((8, 64), F32),
    rowi=((64, 128), F32), chg=((64, 128), F32), lo=((64, 128), F32), t2=((128, 128), BF16),
    cnt=((64, 128), F32), sm=((64, 128), F32), corr=((16, 64), BF16), rem=((64, 128), F32),
    ux=((3, 16, 128), F32), uy=((16, 128), F32), uc=((8, 128), F32),
    uys=((16, 128), F32), ucs=((8, 128), F32), stro=((64, 128), F32),
    ue=((8, 96, 128), F32), uyl=((8, 16, 128), F32), uyh=((8, 16, 128), F32),
    ce=((8, 96, 128), F32), cyl=((8, 16, 128), F32), cyh=((8, 16, 128), F32),
    mw=((9, 32, 128), F32), gr=((9, 32, 128), F32), wtile=((7, 88, 128), F32),
    sr=((3, 64, 128), F32), cr=((3, 64, 128), F32), fac=((64, 128), F32),
    gt=((9, 104, 128), F32), rx=((8, 96, 128), F32), qe=((8, 96, 128), F32),
    ph=((8, 192, 128), BF16), plo=((8, 192, 128), BF16), vs=((7, 704, 128), F32),
    kl=((64, 192), BF16), kap=((8, 128), F32), bt=((4, 64, 128), F32),
    rr=((192, 128), F32), qr=((192, 128), F32), dots=((8, 128), F32),
    ar1=((4, 8, 128), F32), ar2=((16, 1, 128), F32), row=((1, 128), F32),
)


def split(value):
    high = value.astype(BF16)
    return high, (value - high.astype(F32)).astype(BF16)


def dot_nt(a, b):
    return lax.dot_general(a, b, (((1,), (1,)), ((), ())), preferred_element_type=F32)


def dot_nn(a, b):
    return jnp.dot(a, b, preferred_element_type=F32)


def lane_iota(shape=(8, 128)):
    return lax.broadcasted_iota(I32, shape, len(shape) - 1)


def sub_iota(shape=(8, 128)):
    return lax.broadcasted_iota(I32, shape, len(shape) - 2)


def shift_down(value):
    return jnp.where(lane_iota(value.shape) == LANES - 1, 0.0, pltpu.roll(value, LANES - 1, 1))


def shift_up(value):
    return jnp.where(lane_iota(value.shape) == 0, 0.0, pltpu.roll(value, 1, 1))


def loop(count, body, unroll=1):
    def step(i, carry):
        body(i)
        return carry

    lax.fori_loop(0, count, step, 0, unroll=unroll)


def kernel(sizes, *refs):
    groups, nx, ny = sizes
    ins, (po, do), rest = refs[:12], refs[12:14], refs[14:]
    s = dict(zip(SCRATCH, rest))
    in_sems, send_sems, recv_sems, known = rest[len(SCRATCH):]
    g, gx, gy = lax.axis_index("grp"), lax.axis_index("gx"), lax.axis_index("gy")
    top = groups - 1
    mech = g == top
    names = ["pres", "srcs", "stor", "well", "blk", "bas", "host", "disp", "body", "modl", "mask", "stif"]

    def local(name):
        k = names.index(name)
        return pltpu.make_async_copy(ins[k], s[name], in_sems.at[k])

    def inside(dx, dy, dg=0):
        x, y = gx + dx, gy + dy
        ok = (x >= 0) & (x < nx) & (y >= 0) & (y < ny)
        if dg:
            ok = ok & (g + dg >= 0) & (g + dg < top)
        return ok

    def as_int(flag):
        return flag.astype(I32)

    def remote(src, dst, send, recv, device):
        return pltpu.make_async_remote_copy(
            src_ref=src, dst_ref=dst, send_sem=send_sems.at[send], recv_sem=recv_sems.at[recv],
            device_id=device, device_id_type=MESH,
        )

    def start_if(ok, *args):
        @pl.when(ok)
        def _():
            remote(*args).start()

    def wait_recv_if(ok, dst, recv):
        @pl.when(ok)
        def _():
            remote(dst, dst, 0, recv, (g, gx, gy)).wait_recv()

    def wait_send_if(ok, src, send):
        @pl.when(ok)
        def _():
            remote(src, src, send, 0, (g, gx, gy)).wait_send()

    def greet(ok, device):
        @pl.when(ok)
        def _():
            pl.semaphore_signal(pltpu.get_barrier_semaphore(), inc=1, device_id=device, device_id_type=MESH)

    HALO = [(-1, 0, 0), (1, 0, 0), (0, -1, 0), (0, 1, 0), (0, 0, -1), (0, 0, 1)]

    def halo_refs(p, k, way):
        dx, dy, dg = HALO[way]
        if dx:
            src = p.at[0:16] if dx < 0 else p.at[48:64]
            return src, s["xh"].at[2 * k + (1 if dx < 0 else 0)]
        if dy:
            return s["ys"].at[2 * k + (0 if dy < 0 else 1)], s["yh"].at[2 * k + (1 if dy < 0 else 0)]
        return s["zs"].at[2 * k + (0 if dg < 0 else 1)], s["zh"].at[2 * k + (1 if dg < 0 else 0)]

    def stage_halos(p, k):
        lane = lane_iota()
        low = jnp.zeros((8, 128), F32)
        high = jnp.zeros((8, 128), F32)
        for v in range(8):
            tile = p[8 * v : 8 * v + 8]
            low = jnp.where(lane == v, tile if v == 0 else pltpu.roll(tile, v, 1), low)
            high = jnp.where(lane == v, pltpu.roll(tile, v + 1, 1), high)
        s["zs"][2 * k] = low
        s["zs"][2 * k + 1] = high
        for x in range(4):
            s["ys"][2 * k, x : x + 1] = p[16 * x : 16 * x + 1]
            s["ys"][2 * k + 1, x : x + 1] = p[16 * x + 15 : 16 * x + 16]

    def send_halos(p, k):
        for way, (dx, dy, dg) in enumerate(HALO):
            src, dst = halo_refs(p, k, way)
            sem = 6 * k + way
            start_if(inside(dx, dy, dg), src, dst, SEND_AT["halo"] + sem, RECV_AT["halo"] + sem, (g + dg, gx + dx, gy + dy))

    def wait_halos(p, k):
        for way, (dx, dy, dg) in enumerate(HALO):
            _, dst = halo_refs(p, k, way)
            wait_recv_if(inside(-dx, -dy, -dg), dst, RECV_AT["halo"] + 6 * k + way)

    def around(p, k):
        lane = lane_iota()
        value = p[...]
        xlo, xhi = s["xh"][2 * k], s["xh"][2 * k + 1]
        total = jnp.concatenate([xlo, value[:48]], 0) + jnp.concatenate([value[16:], xhi], 0)
        ylo = jnp.concatenate([jnp.broadcast_to(s["yh"][2 * k, x : x + 1], (16, 128)) for x in range(4)], 0)
        yhi = jnp.concatenate([jnp.broadcast_to(s["yh"][2 * k + 1, x : x + 1], (16, 128)) for x in range(4)], 0)
        row = lax.rem(sub_iota((64, 128)), 16)
        total = total + jnp.where(row == 0, ylo, pltpu.roll(value, 1, 0))
        total = total + jnp.where(row == 15, yhi, pltpu.roll(value, 63, 0))
        zlo, zhi = s["zh"][2 * k], s["zh"][2 * k + 1]
        parts = []
        for v in range(8):
            tile = value[8 * v : 8 * v + 8]
            below = zlo if v == 0 else pltpu.roll(zlo, LANES - v, 1)
            above = pltpu.roll(zhi, LANES - 1 - v, 1)
            parts.append(
                jnp.where(lane == 0, below, pltpu.roll(tile, 1, 1))
                + jnp.where(lane == LANES - 1, above, pltpu.roll(tile, LANES - 1, 1))
            )
        return total + jnp.concatenate(parts, 0)

    def cols(i, width=1024):
        return pl.ds(pl.multiple_of(i * width, width), width)

    def rows8(i):
        return pl.ds(pl.multiple_of(i * 8, 8), 8)

    def flow():
        for name in ("pres", "host", "stor", "well", "srcs", "blk", "bas"):
            local(name).start()
        for name in ("xh", "yh", "zh"):
            s[name][...] = jnp.zeros(SCRATCH[name][0], F32)
        count = I32(1)
        greet(gx >= 0, (top, gx, gy))
        for dx, dy, dg in HALO:
            greet(inside(dx, dy, dg), (g + dg, gx + dx, gy + dy))
            count = count + as_int(inside(dx, dy, dg))
        local("pres").wait()
        stage_halos(s["pres"], 0)
        pl.semaphore_wait(pltpu.get_barrier_semaphore(), count)
        send_halos(s["pres"], 0)

        local("host").wait()
        iota_l = sub_iota((128, 128))
        iota_r = sub_iota((64, 128))

        def hosts(i):
            index = s["host"][rows8(i)]
            lanes, rows = index & 127, index >> 7
            s["rowi"][rows8(i)] = rows.astype(F32)
            left, right = [], []
            for r in range(8):
                left.append((iota_l == lanes[r : r + 1]).astype(F32).astype(BF16))
                right.append((iota_r == rows[r : r + 1]).astype(F32).astype(BF16))
            s["ol"][:, cols(i)] = jnp.concatenate(left, 1)
            s["oh"][:, cols(i)] = jnp.concatenate(right, 1)

        loop(8, hosts)
        for name in ("stor", "well", "srcs", "blk", "bas"):
            local(name).wait()
        s["diag"][...] = 6.0 + s["stor"][...] + WELL * s["well"][...].astype(F32)

        def blocks(i):
            index = s["blk"][rows8(i)]
            diag = s["diag"][rows8(i)]
            parts, highs, lows = [], [], []
            for r in range(8):
                parts.append((iota_r == index[r : r + 1]).astype(F32).astype(BF16))
                weight = s["bas"][pl.ds(i * 8 + r, 8, stride=64), :]
                s["wt"][i * 8 + r] = weight
                term = weight * weight * diag[r : r + 1]
                high = term.astype(BF16).astype(F32)
                highs.append(jnp.concatenate([high, term - high], 0).astype(BF16))
            s["ob"][:, cols(i)] = jnp.concatenate(parts, 1)
            s["wr"][:, cols(i)] = jnp.concatenate(highs, 1)

        loop(8, blocks)
        wait_recv_if(gx >= 0, s["sti"], RECV_AT["strain"])
        high, low = split(s["sti"][...])
        s["t2"][0:64] = high
        s["t2"][64:128] = low

        iota_f = iota_r.astype(F32)

        def gather(i):
            table = dot_nn(s["t2"][...], s["ol"][:, cols(i)])
            rows = s["rowi"][rows8(i)]
            parts = []
            for r in range(8):
                column = table[0:64, 128 * r : 128 * r + 128] + table[64:128, 128 * r : 128 * r + 128]
                parts.append(jnp.sum(jnp.where(iota_f == rows[r : r + 1], column, 0.0), axis=0, keepdims=True))
            s["frc"][rows8(i)] = s["srcs"][rows8(i)] - BIOT * jnp.concatenate(parts, 0)

        loop(8, gather)

        def residual(p, k):
            return s["frc"][...] + around(p, k) - s["diag"][...] * p[...]

        wait_halos(s["pres"], 0)
        s["p1"][...] = s["pres"][...] + RELAX * residual(s["pres"], 0) / s["diag"][...]
        stage_halos(s["p1"], 1)
        send_halos(s["p1"], 1)
        norms = dot_nt(s["wr"][...], s["ob"][...])
        s["scale"][...] = 1.0 + norms[0:8] + norms[8:16]
        wait_halos(s["p1"], 1)
        s["p2"][...] = s["p1"][...] + RELAX * residual(s["p1"], 1) / s["diag"][...]
        stage_halos(s["p2"], 2)
        send_halos(s["p2"], 2)
        s["cnt"][...] = dot_nt(s["oh"][...], s["ol"][...])
        start_if(gx >= 0, s["cnt"], s["cr"].at[g], SEND_AT["counts"], RECV_AT["counts"] + g, (top, gx, gy))
        wait_halos(s["p2"], 2)
        s["rem"][...] = residual(s["p2"], 2)

        def weighted(i):
            rem = s["rem"][rows8(i)]
            highs = []
            for r in range(8):
                term = s["wt"][i * 8 + r] * rem[r : r + 1]
                high = term.astype(BF16).astype(F32)
                highs.append(jnp.concatenate([high, term - high], 0).astype(BF16))
            s["wr"][:, cols(i)] = jnp.concatenate(highs, 1)

        loop(8, weighted)
        coarse = dot_nt(s["wr"][...], s["ob"][...])
        fixed = (coarse[0:8] + coarse[8:16]) / s["scale"][...]
        high = fixed.astype(BF16).astype(F32)
        s["corr"][...] = jnp.concatenate([high, fixed - high], 0).astype(BF16)

        def spread_back(i):
            back = dot_nn(s["corr"][...], s["ob"][:, cols(i)])
            back = back[0:8] + back[8:16]
            parts = []
            for r in range(8):
                parts.append(jnp.sum(s["wt"][i * 8 + r] * back[:, 128 * r : 128 * r + 128], axis=0, keepdims=True))
            updated = s["p2"][rows8(i)] + jnp.concatenate(parts, 0)
            po[rows8(i)] = updated
            change = updated - s["pres"][rows8(i)]
            high = change.astype(BF16).astype(F32)
            low = change - high
            tops, lows = [], []
            for r in range(8):
                one = s["oh"][:, pl.ds(pl.multiple_of(i * 1024 + 128 * r, 128), 128)]
                tops.append(one * jnp.broadcast_to(high[r : r + 1], (64, 128)).astype(BF16))
                lows.append(one * jnp.broadcast_to(low[r : r + 1], (64, 128)).astype(BF16))
            s["ar"][0:64, cols(i)] = jnp.concatenate(tops, 1)
            s["ar"][64:128, cols(i)] = jnp.concatenate(lows, 1)

        loop(8, spread_back)
        both = dot_nt(s["ar"][...], s["ol"][...])
        s["sm"][...] = both[0:64] + both[64:128]
        start_if(gx >= 0, s["sm"], s["sr"].at[g], SEND_AT["sums"], RECV_AT["sums"] + g, (top, gx, gy))
        do[...] = jnp.zeros((192, 128), F32)
        for k, p in enumerate((s["pres"], s["p1"], s["p2"])):
            for way, (dx, dy, dg) in enumerate(HALO):
                src, _ = halo_refs(p, k, way)
                wait_send_if(inside(dx, dy, dg), src, SEND_AT["halo"] + 6 * k + way)
        wait_send_if(gx >= 0, s["cnt"], SEND_AT["counts"])
        wait_send_if(gx >= 0, s["sm"], SEND_AT["sums"])

    def x_from(dx, low, high):
        first = low
        if dx == 0:
            return slice(first, first + 4), slice(first, first + 4)
        if dx < 0:
            return slice(first, first + high), slice(first + 4, first + 4 + high)
        return slice(first + 4 - low, first + 4), slice(0, low)

    def node_refs(arr, ylo, yhi, dx, dy):
        xs, xd = x_from(dx, 2, 2)
        if dy == 0:
            return arr.at[xs, 16:80], arr.at[xd, 16:80]
        if dy > 0:
            return arr.at[xs, 64:80], ylo.at[xd]
        return arr.at[xs, 16:32], yhi.at[xd]

    def raw_refs(arr, dx, dy):
        xs, xd = x_from(dx, 3, 2)
        ysrc, ydst = {0: (slice(8, 24), slice(8, 24)), 1: (slice(16, 24), slice(0, 8)), -1: (slice(8, 16), slice(24, 32))}[dy]
        return arr.at[xs, ysrc], arr.at[xd, ydst]

    def exchange_start(refs_of, name):
        for k, (dx, dy) in enumerate(AROUND):
            src, dst = refs_of(dx, dy)
            start_if(inside(dx, dy), src, dst, SEND_AT[name] + k, RECV_AT[name] + k, (g, gx + dx, gy + dy))

    def exchange_wait(refs_of, name):
        for k, (dx, dy) in enumerate(AROUND):
            _, dst = refs_of(dx, dy)
            wait_recv_if(inside(-dx, -dy), dst, RECV_AT[name] + k)

    def exchange_done(refs_of, name):
        for k, (dx, dy) in enumerate(AROUND):
            src, _ = refs_of(dx, dy)
            wait_send_if(inside(dx, dy), src, SEND_AT[name] + k)

    def close_nodes(arr, ylo, yhi):
        half = sub_iota() < 4

        def plane(x):
            for k in range(2):
                own = arr[x, 64 + 8 * k : 72 + 8 * k]
                arr[x, 8 * k : 8 * k + 8] = pltpu.roll(jnp.where(half, own, ylo[x, 8 * k : 8 * k + 8]), 4, 0)
                own = arr[x, 16 + 8 * k : 24 + 8 * k]
                arr[x, 80 + 8 * k : 88 + 8 * k] = pltpu.roll(jnp.where(half, yhi[x, 8 * k : 8 * k + 8], own), 4, 0)

        loop(8, plane)

    def zero_edges(arr, ylo, yhi):
        @pl.when(gx == 0)
        def _():
            arr[0:2] = jnp.zeros((2,) + arr.shape[1:], F32)
            ylo[0:2] = jnp.zeros((2, 16, 128), F32)
            yhi[0:2] = jnp.zeros((2, 16, 128), F32)

        @pl.when(gx == nx - 1)
        def _():
            arr[6:8] = jnp.zeros((2,) + arr.shape[1:], F32)
            ylo[6:8] = jnp.zeros((2, 16, 128), F32)
            yhi[6:8] = jnp.zeros((2, 16, 128), F32)

        @pl.when(gy == 0)
        def _():
            ylo[...] = jnp.zeros((8, 16, 128), F32)

        @pl.when(gy == ny - 1)
        def _():
            yhi[...] = jnp.zeros((8, 16, 128), F32)

    def zero_raw(arr):
        @pl.when(gx == 0)
        def _():
            arr[0:3] = jnp.zeros((3, 32, 128), F32)

        @pl.when(gx == nx - 1)
        def _():
            arr[7:9] = jnp.zeros((2, 32, 128), F32)

        @pl.when(gy == 0)
        def _():
            arr[:, 0:8] = jnp.zeros((9, 8, 128), F32)

        @pl.when(gy == ny - 1)
        def _():
            arr[:, 24:32] = jnp.zeros((9, 8, 128), F32)

    def x_ok(x):
        bad = ((x < 2) & (gx == 0)) | ((x >= 6) & (gx == nx - 1))
        return jnp.where(bad, 0.0, 1.0).astype(F32)

    def y_ok(j):
        sub = sub_iota()
        mask = jnp.where((sub & 3) < 3, 1.0, 0.0)
        if j < 2:
            mask = jnp.where(sub < 4, mask * jnp.where(gy == 0, 0.0, 1.0), mask)
        if j > 9:
            mask = jnp.where(sub >= 4, mask * jnp.where(gy == ny - 1, 0.0, 1.0), mask)
        return mask

    def operate(arr, elem_x, elem_j, use):
        (xa, xb), (ja, jb) = elem_x, elem_j
        ph, plo, vs = s["ph"], s["plo"], s["vs"]
        wide = jb - ja

        def stage(k):
            x = xa + k
            for j in range(ja, jb + 1):
                value = arr[x, 8 * j : 8 * j + 8]
                pair = jnp.concatenate([value, shift_down(value)], 0)
                high, low = split(pair)
                ph[x, 16 * j : 16 * j + 16] = high
                plo[x, 16 * j : 16 * j + 16] = low

        loop(xb - xa + 1, stage)

        def elements(k):
            x = xa + k
            columns = []
            for j in range(ja, jb):
                at = slice(16 * j, 16 * j + 32)
                first, second = ph[x, at], ph[x + 1, at]
                columns.append(jnp.concatenate([first, second, plo[x, at], plo[x + 1, at], first, second], 0))
            product = dot_nn(s["kl"][...], jnp.concatenate(columns, 1))
            for c in range(wide):
                j = ja + c
                weight = s["wtile"][x, 8 * j : 8 * j + 8]
                vs[x, 64 * j : 64 * j + 64] = product[:, 128 * c : 128 * c + 128] * jnp.concatenate([weight] * 8, 0)

        loop(xb - xa, elements)

        spring = SPRING * s["kap"][...]

        def nodes(k):
            x = xa + 1 + k
            for j in range(ja + 1, jb):
                total = None
                for a in range(2):
                    for b in range(2):
                        at = 64 * (j - b) + 16 * (2 * a + b)
                        part = vs[x - a, at : at + 16]
                        total = part if total is None else total + part
                node = arr[x, 8 * j : 8 * j + 8]
                use(x, j, node, total[0:8] + shift_up(total[8:16]) + spring * node)

        loop(xb - xa - 1, nodes)

    def mechanics():
        for name in ("disp", "mask", "modl", "stif", "body"):
            local(name).start()
        greet_count = I32(top)
        for gg in range(top):
            greet(gx >= 0, (gg, gx, gy))
        for dx, dy in AROUND:
            greet(inside(dx, dy), (g, gx + dx, gy + dy))
            greet_count = greet_count + as_int(inside(dx, dy))
        local("disp").wait()
        disp = s["disp"]
        for m in range(3):
            for x in range(4):
                s["uys"][4 * m + x : 4 * m + x + 1] = disp[m, 16 * x : 16 * x + 1]
            s["ucs"][m : m + 1] = disp[m, 0:1]
        pl.semaphore_wait(pltpu.get_barrier_semaphore(), greet_count)

        near = [
            (-1, 0, disp.at[:, 0:16], s["ux"]),
            (0, -1, s["uys"], s["uy"]),
            (-1, -1, s["ucs"], s["uc"]),
        ]
        for k, (dx, dy, src, dst) in enumerate(near):
            start_if(inside(dx, dy), src, dst, SEND_AT["ux"] + k, RECV_AT["ux"] + k, (g, gx + dx, gy + dy))

        @pl.when(gx == nx - 1)
        def _():
            s["ux"][...] = jnp.zeros((3, 16, 128), F32)
            s["uc"][...] = jnp.zeros((8, 128), F32)

        @pl.when(gy == ny - 1)
        def _():
            s["uy"][...] = jnp.zeros((16, 128), F32)
            s["uc"][...] = jnp.zeros((8, 128), F32)

        local("mask").wait()
        for k, (dx, dy, _, dst) in enumerate(near):
            wait_recv_if(inside(-dx, -dy), dst, RECV_AT["ux"] + k)

        row15 = sub_iota((16, 128)) == 15
        before = None
        for x in range(5):
            sums, diffs = [], []
            for m in range(3):
                plane = disp[m, 16 * x : 16 * x + 16] if x < 4 else s["ux"][m]
                beyond = s["uy"][4 * m + x : 4 * m + x + 1] if x < 4 else s["uc"][m : m + 1]
                up = jnp.where(row15, jnp.broadcast_to(beyond, (16, 128)), pltpu.roll(plane, 15, 0))
                sums.append(up + plane)
                diffs.append(up - plane)
            now = (sums[0], diffs[1], sums[2])
            if before is not None:
                plain = (now[0] - before[0]) + (now[1] + before[1])
                third = now[2] + before[2]
                value = (plain - third) + shift_down(plain + third)
                at = 16 * (x - 1)
                s["stro"][at : at + 16] = 0.25 * s["mask"][at : at + 16].astype(F32) * value
            before = now
        for gg in range(top):
            start_if(gx >= 0, s["stro"], s["sti"], SEND_AT["strain"] + gg, RECV_AT["strain"], (gg, gx, gy))

        ue, ce = s["ue"], s["ce"]
        local("modl").wait()
        local("body").wait()
        local("stif").wait()
        zero = jnp.zeros((64, 128), F32)
        for x in range(4):
            ue[x + 2, 16:80] = zero
            s["bt"][x] = zero
            for m in range(3):
                for h in range(2):
                    at = 16 * x + 8 * h
                    ue[x + 2, pl.ds(16 + 4 * h + m, 8, stride=8), :] = disp[m, at : at + 8]
                    at = 64 * m + at
                    s["bt"][x, pl.ds(4 * h + m, 8, stride=8), :] = s["body"][at : at + 8]
            at = 16 * x
            s["mw"][x + 3, 8:24] = s["modl"][at : at + 16] * s["mask"][at : at + 16].astype(F32)
        ue_refs = functools.partial(node_refs, ue, s["uyl"], s["uyh"])
        ce_refs = functools.partial(node_refs, ce, s["cyl"], s["cyh"])
        mw_refs = functools.partial(raw_refs, s["mw"])
        gr_refs = functools.partial(raw_refs, s["gr"])
        exchange_start(ue_refs, "ue")
        exchange_start(mw_refs, "mw")
        zero_edges(ue, s["uyl"], s["uyh"])
        zero_edges(ce, s["cyl"], s["cyh"])
        zero_raw(s["mw"])
        zero_raw(s["gr"])

        stiff = s["stif"][...]
        largest = jnp.max(jnp.max(jnp.abs(stiff), axis=1, keepdims=True), axis=0, keepdims=True)
        s["kap"][...] = jnp.broadcast_to(1.0 / largest, (8, 128))
        high, low = split(stiff / largest)
        line = lax.broadcasted_iota(I32, (64, 24), 0)
        entry = lax.broadcasted_iota(I32, (64, 24), 1)
        pick = jnp.where(((line & 3) < 3) & (3 * (line >> 3) + (line & 3) == entry), 1.0, 0.0).astype(BF16)
        r_half = (lax.broadcasted_iota(I32, (64, 64), 0) >> 2) & 1
        c_half = (lax.broadcasted_iota(I32, (64, 64), 1) >> 2) & 1
        wide = []
        for part in (high, low):
            rows = dot_nn(pick, part).astype(BF16)
            wide.append(jnp.where(r_half == c_half, dot_nt(rows, pick), 0.0).astype(BF16))
        s["kl"][...] = jnp.concatenate([wide[0], wide[0], wide[1]], 1)

        step, turn = 1, 0
        for size, coord, axis in ((nx, gx, 1), (ny, gy, 2)):
            step = 1
            while step < size:
                back, ahead = coord - step >= 0, coord + step < size
                for ok, move in ((back, -step), (ahead, step)):
                    device = (g, gx + move, gy) if axis == 1 else (g, gx, gy + move)

                    @pl.when(ok)
                    def _():
                        pl.semaphore_signal(known.at[turn], inc=1, device_id=device, device_id_type=MESH)

                pl.semaphore_wait(known.at[turn], as_int(back) + as_int(ahead))
                step, turn = step * 2, turn + 1

        exchange_wait(mw_refs, "mw")
        half = sub_iota() < 4

        def pair_of_rows(arr, x, low):
            return jnp.where(
                half,
                jnp.broadcast_to(arr[x, low : low + 1], (8, 128)),
                jnp.broadcast_to(arr[x, low + 8 : low + 9], (8, 128)),
            )

        def weights(x):
            for j in range(11):
                s["wtile"][x, 8 * j : 8 * j + 8] = pair_of_rows(s["mw"], x + 1, 6 + j)

        loop(7, weights)
        exchange_wait(ue_refs, "ue")
        close_nodes(ue, s["uyl"], s["uyh"])
        kappa = jnp.broadcast_to(largest, (8, 128))

        def initial(x, j, node, product):
            ce[x, 8 * j : 8 * j + 8] = s["bt"][x - 2, 8 * (j - 2) : 8 * (j - 2) + 8] - kappa * product

        operate(ue, (1, 6), (1, 10), initial)
        exchange_start(ce_refs, "ce")
        exchange_wait(ce_refs, "ce")
        close_nodes(ce, s["cyl"], s["cyh"])

        for gg in range(top):
            wait_recv_if(gx >= 0, s["cr"].at[gg], RECV_AT["counts"] + gg)
        counts = s["cr"][0]
        for gg in range(1, top):
            counts = counts + s["cr"][gg]
        s["fac"][...] = (0.25 * BIOT) * s["mask"][...].astype(F32) / jnp.maximum(counts, 1.0)
        po[...] = jnp.zeros((64, 128), F32)

        for gg in range(top):
            wait_recv_if(gx >= 0, s["sr"].at[gg], RECV_AT["sums"] + gg)
        sums = s["sr"][0]
        for gg in range(1, top):
            sums = sums + s["sr"][gg]
        value = s["fac"][...] * sums
        for x in range(4):
            s["gr"][x + 3, 8:24] = value[16 * x : 16 * x + 16]
        exchange_start(gr_refs, "gr")
        exchange_wait(gr_refs, "gr")

        def tiles(x):
            for j in range(13):
                s["gt"][x, 8 * j : 8 * j + 8] = pair_of_rows(s["gr"], x, 5 + j)

        loop(9, tiles)
        part = sub_iota() & 3
        signs = [jnp.where(part == m, -1.0, 1.0).astype(F32) for m in range(3)]
        rx, qe = s["rx"], s["qe"]

        def force(x):
            okay = x_ok(x)
            last = None
            for j in range(13):
                at = slice(8 * j, 8 * j + 8)
                along_x = s["gt"][x, at] + signs[0] * s["gt"][x + 1, at]
                if last is not None:
                    both = last + signs[1] * along_x
                    node = shift_up(both) + signs[2] * both
                    k = j - 1
                    at = slice(8 * k, 8 * k + 8)
                    rx[x, at] = (ce[x, at] + node) * (y_ok(k) * okay)
                last = along_x

        loop(8, force)

        def first(x, j, node, product):
            qe[x, 8 * j : 8 * j + 8] = product * (y_ok(j) * x_ok(x))

        operate(rx, (0, 7), (0, 11), first)
        acc = s["dots"]
        acc[...] = jnp.zeros((8, 128), F32)

        def second(x, j, node, product):
            r = rx[x, 8 * j : 8 * j + 8]
            terms = [r * r, r * node, node * node, node * product]
            rows = [jnp.sum(term, axis=0, keepdims=True) for term in terms]
            acc[0:4] += jnp.concatenate(rows, 0)

        operate(qe, (1, 6), (1, 10), second)
        ar1, ar2 = s["ar1"], s["ar2"]
        for d in range(1, ny):
            start_if(gx >= 0, acc, ar1.at[d], SEND_AT["ary"] + d, RECV_AT["ary"] + d, (g, gx, lax.rem(gy + d, ny)))

        def to_rows(arr, out):
            for x in range(4):
                for m in range(3):
                    for h in range(2):
                        at = 64 * m + 16 * x + 8 * h
                        out[at : at + 8] = arr[x + 2, pl.ds(16 + 4 * h + m, 8, stride=8), :]

        to_rows(rx, s["rr"])
        total = acc[...]
        for d in range(1, ny):
            wait_recv_if(gx >= 0, ar1.at[d], RECV_AT["ary"] + d)
            total = total + ar1[d]
        total = jnp.broadcast_to(jnp.sum(total, axis=1, keepdims=True), (8, 128))
        s["row"][...] = jnp.sum(jnp.where(lane_iota() == sub_iota(), total, 0.0), axis=0, keepdims=True)
        for d in range(1, nx):
            start_if(gx >= 0, s["row"], ar2.at[d], SEND_AT["arx"] + d, RECV_AT["arx"] + d, (g, lax.rem(gx + d, nx), gy))
        to_rows(qe, s["qr"])
        total = s["row"][...]
        for d in range(1, nx):
            wait_recv_if(gx >= 0, ar2.at[d], RECV_AT["arx"] + d)
            total = total + ar2[d]
        lane = lane_iota((1, 128))
        aa, bb, cc, ee = [
            jnp.broadcast_to(jnp.sum(jnp.where(lane == k, total, 0.0), axis=1, keepdims=True), (8, 128)) for k in range(4)
        ]
        step0 = aa / bb
        new = step0 * step0 * cc - aa
        along = bb - 2.0 * step0 * cc + step0 * step0 * ee
        ratio = new / aa
        step1 = new / (along - ratio * new / step0)
        inverse = s["kap"][...]
        alpha = (step0 + step1 * (1.0 + ratio)) * inverse
        gamma = step1 * step0 * inverse
        for k in range(24):
            at = 8 * k
            m, r = divmod(at, 64)
            do[at : at + 8] = disp[m, r : r + 8] + alpha * s["rr"][at : at + 8] - gamma * s["qr"][at : at + 8]

        for k, (dx, dy, src, _) in enumerate(near):
            wait_send_if(inside(dx, dy), src, SEND_AT["ux"] + k)
        for gg in range(top):
            wait_send_if(gx >= 0, s["stro"], SEND_AT["strain"] + gg)
        for refs_of, name in ((ue_refs, "ue"), (mw_refs, "mw"), (ce_refs, "ce"), (gr_refs, "gr")):
            exchange_done(refs_of, name)
        for d in range(1, ny):
            wait_send_if(gx >= 0, acc, SEND_AT["ary"] + d)
        for d in range(1, nx):
            wait_send_if(gx >= 0, s["row"], SEND_AT["arx"] + d)

    pl.when(jnp.logical_not(mech))(flow)
    pl.when(mech)(mechanics)


def local(sizes, *arrays):
    shapes = [(64, 128)] * 5 + [(512, 128), (64, 128), (3, 64, 128), (192, 128), (64, 128), (64, 128), (24, 24)]
    flat = [array.reshape(shape) for array, shape in zip(arrays, shapes)]
    scratch = [pltpu.VMEM(shape, dtype) for shape, dtype in SCRATCH.values()]
    scratch += [
        pltpu.SemaphoreType.DMA((12,)),
        pltpu.SemaphoreType.DMA((N_SEND,)),
        pltpu.SemaphoreType.DMA((N_RECV,)),
        pltpu.SemaphoreType.REGULAR((8,)),
    ]
    pressure, displacement = pl.pallas_call(
        functools.partial(kernel, sizes),
        out_shape=(jax.ShapeDtypeStruct((64, 128), F32), jax.ShapeDtypeStruct((192, 128), F32)),
        in_specs=[pl.BlockSpec(memory_space=pl.ANY)] * 12,
        out_specs=(pl.BlockSpec(memory_space=pltpu.VMEM),) * 2,
        scratch_shapes=scratch,
        compiler_params=pltpu.CompilerParams(collective_id=0, has_side_effects=True),
    )(*flat)
    return pressure.reshape(arrays[0].shape), displacement.reshape(arrays[7].shape)


def solution(mesh):
    cell = P("grp", "gx", "gy", None)
    many = P("grp", None, "gx", "gy", None)
    sizes = (mesh.shape["grp"], mesh.shape["gx"], mesh.shape["gy"])
    return jax.shard_map(
        functools.partial(local, sizes),
        mesh=mesh,
        in_specs=(cell,) * 5 + (many, cell, many, many, cell, cell, P()),
        out_specs=(cell, many),
        check_vma=False,
    )
```

```python
import functools

import jax
import jax.numpy as jnp
from jax import lax
from jax.experimental import pallas as pl
from jax.experimental.pallas import tpu as pltpu
from jax.sharding import PartitionSpec as P

F32 = jnp.float32
BF16 = jnp.bfloat16
I32 = jnp.int32
MESH = pl.DeviceIdType.MESH
NBLK = 64
LANES = 128
ROWS = 64
BIOT = 1.5
RELAX = 0.8
SPRING = 0.5
WELL = 4.0
AROUND = [(dx, dy) for dx in (-1, 0, 1) for dy in (-1, 0, 1) if (dx, dy) != (0, 0)]

SEND = dict(ux=3, strain=3, ue=8, ce=8, mw=8, gr=8, sums=1, counts=1, halo=18, ary=4, arx=16)
RECV = dict(ux=3, strain=1, ue=8, ce=8, mw=8, gr=8, sums=3, counts=3, halo=18, ary=4, arx=16)


def offsets(table):
    at, out = 0, {}
    for name, count in table.items():
        out[name] = at
        at += count
    return out, at


SEND_AT, N_SEND = offsets(SEND)
RECV_AT, N_RECV = offsets(RECV)

SCRATCH = dict(
    pres=((64, 128), F32), srcs=((64, 128), F32), stor=((64, 128), F32), well=((64, 128), I32),
    blk=((64, 128), I32), bas=((512, 128), F32), host=((64, 128), I32),
    disp=((3, 64, 128), F32), body=((192, 128), F32), modl=((64, 128), F32), mask=((64, 128), I32),
    stif=((24, 24), F32),
    p1=((64, 128), F32), p2=((64, 128), F32), diag=((64, 128), F32), frc=((64, 128), F32),
    xh=((6, 16, 128), F32), yh=((6, 8, 128), F32), zh=((6, 8, 128), F32),
    ys=((6, 8, 128), F32), zs=((6, 8, 128), F32),
    sti=((64, 128), F32), ol=((128, 8192), BF16), oh=((64, 8192), BF16), ob=((64, 8192), BF16),
    wt=((64, 8, 128), F32), wr=((16, 8192), BF16), scale=((8, 64), F32),
    chg=((64, 128), F32), lo=((64, 128), F32),
    cnt=((64, 128), F32), sm=((64, 128), F32), rem=((64, 128), F32),
    ux=((3, 16, 128), F32), uy=((16, 128), F32), uc=((8, 128), F32),
    uys=((16, 128), F32), ucs=((8, 128), F32), stro=((64, 128), F32),
    ue=((8, 96, 128), F32), uyl=((8, 16, 128), F32), uyh=((8, 16, 128), F32),
    ce=((8, 96, 128), F32), cyl=((8, 16, 128), F32), cyh=((8, 16, 128), F32),
    mw=((9, 32, 128), F32), gr=((9, 32, 128), F32), wtile=((7, 88, 128), F32),
    sr=((3, 64, 128), F32), cr=((3, 64, 128), F32), fac=((64, 128), F32),
    gt=((9, 104, 128), F32), rx=((8, 96, 128), F32), qe=((8, 96, 128), F32),
    ph=((8, 192, 128), BF16), plo=((8, 192, 128), BF16), vs=((7, 704, 128), F32),
    kl=((64, 192), BF16), kap=((8, 128), F32), bt=((4, 64, 128), F32),
    rr=((192, 128), F32), qr=((192, 128), F32), dots=((8, 128), F32),
    ar1=((4, 8, 128), F32), ar2=((16, 1, 128), F32), row=((1, 128), F32),
)


def split(value):
    high = value.astype(BF16)
    return high, (value - high.astype(F32)).astype(BF16)


def dot_nt(a, b):
    return lax.dot_general(a, b, (((1,), (1,)), ((), ())), preferred_element_type=F32)


def dot_nn(a, b):
    return jnp.dot(a, b, preferred_element_type=F32)


def lane_iota(shape=(8, 128)):
    return lax.broadcasted_iota(I32, shape, len(shape) - 1)


def sub_iota(shape=(8, 128)):
    return lax.broadcasted_iota(I32, shape, len(shape) - 2)


def shift_down(value):
    return jnp.where(lane_iota(value.shape) == LANES - 1, 0.0, pltpu.roll(value, LANES - 1, 1))


def shift_up(value):
    return jnp.where(lane_iota(value.shape) == 0, 0.0, pltpu.roll(value, 1, 1))


def loop(count, body, unroll=1):
    def step(i, carry):
        body(i)
        return carry

    lax.fori_loop(0, count, step, 0, unroll=unroll)


def kernel(sizes, *refs):
    groups, nx, ny = sizes
    ins, (po, do), rest = refs[:12], refs[12:14], refs[14:]
    s = dict(zip(SCRATCH, rest))
    in_sems, send_sems, recv_sems, known = rest[len(SCRATCH):]
    g, gx, gy = lax.axis_index("grp"), lax.axis_index("gx"), lax.axis_index("gy")
    top = groups - 1
    mech = g == top
    names = ["pres", "srcs", "stor", "well", "blk", "bas", "host", "disp", "body", "modl", "mask", "stif"]

    def local(name):
        k = names.index(name)
        return pltpu.make_async_copy(ins[k], s[name], in_sems.at[k])

    def inside(dx, dy, dg=0):
        x, y = gx + dx, gy + dy
        ok = (x >= 0) & (x < nx) & (y >= 0) & (y < ny)
        if dg:
            ok = ok & (g + dg >= 0) & (g + dg < top)
        return ok

    def as_int(flag):
        return flag.astype(I32)

    def remote(src, dst, send, recv, device):
        return pltpu.make_async_remote_copy(
            src_ref=src, dst_ref=dst, send_sem=send_sems.at[send], recv_sem=recv_sems.at[recv],
            device_id=device, device_id_type=MESH,
        )

    def start_if(ok, *args):
        @pl.when(ok)
        def _():
            remote(*args).start()

    def wait_recv_if(ok, dst, recv):
        @pl.when(ok)
        def _():
            remote(dst, dst, 0, recv, (g, gx, gy)).wait_recv()

    def wait_send_if(ok, src, send):
        @pl.when(ok)
        def _():
            remote(src, src, send, 0, (g, gx, gy)).wait_send()

    def greet(ok, device):
        @pl.when(ok)
        def _():
            pl.semaphore_signal(pltpu.get_barrier_semaphore(), inc=1, device_id=device, device_id_type=MESH)

    HALO = [(-1, 0, 0), (1, 0, 0), (0, -1, 0), (0, 1, 0), (0, 0, -1), (0, 0, 1)]

    def halo_refs(p, k, way):
        dx, dy, dg = HALO[way]
        if dx:
            src = p.at[0:16] if dx < 0 else p.at[48:64]
            return src, s["xh"].at[2 * k + (1 if dx < 0 else 0)]
        if dy:
            return s["ys"].at[2 * k + (0 if dy < 0 else 1)], s["yh"].at[2 * k + (1 if dy < 0 else 0)]
        return s["zs"].at[2 * k + (0 if dg < 0 else 1)], s["zh"].at[2 * k + (1 if dg < 0 else 0)]

    def stage_halos(p, k):
        lane = lane_iota()
        low = jnp.zeros((8, 128), F32)
        high = jnp.zeros((8, 128), F32)
        for v in range(8):
            tile = p[8 * v : 8 * v + 8]
            low = jnp.where(lane == v, tile if v == 0 else pltpu.roll(tile, v, 1), low)
            high = jnp.where(lane == v, pltpu.roll(tile, v + 1, 1), high)
        s["zs"][2 * k] = low
        s["zs"][2 * k + 1] = high
        for x in range(4):
            s["ys"][2 * k, x : x + 1] = p[16 * x : 16 * x + 1]
            s["ys"][2 * k + 1, x : x + 1] = p[16 * x + 15 : 16 * x + 16]

    def send_halos(p, k):
        for way, (dx, dy, dg) in enumerate(HALO):
            src, dst = halo_refs(p, k, way)
            sem = 6 * k + way
            start_if(inside(dx, dy, dg), src, dst, SEND_AT["halo"] + sem, RECV_AT["halo"] + sem, (g + dg, gx + dx, gy + dy))

    def wait_halos(p, k):
        for way, (dx, dy, dg) in enumerate(HALO):
            _, dst = halo_refs(p, k, way)
            wait_recv_if(inside(-dx, -dy, -dg), dst, RECV_AT["halo"] + 6 * k + way)

    def around(p, k):
        lane = lane_iota()
        value = p[...]
        xlo, xhi = s["xh"][2 * k], s["xh"][2 * k + 1]
        total = jnp.concatenate([xlo, value[:48]], 0) + jnp.concatenate([value[16:], xhi], 0)
        ylo = jnp.concatenate([jnp.broadcast_to(s["yh"][2 * k, x : x + 1], (16, 128)) for x in range(4)], 0)
        yhi = jnp.concatenate([jnp.broadcast_to(s["yh"][2 * k + 1, x : x + 1], (16, 128)) for x in range(4)], 0)
        row = lax.rem(sub_iota((64, 128)), 16)
        total = total + jnp.where(row == 0, ylo, pltpu.roll(value, 1, 0))
        total = total + jnp.where(row == 15, yhi, pltpu.roll(value, 63, 0))
        zlo, zhi = s["zh"][2 * k], s["zh"][2 * k + 1]
        parts = []
        for v in range(8):
            tile = value[8 * v : 8 * v + 8]
            below = zlo if v == 0 else pltpu.roll(zlo, LANES - v, 1)
            above = pltpu.roll(zhi, LANES - 1 - v, 1)
            parts.append(
                jnp.where(lane == 0, below, pltpu.roll(tile, 1, 1))
                + jnp.where(lane == LANES - 1, above, pltpu.roll(tile, LANES - 1, 1))
            )
        return total + jnp.concatenate(parts, 0)

    def cols(i, width=1024):
        return pl.ds(pl.multiple_of(i * width, width), width)

    def rows8(i):
        return pl.ds(pl.multiple_of(i * 8, 8), 8)

    def flow():
        for name in ("pres", "host", "stor", "well", "srcs", "blk", "bas"):
            local(name).start()
        for name in ("xh", "yh", "zh"):
            s[name][...] = jnp.zeros(SCRATCH[name][0], F32)
        count = I32(1)
        greet(gx >= 0, (top, gx, gy))
        for dx, dy, dg in HALO:
            greet(inside(dx, dy, dg), (g + dg, gx + dx, gy + dy))
            count = count + as_int(inside(dx, dy, dg))
        local("pres").wait()
        stage_halos(s["pres"], 0)
        pl.semaphore_wait(pltpu.get_barrier_semaphore(), count)
        send_halos(s["pres"], 0)

        local("host").wait()
        iota_l = sub_iota((128, 128))
        iota_r = sub_iota((64, 128))

        def hosts(i):
            index = s["host"][rows8(i)]
            lanes, rows = index & 127, index >> 7
            left, right = [], []
            for r in range(8):
                left.append((iota_l == lanes[r : r + 1]).astype(F32).astype(BF16))
                right.append((iota_r == rows[r : r + 1]).astype(F32).astype(BF16))
            s["ol"][:, cols(i)] = jnp.concatenate(left, 1)
            s["oh"][:, cols(i)] = jnp.concatenate(right, 1)

        loop(8, hosts)
        for name in ("stor", "well", "srcs", "blk", "bas"):
            local(name).wait()
        s["diag"][...] = 6.0 + s["stor"][...] + WELL * s["well"][...].astype(F32)

        def blocks(i):
            index = s["blk"][rows8(i)]
            diag = s["diag"][rows8(i)]
            parts, highs, lows = [], [], []
            for r in range(8):
                parts.append((iota_r == index[r : r + 1]).astype(F32).astype(BF16))
                weight = s["bas"][pl.ds(i * 8 + r, 8, stride=64), :]
                s["wt"][i * 8 + r] = weight
                term = weight * weight * diag[r : r + 1]
                high = term.astype(BF16).astype(F32)
                highs.append(jnp.concatenate([high, term - high], 0).astype(BF16))
            s["ob"][:, cols(i)] = jnp.concatenate(parts, 1)
            s["wr"][:, cols(i)] = jnp.concatenate(highs, 1)

        loop(8, blocks)
        wait_recv_if(gx >= 0, s["sti"], RECV_AT["strain"])
        def gather(i):
            index = s["host"][rows8(i)]
            lanes, rows = index & 127, index >> 7
            found = jnp.zeros((8, 128), F32)
            for r in range(64):
                row = jnp.broadcast_to(s["sti"][r : r + 1], (8, 128))
                found = jnp.where(rows == r, jnp.take_along_axis(row, lanes, axis=1), found)
            s["frc"][rows8(i)] = s["srcs"][rows8(i)] - BIOT * found

        loop(8, gather, True)

        def residual(p, k):
            return s["frc"][...] + around(p, k) - s["diag"][...] * p[...]

        wait_halos(s["pres"], 0)
        s["p1"][...] = s["pres"][...] + RELAX * residual(s["pres"], 0) / s["diag"][...]
        stage_halos(s["p1"], 1)
        send_halos(s["p1"], 1)
        norms = dot_nt(s["wr"][...], s["ob"][...])
        s["scale"][...] = 1.0 + norms[0:8] + norms[8:16]
        wait_halos(s["p1"], 1)
        s["p2"][...] = s["p1"][...] + RELAX * residual(s["p1"], 1) / s["diag"][...]
        stage_halos(s["p2"], 2)
        send_halos(s["p2"], 2)
        s["cnt"][...] = dot_nt(s["oh"][...], s["ol"][...])
        start_if(gx >= 0, s["cnt"], s["cr"].at[g], SEND_AT["counts"], RECV_AT["counts"] + g, (top, gx, gy))
        wait_halos(s["p2"], 2)
        s["rem"][...] = residual(s["p2"], 2)

        coarse = jnp.zeros((16, 64), F32)
        for i in range(8):
            rem = s["rem"][8 * i : 8 * i + 8]
            parts = []
            for r in range(8):
                term = s["wt"][8 * i + r] * rem[r : r + 1]
                high = term.astype(BF16).astype(F32)
                parts.append(jnp.concatenate([high, term - high], 0).astype(BF16))
            coarse = coarse + dot_nt(jnp.concatenate(parts, 1), s["ob"][:, 1024 * i : 1024 * i + 1024])
        fixed = (coarse[0:8] + coarse[8:16]) / s["scale"][...]
        table = jnp.concatenate([fixed, fixed], 1)
        both = jnp.zeros((128, 128), F32)
        for i in range(8):
            at = slice(8 * i, 8 * i + 8)
            blocks_of = s["blk"][at]
            parts = []
            for r in range(8):
                back = jnp.take_along_axis(table, jnp.broadcast_to(blocks_of[r : r + 1], (8, 128)), axis=1)
                parts.append(jnp.sum(s["wt"][8 * i + r] * back, axis=0, keepdims=True))
            updated = s["p2"][at] + jnp.concatenate(parts, 0)
            po[at] = updated
            change = updated - s["pres"][at]
            high = change.astype(BF16).astype(F32)
            low = change - high
            tops, lows = [], []
            for r in range(8):
                one = s["oh"][:, 1024 * i + 128 * r : 1024 * i + 128 * r + 128]
                tops.append(one * jnp.broadcast_to(high[r : r + 1], (64, 128)).astype(BF16))
                lows.append(one * jnp.broadcast_to(low[r : r + 1], (64, 128)).astype(BF16))
            scaled = jnp.concatenate([jnp.concatenate(tops, 1), jnp.concatenate(lows, 1)], 0)
            both = both + dot_nt(scaled, s["ol"][:, 1024 * i : 1024 * i + 1024])
        s["sm"][...] = both[0:64] + both[64:128]
        start_if(gx >= 0, s["sm"], s["sr"].at[g], SEND_AT["sums"], RECV_AT["sums"] + g, (top, gx, gy))
        do[...] = jnp.zeros((192, 128), F32)
        for k, p in enumerate((s["pres"], s["p1"], s["p2"])):
            for way, (dx, dy, dg) in enumerate(HALO):
                src, _ = halo_refs(p, k, way)
                wait_send_if(inside(dx, dy, dg), src, SEND_AT["halo"] + 6 * k + way)
        wait_send_if(gx >= 0, s["cnt"], SEND_AT["counts"])
        wait_send_if(gx >= 0, s["sm"], SEND_AT["sums"])

    def x_from(dx, low, high):
        first = low
        if dx == 0:
            return slice(first, first + 4), slice(first, first + 4)
        if dx < 0:
            return slice(first, first + high), slice(first + 4, first + 4 + high)
        return slice(first + 4 - low, first + 4), slice(0, low)

    def node_refs(arr, ylo, yhi, dx, dy):
        xs, xd = x_from(dx, 2, 2)
        if dy == 0:
            return arr.at[xs, 16:80], arr.at[xd, 16:80]
        if dy > 0:
            return arr.at[xs, 64:80], ylo.at[xd]
        return arr.at[xs, 16:32], yhi.at[xd]

    def raw_refs(arr, dx, dy):
        xs, xd = x_from(dx, 3, 2)
        ysrc, ydst = {0: (slice(8, 24), slice(8, 24)), 1: (slice(16, 24), slice(0, 8)), -1: (slice(8, 16), slice(24, 32))}[dy]
        return arr.at[xs, ysrc], arr.at[xd, ydst]

    def exchange_start(refs_of, name):
        for k, (dx, dy) in enumerate(AROUND):
            src, dst = refs_of(dx, dy)
            start_if(inside(dx, dy), src, dst, SEND_AT[name] + k, RECV_AT[name] + k, (g, gx + dx, gy + dy))

    def exchange_wait(refs_of, name):
        for k, (dx, dy) in enumerate(AROUND):
            _, dst = refs_of(dx, dy)
            wait_recv_if(inside(-dx, -dy), dst, RECV_AT[name] + k)

    def exchange_done(refs_of, name):
        for k, (dx, dy) in enumerate(AROUND):
            src, _ = refs_of(dx, dy)
            wait_send_if(inside(dx, dy), src, SEND_AT[name] + k)

    def close_nodes(arr, ylo, yhi):
        half = sub_iota() < 4

        def plane(x):
            for k in range(2):
                own = arr[x, 64 + 8 * k : 72 + 8 * k]
                arr[x, 8 * k : 8 * k + 8] = pltpu.roll(jnp.where(half, own, ylo[x, 8 * k : 8 * k + 8]), 4, 0)
                own = arr[x, 16 + 8 * k : 24 + 8 * k]
                arr[x, 80 + 8 * k : 88 + 8 * k] = pltpu.roll(jnp.where(half, yhi[x, 8 * k : 8 * k + 8], own), 4, 0)

        loop(8, plane)

    def zero_edges(arr, ylo, yhi):
        @pl.when(gx == 0)
        def _():
            arr[0:2] = jnp.zeros((2,) + arr.shape[1:], F32)
            ylo[0:2] = jnp.zeros((2, 16, 128), F32)
            yhi[0:2] = jnp.zeros((2, 16, 128), F32)

        @pl.when(gx == nx - 1)
        def _():
            arr[6:8] = jnp.zeros((2,) + arr.shape[1:], F32)
            ylo[6:8] = jnp.zeros((2, 16, 128), F32)
            yhi[6:8] = jnp.zeros((2, 16, 128), F32)

        @pl.when(gy == 0)
        def _():
            ylo[...] = jnp.zeros((8, 16, 128), F32)

        @pl.when(gy == ny - 1)
        def _():
            yhi[...] = jnp.zeros((8, 16, 128), F32)

    def zero_raw(arr):
        @pl.when(gx == 0)
        def _():
            arr[0:3] = jnp.zeros((3, 32, 128), F32)

        @pl.when(gx == nx - 1)
        def _():
            arr[7:9] = jnp.zeros((2, 32, 128), F32)

        @pl.when(gy == 0)
        def _():
            arr[:, 0:8] = jnp.zeros((9, 8, 128), F32)

        @pl.when(gy == ny - 1)
        def _():
            arr[:, 24:32] = jnp.zeros((9, 8, 128), F32)

    def x_ok(x):
        bad = ((x < 2) & (gx == 0)) | ((x >= 6) & (gx == nx - 1))
        return jnp.where(bad, 0.0, 1.0).astype(F32)

    def y_ok(j):
        sub = sub_iota()
        mask = jnp.where((sub & 3) < 3, 1.0, 0.0)
        if j < 2:
            mask = jnp.where(sub < 4, mask * jnp.where(gy == 0, 0.0, 1.0), mask)
        if j > 9:
            mask = jnp.where(sub >= 4, mask * jnp.where(gy == ny - 1, 0.0, 1.0), mask)
        return mask

    def operate(arr, elem_x, elem_j, use, unroll=True):
        (xa, xb), (ja, jb) = elem_x, elem_j
        ph, plo, vs = s["ph"], s["plo"], s["vs"]
        wide = jb - ja

        def stage(k):
            x = xa + k
            for j in range(ja, jb + 1):
                value = arr[x, 8 * j : 8 * j + 8]
                pair = jnp.concatenate([value, shift_down(value)], 0)
                high, low = split(pair)
                ph[x, 16 * j : 16 * j + 16] = high
                plo[x, 16 * j : 16 * j + 16] = low

        loop(xb - xa + 1, stage, unroll)

        def elements(k):
            x = xa + k
            columns = []
            for j in range(ja, jb):
                at = slice(16 * j, 16 * j + 32)
                first, second = ph[x, at], ph[x + 1, at]
                columns.append(jnp.concatenate([first, second, plo[x, at], plo[x + 1, at], first, second], 0))
            product = dot_nn(s["kl"][...], jnp.concatenate(columns, 1))
            for c in range(wide):
                j = ja + c
                weight = s["wtile"][x, 8 * j : 8 * j + 8]
                vs[x, 64 * j : 64 * j + 64] = product[:, 128 * c : 128 * c + 128] * jnp.concatenate([weight] * 8, 0)

        loop(xb - xa, elements, unroll)

        spring = SPRING * s["kap"][...]

        def nodes(k):
            x = xa + 1 + k
            for j in range(ja + 1, jb):
                total = None
                for a in range(2):
                    for b in range(2):
                        at = 64 * (j - b) + 16 * (2 * a + b)
                        part = vs[x - a, at : at + 16]
                        total = part if total is None else total + part
                node = arr[x, 8 * j : 8 * j + 8]
                use(x, j, node, total[0:8] + shift_up(total[8:16]) + spring * node)

        loop(xb - xa - 1, nodes, unroll)

    def mechanics():
        for name in ("disp", "mask", "modl", "stif", "body"):
            local(name).start()
        greet_count = I32(top)
        for gg in range(top):
            greet(gx >= 0, (gg, gx, gy))
        for dx, dy in AROUND:
            greet(inside(dx, dy), (g, gx + dx, gy + dy))
            greet_count = greet_count + as_int(inside(dx, dy))
        local("disp").wait()
        disp = s["disp"]
        for m in range(3):
            for x in range(4):
                s["uys"][4 * m + x : 4 * m + x + 1] = disp[m, 16 * x : 16 * x + 1]
            s["ucs"][m : m + 1] = disp[m, 0:1]
        pl.semaphore_wait(pltpu.get_barrier_semaphore(), greet_count)

        near = [
            (-1, 0, disp.at[:, 0:16], s["ux"]),
            (0, -1, s["uys"], s["uy"]),
            (-1, -1, s["ucs"], s["uc"]),
        ]
        for k, (dx, dy, src, dst) in enumerate(near):
            start_if(inside(dx, dy), src, dst, SEND_AT["ux"] + k, RECV_AT["ux"] + k, (g, gx + dx, gy + dy))

        @pl.when(gx == nx - 1)
        def _():
            s["ux"][...] = jnp.zeros((3, 16, 128), F32)
            s["uc"][...] = jnp.zeros((8, 128), F32)

        @pl.when(gy == ny - 1)
        def _():
            s["uy"][...] = jnp.zeros((16, 128), F32)
            s["uc"][...] = jnp.zeros((8, 128), F32)

        local("mask").wait()
        for k, (dx, dy, _, dst) in enumerate(near):
            wait_recv_if(inside(-dx, -dy), dst, RECV_AT["ux"] + k)

        row15 = sub_iota((16, 128)) == 15
        before = None
        for x in range(5):
            sums, diffs = [], []
            for m in range(3):
                plane = disp[m, 16 * x : 16 * x + 16] if x < 4 else s["ux"][m]
                beyond = s["uy"][4 * m + x : 4 * m + x + 1] if x < 4 else s["uc"][m : m + 1]
                up = jnp.where(row15, jnp.broadcast_to(beyond, (16, 128)), pltpu.roll(plane, 15, 0))
                sums.append(up + plane)
                diffs.append(up - plane)
            now = (sums[0], diffs[1], sums[2])
            if before is not None:
                plain = (now[0] - before[0]) + (now[1] + before[1])
                third = now[2] + before[2]
                value = (plain - third) + shift_down(plain + third)
                at = 16 * (x - 1)
                s["stro"][at : at + 16] = 0.25 * s["mask"][at : at + 16].astype(F32) * value
            before = now
        for gg in range(top):
            start_if(gx >= 0, s["stro"], s["sti"], SEND_AT["strain"] + gg, RECV_AT["strain"], (gg, gx, gy))

        ue, ce = s["ue"], s["ce"]
        local("modl").wait()
        local("body").wait()
        local("stif").wait()
        zero = jnp.zeros((64, 128), F32)
        for x in range(4):
            ue[x + 2, 16:80] = zero
            s["bt"][x] = zero
            for m in range(3):
                for h in range(2):
                    at = 16 * x + 8 * h
                    ue[x + 2, pl.ds(16 + 4 * h + m, 8, stride=8), :] = disp[m, at : at + 8]
                    at = 64 * m + at
                    s["bt"][x, pl.ds(4 * h + m, 8, stride=8), :] = s["body"][at : at + 8]
            at = 16 * x
            s["mw"][x + 3, 8:24] = s["modl"][at : at + 16] * s["mask"][at : at + 16].astype(F32)
        ue_refs = functools.partial(node_refs, ue, s["uyl"], s["uyh"])
        ce_refs = functools.partial(node_refs, ce, s["cyl"], s["cyh"])
        mw_refs = functools.partial(raw_refs, s["mw"])
        gr_refs = functools.partial(raw_refs, s["gr"])
        exchange_start(ue_refs, "ue")
        exchange_start(mw_refs, "mw")
        zero_edges(ue, s["uyl"], s["uyh"])
        zero_edges(ce, s["cyl"], s["cyh"])
        zero_raw(s["mw"])
        zero_raw(s["gr"])

        stiff = s["stif"][...]
        largest = jnp.max(jnp.max(jnp.abs(stiff), axis=1, keepdims=True), axis=0, keepdims=True)
        s["kap"][...] = jnp.broadcast_to(1.0 / largest, (8, 128))
        high, low = split(stiff / largest)
        line = lax.broadcasted_iota(I32, (64, 24), 0)
        entry = lax.broadcasted_iota(I32, (64, 24), 1)
        pick = jnp.where(((line & 3) < 3) & (3 * (line >> 3) + (line & 3) == entry), 1.0, 0.0).astype(BF16)
        r_half = (lax.broadcasted_iota(I32, (64, 64), 0) >> 2) & 1
        c_half = (lax.broadcasted_iota(I32, (64, 64), 1) >> 2) & 1
        wide = []
        for part in (high, low):
            rows = dot_nn(pick, part).astype(BF16)
            wide.append(jnp.where(r_half == c_half, dot_nt(rows, pick), 0.0).astype(BF16))
        s["kl"][...] = jnp.concatenate([wide[0], wide[0], wide[1]], 1)

        step, turn = 1, 0
        for size, coord, axis in ((nx, gx, 1), (ny, gy, 2)):
            step = 1
            while step < size:
                back, ahead = coord - step >= 0, coord + step < size
                for ok, move in ((back, -step), (ahead, step)):
                    device = (g, gx + move, gy) if axis == 1 else (g, gx, gy + move)

                    @pl.when(ok)
                    def _():
                        pl.semaphore_signal(known.at[turn], inc=1, device_id=device, device_id_type=MESH)

                pl.semaphore_wait(known.at[turn], as_int(back) + as_int(ahead))
                step, turn = step * 2, turn + 1

        exchange_wait(mw_refs, "mw")
        half = sub_iota() < 4

        def pair_of_rows(arr, x, low):
            return jnp.where(
                half,
                jnp.broadcast_to(arr[x, low : low + 1], (8, 128)),
                jnp.broadcast_to(arr[x, low + 8 : low + 9], (8, 128)),
            )

        def weights(x):
            for j in range(11):
                s["wtile"][x, 8 * j : 8 * j + 8] = pair_of_rows(s["mw"], x + 1, 6 + j)

        loop(7, weights)
        exchange_wait(ue_refs, "ue")
        close_nodes(ue, s["uyl"], s["uyh"])
        kappa = jnp.broadcast_to(largest, (8, 128))

        def initial(x, j, node, product):
            ce[x, 8 * j : 8 * j + 8] = s["bt"][x - 2, 8 * (j - 2) : 8 * (j - 2) + 8] - kappa * product

        operate(ue, (1, 6), (1, 10), initial, 1)
        exchange_start(ce_refs, "ce")
        exchange_wait(ce_refs, "ce")
        close_nodes(ce, s["cyl"], s["cyh"])

        for gg in range(top):
            wait_recv_if(gx >= 0, s["cr"].at[gg], RECV_AT["counts"] + gg)
        counts = s["cr"][0]
        for gg in range(1, top):
            counts = counts + s["cr"][gg]
        s["fac"][...] = (0.25 * BIOT) * s["mask"][...].astype(F32) / jnp.maximum(counts, 1.0)
        po[...] = jnp.zeros((64, 128), F32)

        for gg in range(top):
            wait_recv_if(gx >= 0, s["sr"].at[gg], RECV_AT["sums"] + gg)
        sums = s["sr"][0]
        for gg in range(1, top):
            sums = sums + s["sr"][gg]
        value = s["fac"][...] * sums
        for x in range(4):
            s["gr"][x + 3, 8:24] = value[16 * x : 16 * x + 16]
        exchange_start(gr_refs, "gr")
        exchange_wait(gr_refs, "gr")

        def tiles(x):
            for j in range(13):
                s["gt"][x, 8 * j : 8 * j + 8] = pair_of_rows(s["gr"], x, 5 + j)

        loop(9, tiles, True)
        part = sub_iota() & 3
        signs = [jnp.where(part == m, -1.0, 1.0).astype(F32) for m in range(3)]
        rx, qe = s["rx"], s["qe"]

        def force(x):
            okay = x_ok(x)
            last = None
            for j in range(13):
                at = slice(8 * j, 8 * j + 8)
                along_x = s["gt"][x, at] + signs[0] * s["gt"][x + 1, at]
                if last is not None:
                    both = last + signs[1] * along_x
                    node = shift_up(both) + signs[2] * both
                    k = j - 1
                    at = slice(8 * k, 8 * k + 8)
                    rx[x, at] = (ce[x, at] + node) * (y_ok(k) * okay)
                last = along_x

        loop(8, force, True)

        def first(x, j, node, product):
            qe[x, 8 * j : 8 * j + 8] = product * (y_ok(j) * x_ok(x))

        operate(rx, (0, 7), (0, 11), first)
        acc = s["dots"]
        acc[...] = jnp.zeros((8, 128), F32)

        def second(x, j, node, product):
            r = rx[x, 8 * j : 8 * j + 8]
            terms = [r * r, r * node, node * node, node * product]
            rows = [jnp.sum(term, axis=0, keepdims=True) for term in terms]
            acc[0:4] += jnp.concatenate(rows, 0)

        operate(qe, (1, 6), (1, 10), second)
        ar1, ar2 = s["ar1"], s["ar2"]
        for d in range(1, ny):
            start_if(gx >= 0, acc, ar1.at[d], SEND_AT["ary"] + d, RECV_AT["ary"] + d, (g, gx, lax.rem(gy + d, ny)))

        def to_rows(arr, out):
            for x in range(4):
                for m in range(3):
                    for h in range(2):
                        at = 64 * m + 16 * x + 8 * h
                        out[at : at + 8] = arr[x + 2, pl.ds(16 + 4 * h + m, 8, stride=8), :]

        to_rows(rx, s["rr"])
        total = acc[...]
        for d in range(1, ny):
            wait_recv_if(gx >= 0, ar1.at[d], RECV_AT["ary"] + d)
            total = total + ar1[d]
        total = jnp.broadcast_to(jnp.sum(total, axis=1, keepdims=True), (8, 128))
        s["row"][...] = jnp.sum(jnp.where(lane_iota() == sub_iota(), total, 0.0), axis=0, keepdims=True)
        for d in range(1, nx):
            start_if(gx >= 0, s["row"], ar2.at[d], SEND_AT["arx"] + d, RECV_AT["arx"] + d, (g, lax.rem(gx + d, nx), gy))
        to_rows(qe, s["qr"])
        total = s["row"][...]
        for d in range(1, nx):
            wait_recv_if(gx >= 0, ar2.at[d], RECV_AT["arx"] + d)
            total = total + ar2[d]
        lane = lane_iota((1, 128))
        aa, bb, cc, ee = [
            jnp.broadcast_to(jnp.sum(jnp.where(lane == k, total, 0.0), axis=1, keepdims=True), (8, 128)) for k in range(4)
        ]
        step0 = aa / bb
        new = step0 * step0 * cc - aa
        along = bb - 2.0 * step0 * cc + step0 * step0 * ee
        ratio = new / aa
        step1 = new / (along - ratio * new / step0)
        inverse = s["kap"][...]
        alpha = (step0 + step1 * (1.0 + ratio)) * inverse
        gamma = step1 * step0 * inverse
        for k in range(24):
            at = 8 * k
            m, r = divmod(at, 64)
            do[at : at + 8] = disp[m, r : r + 8] + alpha * s["rr"][at : at + 8] - gamma * s["qr"][at : at + 8]

        for k, (dx, dy, src, _) in enumerate(near):
            wait_send_if(inside(dx, dy), src, SEND_AT["ux"] + k)
        for gg in range(top):
            wait_send_if(gx >= 0, s["stro"], SEND_AT["strain"] + gg)
        for refs_of, name in ((ue_refs, "ue"), (mw_refs, "mw"), (ce_refs, "ce"), (gr_refs, "gr")):
            exchange_done(refs_of, name)
        for d in range(1, ny):
            wait_send_if(gx >= 0, acc, SEND_AT["ary"] + d)
        for d in range(1, nx):
            wait_send_if(gx >= 0, s["row"], SEND_AT["arx"] + d)

    pl.when(jnp.logical_not(mech))(flow)
    pl.when(mech)(mechanics)


def hand_over(p_ref, d_ref, p_out, d_out, sems):
    copies = [pltpu.make_async_copy(p_ref, p_out, sems.at[0]), pltpu.make_async_copy(d_ref, d_out, sems.at[1])]
    for copy in copies:
        copy.start()
    for copy in copies:
        copy.wait()


def local(sizes, *arrays):
    shapes = [(64, 128)] * 5 + [(512, 128), (64, 128), (3, 64, 128), (192, 128), (64, 128), (64, 128), (24, 24)]
    flat = [array.reshape(shape) for array, shape in zip(arrays, shapes)]
    scratch = [pltpu.VMEM(shape, dtype) for shape, dtype in SCRATCH.values()]
    scratch += [
        pltpu.SemaphoreType.DMA((12,)),
        pltpu.SemaphoreType.DMA((N_SEND,)),
        pltpu.SemaphoreType.DMA((N_RECV,)),
        pltpu.SemaphoreType.REGULAR((8,)),
    ]
    pressure, displacement = pl.pallas_call(
        functools.partial(kernel, sizes),
        out_shape=(pltpu.VMEM((64, 128), F32), pltpu.VMEM((192, 128), F32)),
        in_specs=[pl.BlockSpec(memory_space=pl.ANY)] * 12,
        out_specs=(pl.BlockSpec(memory_space=pltpu.VMEM),) * 2,
        scratch_shapes=scratch,
        compiler_params=pltpu.CompilerParams(collective_id=0, has_side_effects=True),
    )(*flat)
    pressure, displacement = pl.pallas_call(
        hand_over,
        out_shape=(jax.ShapeDtypeStruct((64, 128), F32), jax.ShapeDtypeStruct((192, 128), F32)),
        in_specs=[pl.BlockSpec(memory_space=pltpu.VMEM)] * 2,
        out_specs=(pl.BlockSpec(memory_space=pl.ANY),) * 2,
        scratch_shapes=[pltpu.SemaphoreType.DMA((2,))],
    )(pltpu.with_memory_space_constraint(pressure, pltpu.VMEM), pltpu.with_memory_space_constraint(displacement, pltpu.VMEM))
    return pressure.reshape(arrays[0].shape), displacement.reshape(arrays[7].shape)


def solution(mesh):
    cell = P("grp", "gx", "gy", None)
    many = P("grp", None, "gx", "gy", None)
    sizes = (mesh.shape["grp"], mesh.shape["gx"], mesh.shape["gy"])
    return jax.shard_map(
        functools.partial(local, sizes),
        mesh=mesh,
        in_specs=(cell,) * 5 + (many, cell, many, many, cell, cell, P()),
        out_specs=(cell, many),
        check_vma=False,
    )
```

```python
import functools

import jax
import jax.numpy as jnp
from jax import lax
from jax.experimental import pallas as pl
from jax.experimental.pallas import tpu as pltpu
from jax.sharding import PartitionSpec as P

F32 = jnp.float32
BF16 = jnp.bfloat16
I32 = jnp.int32
MESH = pl.DeviceIdType.MESH
NBLK = 64
LANES = 128
ROWS = 64
BIOT = 1.5
RELAX = 0.8
SPRING = 0.5
WELL = 4.0
AROUND = [(-1, -1), (-1, 1), (1, -1), (1, 1), (-1, 0), (1, 0), (0, -1), (0, 1)]

SEND = dict(ux=3, strain=3, ue=8, ce=8, mw=8, gr=8, sums=1, counts=1, halo=18, ar=1)
RECV = dict(ux=3, strain=1, ue=8, ce=8, mw=8, gr=8, sums=3, counts=3, halo=18, ar=1)


def offsets(table):
    at, out = 0, {}
    for name, count in table.items():
        out[name] = at
        at += count
    return out, at


SEND_AT, N_SEND = offsets(SEND)
RECV_AT, N_RECV = offsets(RECV)

SCRATCH = dict(
    pres=((64, 128), F32), srcs=((64, 128), F32), stor=((64, 128), F32), well=((64, 128), I32),
    blk=((64, 128), I32), bas=((512, 128), F32), host=((64, 128), I32),
    disp=((3, 64, 128), F32), body=((192, 128), F32), modl=((64, 128), F32), mask=((64, 128), I32),
    stif=((24, 24), F32),
    p1=((64, 128), F32), p2=((64, 128), F32), diag=((64, 128), F32), frc=((64, 128), F32),
    xh=((6, 16, 128), F32), yh=((6, 8, 128), F32), zh=((6, 8, 128), F32),
    ys=((6, 8, 128), F32), zs=((6, 8, 128), F32),
    sti=((64, 128), F32), ol=((128, 8192), BF16), oh=((64, 8192), BF16), ob=((64, 8192), BF16),
    wt=((64, 8, 128), F32), wr=((16, 8192), BF16), scale=((8, 64), F32),
    chg=((64, 128), F32), lo=((64, 128), F32),
    cnt=((64, 128), F32), sm=((64, 128), F32), rem=((64, 128), F32),
    ux=((3, 16, 128), F32), uy=((16, 128), F32), uc=((8, 128), F32),
    uys=((16, 128), F32), ucs=((8, 128), F32), stro=((64, 128), F32),
    ue=((8, 96, 128), F32), uyl=((8, 16, 128), F32), uyh=((8, 16, 128), F32),
    ce=((8, 96, 128), F32), cyl=((8, 16, 128), F32), cyh=((8, 16, 128), F32),
    mw=((9, 32, 128), F32), gr=((9, 32, 128), F32), wtile=((7, 88, 128), F32),
    sr=((3, 64, 128), F32), cr=((3, 64, 128), F32), fac=((64, 128), F32),
    gt=((9, 104, 128), F32), rx=((8, 96, 128), F32), qe=((8, 96, 128), F32),
    ph=((8, 192, 128), BF16), plo=((8, 192, 128), BF16), vs=((7, 704, 128), F32),
    kl=((64, 192), BF16), kap=((8, 128), F32), bt=((4, 64, 128), F32),
    rr=((192, 128), F32), qr=((192, 128), F32), dots=((8, 128), F32),
    ar=((64, 1, 128), F32), row=((1, 128), F32),
)


def split(value):
    high = value.astype(BF16)
    return high, (value - high.astype(F32)).astype(BF16)


def dot_nt(a, b):
    return lax.dot_general(a, b, (((1,), (1,)), ((), ())), preferred_element_type=F32)


def dot_nn(a, b):
    return jnp.dot(a, b, preferred_element_type=F32)


def lane_iota(shape=(8, 128)):
    return lax.broadcasted_iota(I32, shape, len(shape) - 1)


def sub_iota(shape=(8, 128)):
    return lax.broadcasted_iota(I32, shape, len(shape) - 2)


def shift_down(value):
    return jnp.where(lane_iota(value.shape) == LANES - 1, 0.0, pltpu.roll(value, LANES - 1, 1))


def shift_up(value):
    return jnp.where(lane_iota(value.shape) == 0, 0.0, pltpu.roll(value, 1, 1))


def loop(count, body, unroll=1):
    def step(i, carry):
        body(i)
        return carry

    lax.fori_loop(0, count, step, 0, unroll=unroll)


def kernel(sizes, *refs):
    groups, nx, ny = sizes
    ins, (po, do), rest = refs[:12], refs[12:14], refs[14:]
    s = dict(zip(SCRATCH, rest))
    in_sems, send_sems, recv_sems, known = rest[len(SCRATCH):]
    g, gx, gy = lax.axis_index("grp"), lax.axis_index("gx"), lax.axis_index("gy")
    top = groups - 1
    mech = g == top
    names = ["pres", "srcs", "stor", "well", "blk", "bas", "host", "disp", "body", "modl", "mask", "stif"]

    def local(name):
        k = names.index(name)
        return pltpu.make_async_copy(ins[k], s[name], in_sems.at[k])

    def inside(dx, dy, dg=0):
        x, y = gx + dx, gy + dy
        ok = (x >= 0) & (x < nx) & (y >= 0) & (y < ny)
        if dg:
            ok = ok & (g + dg >= 0) & (g + dg < top)
        return ok

    def as_int(flag):
        return flag.astype(I32)

    def remote(src, dst, send, recv, device):
        return pltpu.make_async_remote_copy(
            src_ref=src, dst_ref=dst, send_sem=send_sems.at[send], recv_sem=recv_sems.at[recv],
            device_id=device, device_id_type=MESH,
        )

    def start_if(ok, *args):
        @pl.when(ok)
        def _():
            remote(*args).start()

    def wait_recv_if(ok, dst, recv):
        @pl.when(ok)
        def _():
            remote(dst, dst, 0, recv, (g, gx, gy)).wait_recv()

    def wait_send_if(ok, src, send):
        @pl.when(ok)
        def _():
            remote(src, src, send, 0, (g, gx, gy)).wait_send()

    def greet(ok, device):
        @pl.when(ok)
        def _():
            pl.semaphore_signal(pltpu.get_barrier_semaphore(), inc=1, device_id=device, device_id_type=MESH)

    HALO = [(-1, 0, 0), (1, 0, 0), (0, -1, 0), (0, 1, 0), (0, 0, -1), (0, 0, 1)]

    def halo_refs(p, k, way):
        dx, dy, dg = HALO[way]
        if dx:
            src = p.at[0:16] if dx < 0 else p.at[48:64]
            return src, s["xh"].at[2 * k + (1 if dx < 0 else 0)]
        if dy:
            return s["ys"].at[2 * k + (0 if dy < 0 else 1)], s["yh"].at[2 * k + (1 if dy < 0 else 0)]
        return s["zs"].at[2 * k + (0 if dg < 0 else 1)], s["zh"].at[2 * k + (1 if dg < 0 else 0)]

    def stage_halos(p, k):
        lane = lane_iota()
        low = jnp.zeros((8, 128), F32)
        high = jnp.zeros((8, 128), F32)
        for v in range(8):
            tile = p[8 * v : 8 * v + 8]
            low = jnp.where(lane == v, tile if v == 0 else pltpu.roll(tile, v, 1), low)
            high = jnp.where(lane == v, pltpu.roll(tile, v + 1, 1), high)
        s["zs"][2 * k] = low
        s["zs"][2 * k + 1] = high
        for x in range(4):
            s["ys"][2 * k, x : x + 1] = p[16 * x : 16 * x + 1]
            s["ys"][2 * k + 1, x : x + 1] = p[16 * x + 15 : 16 * x + 16]

    def send_halos(p, k):
        for way, (dx, dy, dg) in enumerate(HALO):
            src, dst = halo_refs(p, k, way)
            sem = 6 * k + way
            start_if(inside(dx, dy, dg), src, dst, SEND_AT["halo"] + sem, RECV_AT["halo"] + sem, (g + dg, gx + dx, gy + dy))

    def wait_halos(p, k):
        for way, (dx, dy, dg) in enumerate(HALO):
            _, dst = halo_refs(p, k, way)
            wait_recv_if(inside(-dx, -dy, -dg), dst, RECV_AT["halo"] + 6 * k + way)

    def around(p, k):
        lane = lane_iota()
        value = p[...]
        xlo, xhi = s["xh"][2 * k], s["xh"][2 * k + 1]
        total = jnp.concatenate([xlo, value[:48]], 0) + jnp.concatenate([value[16:], xhi], 0)
        ylo = jnp.concatenate([jnp.broadcast_to(s["yh"][2 * k, x : x + 1], (16, 128)) for x in range(4)], 0)
        yhi = jnp.concatenate([jnp.broadcast_to(s["yh"][2 * k + 1, x : x + 1], (16, 128)) for x in range(4)], 0)
        row = lax.rem(sub_iota((64, 128)), 16)
        total = total + jnp.where(row == 0, ylo, pltpu.roll(value, 1, 0))
        total = total + jnp.where(row == 15, yhi, pltpu.roll(value, 63, 0))
        zlo, zhi = s["zh"][2 * k], s["zh"][2 * k + 1]
        parts = []
        for v in range(8):
            tile = value[8 * v : 8 * v + 8]
            below = zlo if v == 0 else pltpu.roll(zlo, LANES - v, 1)
            above = pltpu.roll(zhi, LANES - 1 - v, 1)
            parts.append(
                jnp.where(lane == 0, below, pltpu.roll(tile, 1, 1))
                + jnp.where(lane == LANES - 1, above, pltpu.roll(tile, LANES - 1, 1))
            )
        return total + jnp.concatenate(parts, 0)

    def cols(i, width=1024):
        return pl.ds(pl.multiple_of(i * width, width), width)

    def rows8(i):
        return pl.ds(pl.multiple_of(i * 8, 8), 8)

    def flow():
        for name in ("pres", "host", "stor", "well", "srcs", "blk", "bas"):
            local(name).start()
        for name in ("xh", "yh", "zh"):
            s[name][...] = jnp.zeros(SCRATCH[name][0], F32)
        count = I32(1)
        greet(gx >= 0, (top, gx, gy))
        for dx, dy, dg in HALO:
            greet(inside(dx, dy, dg), (g + dg, gx + dx, gy + dy))
            count = count + as_int(inside(dx, dy, dg))
        local("pres").wait()
        stage_halos(s["pres"], 0)
        pl.semaphore_wait(pltpu.get_barrier_semaphore(), count)
        send_halos(s["pres"], 0)

        local("host").wait()
        iota_l = sub_iota((128, 128))
        iota_r = sub_iota((64, 128))

        def hosts(i):
            index = s["host"][rows8(i)]
            lanes, rows = index & 127, index >> 7
            left, right = [], []
            for r in range(8):
                left.append((iota_l == lanes[r : r + 1]).astype(F32).astype(BF16))
                right.append((iota_r == rows[r : r + 1]).astype(F32).astype(BF16))
            s["ol"][:, cols(i)] = jnp.concatenate(left, 1)
            s["oh"][:, cols(i)] = jnp.concatenate(right, 1)

        loop(8, hosts)
        for name in ("stor", "well", "srcs", "blk", "bas"):
            local(name).wait()
        s["diag"][...] = 6.0 + s["stor"][...] + WELL * s["well"][...].astype(F32)

        def blocks(i):
            index = s["blk"][rows8(i)]
            diag = s["diag"][rows8(i)]
            parts, highs, lows = [], [], []
            for r in range(8):
                parts.append((iota_r == index[r : r + 1]).astype(F32).astype(BF16))
                weight = s["bas"][pl.ds(i * 8 + r, 8, stride=64), :]
                s["wt"][i * 8 + r] = weight
                term = weight * weight * diag[r : r + 1]
                high = term.astype(BF16).astype(F32)
                highs.append(jnp.concatenate([high, term - high], 0).astype(BF16))
            s["ob"][:, cols(i)] = jnp.concatenate(parts, 1)
            s["wr"][:, cols(i)] = jnp.concatenate(highs, 1)

        loop(8, blocks)
        wait_recv_if(gx >= 0, s["sti"], RECV_AT["strain"])
        def gather(i):
            index = s["host"][rows8(i)]
            lanes, rows = index & 127, index >> 7
            found = jnp.zeros((8, 128), F32)
            for r in range(64):
                row = jnp.broadcast_to(s["sti"][r : r + 1], (8, 128))
                found = jnp.where(rows == r, jnp.take_along_axis(row, lanes, axis=1), found)
            s["frc"][rows8(i)] = s["srcs"][rows8(i)] - BIOT * found

        loop(8, gather, True)

        def residual(p, k):
            return s["frc"][...] + around(p, k) - s["diag"][...] * p[...]

        wait_halos(s["pres"], 0)
        s["p1"][...] = s["pres"][...] + RELAX * residual(s["pres"], 0) / s["diag"][...]
        stage_halos(s["p1"], 1)
        send_halos(s["p1"], 1)
        norms = dot_nt(s["wr"][...], s["ob"][...])
        s["scale"][...] = 1.0 + norms[0:8] + norms[8:16]
        wait_halos(s["p1"], 1)
        s["p2"][...] = s["p1"][...] + RELAX * residual(s["p1"], 1) / s["diag"][...]
        stage_halos(s["p2"], 2)
        send_halos(s["p2"], 2)
        s["cnt"][...] = dot_nt(s["oh"][...], s["ol"][...])
        start_if(gx >= 0, s["cnt"], s["cr"].at[g], SEND_AT["counts"], RECV_AT["counts"] + g, (top, gx, gy))
        wait_halos(s["p2"], 2)
        s["rem"][...] = residual(s["p2"], 2)

        coarse = jnp.zeros((16, 64), F32)
        for i in range(8):
            rem = s["rem"][8 * i : 8 * i + 8]
            parts = []
            for r in range(8):
                term = s["wt"][8 * i + r] * rem[r : r + 1]
                high = term.astype(BF16).astype(F32)
                parts.append(jnp.concatenate([high, term - high], 0).astype(BF16))
            coarse = coarse + dot_nt(jnp.concatenate(parts, 1), s["ob"][:, 1024 * i : 1024 * i + 1024])
        fixed = (coarse[0:8] + coarse[8:16]) / s["scale"][...]
        table = jnp.concatenate([fixed, fixed], 1)
        both = jnp.zeros((128, 128), F32)
        for i in range(8):
            at = slice(8 * i, 8 * i + 8)
            blocks_of = s["blk"][at]
            parts = []
            for r in range(8):
                back = jnp.take_along_axis(table, jnp.broadcast_to(blocks_of[r : r + 1], (8, 128)), axis=1)
                parts.append(jnp.sum(s["wt"][8 * i + r] * back, axis=0, keepdims=True))
            updated = s["p2"][at] + jnp.concatenate(parts, 0)
            po[at] = updated
            change = updated - s["pres"][at]
            high = change.astype(BF16).astype(F32)
            low = change - high
            tops, lows = [], []
            for r in range(8):
                one = s["oh"][:, 1024 * i + 128 * r : 1024 * i + 128 * r + 128]
                tops.append(one * jnp.broadcast_to(high[r : r + 1], (64, 128)).astype(BF16))
                lows.append(one * jnp.broadcast_to(low[r : r + 1], (64, 128)).astype(BF16))
            scaled = jnp.concatenate([jnp.concatenate(tops, 1), jnp.concatenate(lows, 1)], 0)
            both = both + dot_nt(scaled, s["ol"][:, 1024 * i : 1024 * i + 1024])
        s["sm"][...] = both[0:64] + both[64:128]
        start_if(gx >= 0, s["sm"], s["sr"].at[g], SEND_AT["sums"], RECV_AT["sums"] + g, (top, gx, gy))
        do[...] = jnp.zeros((192, 128), F32)
        for k, p in enumerate((s["pres"], s["p1"], s["p2"])):
            for way, (dx, dy, dg) in enumerate(HALO):
                src, _ = halo_refs(p, k, way)
                wait_send_if(inside(dx, dy, dg), src, SEND_AT["halo"] + 6 * k + way)
        wait_send_if(gx >= 0, s["cnt"], SEND_AT["counts"])
        wait_send_if(gx >= 0, s["sm"], SEND_AT["sums"])

    def x_from(dx, low, high):
        first = low
        if dx == 0:
            return slice(first, first + 4), slice(first, first + 4)
        if dx < 0:
            return slice(first, first + high), slice(first + 4, first + 4 + high)
        return slice(first + 4 - low, first + 4), slice(0, low)

    def node_refs(arr, ylo, yhi, dx, dy):
        xs, xd = x_from(dx, 2, 2)
        if dy == 0:
            return arr.at[xs, 16:80], arr.at[xd, 16:80]
        if dy > 0:
            return arr.at[xs, 64:80], ylo.at[xd]
        return arr.at[xs, 16:32], yhi.at[xd]

    def raw_refs(arr, dx, dy):
        xs, xd = x_from(dx, 3, 2)
        ysrc, ydst = {0: (slice(8, 24), slice(8, 24)), 1: (slice(16, 24), slice(0, 8)), -1: (slice(8, 16), slice(24, 32))}[dy]
        return arr.at[xs, ysrc], arr.at[xd, ydst]

    def exchange_start(refs_of, name):
        for k, (dx, dy) in enumerate(AROUND):
            src, dst = refs_of(dx, dy)
            start_if(inside(dx, dy), src, dst, SEND_AT[name] + k, RECV_AT[name] + k, (g, gx + dx, gy + dy))

    def exchange_wait(refs_of, name):
        for k, (dx, dy) in enumerate(AROUND):
            _, dst = refs_of(dx, dy)
            wait_recv_if(inside(-dx, -dy), dst, RECV_AT[name] + k)

    def exchange_done(refs_of, name):
        for k, (dx, dy) in enumerate(AROUND):
            src, _ = refs_of(dx, dy)
            wait_send_if(inside(dx, dy), src, SEND_AT[name] + k)

    def close_nodes(arr, ylo, yhi):
        half = sub_iota() < 4

        def plane(x):
            for k in range(2):
                own = arr[x, 64 + 8 * k : 72 + 8 * k]
                arr[x, 8 * k : 8 * k + 8] = pltpu.roll(jnp.where(half, own, ylo[x, 8 * k : 8 * k + 8]), 4, 0)
                own = arr[x, 16 + 8 * k : 24 + 8 * k]
                arr[x, 80 + 8 * k : 88 + 8 * k] = pltpu.roll(jnp.where(half, yhi[x, 8 * k : 8 * k + 8], own), 4, 0)

        loop(8, plane)

    def zero_edges(arr, ylo, yhi):
        @pl.when(gx == 0)
        def _():
            arr[0:2] = jnp.zeros((2,) + arr.shape[1:], F32)
            ylo[0:2] = jnp.zeros((2, 16, 128), F32)
            yhi[0:2] = jnp.zeros((2, 16, 128), F32)

        @pl.when(gx == nx - 1)
        def _():
            arr[6:8] = jnp.zeros((2,) + arr.shape[1:], F32)
            ylo[6:8] = jnp.zeros((2, 16, 128), F32)
            yhi[6:8] = jnp.zeros((2, 16, 128), F32)

        @pl.when(gy == 0)
        def _():
            ylo[...] = jnp.zeros((8, 16, 128), F32)

        @pl.when(gy == ny - 1)
        def _():
            yhi[...] = jnp.zeros((8, 16, 128), F32)

    def zero_raw(arr):
        @pl.when(gx == 0)
        def _():
            arr[0:3] = jnp.zeros((3, 32, 128), F32)

        @pl.when(gx == nx - 1)
        def _():
            arr[7:9] = jnp.zeros((2, 32, 128), F32)

        @pl.when(gy == 0)
        def _():
            arr[:, 0:8] = jnp.zeros((9, 8, 128), F32)

        @pl.when(gy == ny - 1)
        def _():
            arr[:, 24:32] = jnp.zeros((9, 8, 128), F32)

    def x_ok(x):
        bad = ((x < 2) & (gx == 0)) | ((x >= 6) & (gx == nx - 1))
        return jnp.where(bad, 0.0, 1.0).astype(F32)

    def y_ok(j):
        sub = sub_iota()
        mask = jnp.where((sub & 3) < 3, 1.0, 0.0)
        if j < 2:
            mask = jnp.where(sub < 4, mask * jnp.where(gy == 0, 0.0, 1.0), mask)
        if j > 9:
            mask = jnp.where(sub >= 4, mask * jnp.where(gy == ny - 1, 0.0, 1.0), mask)
        return mask

    def operate(arr, elem_x, elem_j, use, unroll=True):
        (xa, xb), (ja, jb) = elem_x, elem_j
        ph, plo, vs = s["ph"], s["plo"], s["vs"]
        wide = jb - ja

        def stage(k):
            x = xa + k
            for j in range(ja, jb + 1):
                value = arr[x, 8 * j : 8 * j + 8]
                pair = jnp.concatenate([value, shift_down(value)], 0)
                high, low = split(pair)
                ph[x, 16 * j : 16 * j + 16] = high
                plo[x, 16 * j : 16 * j + 16] = low

        loop(xb - xa + 1, stage, unroll)

        def elements(k):
            x = xa + k
            columns = []
            for j in range(ja, jb):
                at = slice(16 * j, 16 * j + 32)
                first, second = ph[x, at], ph[x + 1, at]
                columns.append(jnp.concatenate([first, second, plo[x, at], plo[x + 1, at], first, second], 0))
            product = dot_nn(s["kl"][...], jnp.concatenate(columns, 1))
            for c in range(wide):
                j = ja + c
                weight = s["wtile"][x, 8 * j : 8 * j + 8]
                vs[x, 64 * j : 64 * j + 64] = product[:, 128 * c : 128 * c + 128] * jnp.concatenate([weight] * 8, 0)

        loop(xb - xa, elements, unroll)

        spring = SPRING * s["kap"][...]

        def nodes(k):
            x = xa + 1 + k
            for j in range(ja + 1, jb):
                total = None
                for a in range(2):
                    for b in range(2):
                        at = 64 * (j - b) + 16 * (2 * a + b)
                        part = vs[x - a, at : at + 16]
                        total = part if total is None else total + part
                node = arr[x, 8 * j : 8 * j + 8]
                use(x, j, node, total[0:8] + shift_up(total[8:16]) + spring * node)

        loop(xb - xa - 1, nodes, unroll)

    def mechanics():
        for name in ("disp", "mask", "modl", "stif", "body"):
            local(name).start()
        greet_count = I32(top)
        for gg in range(top):
            greet(gx >= 0, (gg, gx, gy))
        for dx, dy in AROUND:
            greet(inside(dx, dy), (g, gx + dx, gy + dy))
            greet_count = greet_count + as_int(inside(dx, dy))
        local("disp").wait()
        disp = s["disp"]
        for m in range(3):
            for x in range(4):
                s["uys"][4 * m + x : 4 * m + x + 1] = disp[m, 16 * x : 16 * x + 1]
            s["ucs"][m : m + 1] = disp[m, 0:1]
        pl.semaphore_wait(pltpu.get_barrier_semaphore(), greet_count)

        near = [
            (-1, -1, s["ucs"], s["uc"]),
            (-1, 0, disp.at[:, 0:16], s["ux"]),
            (0, -1, s["uys"], s["uy"]),
        ]
        for k, (dx, dy, src, dst) in enumerate(near):
            start_if(inside(dx, dy), src, dst, SEND_AT["ux"] + k, RECV_AT["ux"] + k, (g, gx + dx, gy + dy))

        rounds, step = [], 1
        while step < nx:
            rounds.append((1, step))
            step *= 2
        step = 1
        while step < ny:
            rounds.append((2, step))
            step *= 2

        def ends(turn):
            axis, step = rounds[turn]
            coord, size = ((gx, nx), (gy, ny))[axis - 1]
            return coord - step >= 0, coord + step < size

        def call_out(turn):
            axis, step = rounds[turn]
            for ok, move in zip(ends(turn), (-step, step)):
                device = (g, gx + move, gy) if axis == 1 else (g, gx, gy + move)

                @pl.when(ok)
                def _():
                    pl.semaphore_signal(known.at[turn], inc=1, device_id=device, device_id_type=MESH)

        def hear(turn):
            back, ahead = ends(turn)
            pl.semaphore_wait(known.at[turn], as_int(back) + as_int(ahead))

        call_out(0)

        @pl.when(gx == nx - 1)
        def _():
            s["ux"][...] = jnp.zeros((3, 16, 128), F32)
            s["uc"][...] = jnp.zeros((8, 128), F32)

        @pl.when(gy == ny - 1)
        def _():
            s["uy"][...] = jnp.zeros((16, 128), F32)
            s["uc"][...] = jnp.zeros((8, 128), F32)

        ue, ce = s["ue"], s["ce"]
        local("modl").wait()
        local("mask").wait()
        local("body").wait()
        zero = jnp.zeros((64, 128), F32)
        for x in range(4):
            ue[x + 2, 16:80] = zero
            s["bt"][x] = zero
            for m in range(3):
                for h in range(2):
                    at = 16 * x + 8 * h
                    ue[x + 2, pl.ds(16 + 4 * h + m, 8, stride=8), :] = disp[m, at : at + 8]
                    at = 64 * m + at
                    s["bt"][x, pl.ds(4 * h + m, 8, stride=8), :] = s["body"][at : at + 8]
            at = 16 * x
            s["mw"][x + 3, 8:24] = s["modl"][at : at + 16] * s["mask"][at : at + 16].astype(F32)
        ue_refs = functools.partial(node_refs, ue, s["uyl"], s["uyh"])
        ce_refs = functools.partial(node_refs, ce, s["cyl"], s["cyh"])
        mw_refs = functools.partial(raw_refs, s["mw"])
        gr_refs = functools.partial(raw_refs, s["gr"])
        exchange_start(ue_refs, "ue")
        exchange_start(mw_refs, "mw")
        zero_edges(ue, s["uyl"], s["uyh"])
        zero_edges(ce, s["cyl"], s["cyh"])
        zero_raw(s["mw"])
        zero_raw(s["gr"])

        for k, (dx, dy, _, dst) in enumerate(near):
            wait_recv_if(inside(-dx, -dy), dst, RECV_AT["ux"] + k)

        row15 = sub_iota((16, 128)) == 15
        before = None
        for x in range(5):
            sums, diffs = [], []
            for m in range(3):
                plane = disp[m, 16 * x : 16 * x + 16] if x < 4 else s["ux"][m]
                beyond = s["uy"][4 * m + x : 4 * m + x + 1] if x < 4 else s["uc"][m : m + 1]
                up = jnp.where(row15, jnp.broadcast_to(beyond, (16, 128)), pltpu.roll(plane, 15, 0))
                sums.append(up + plane)
                diffs.append(up - plane)
            now = (sums[0], diffs[1], sums[2])
            if before is not None:
                plain = (now[0] - before[0]) + (now[1] + before[1])
                third = now[2] + before[2]
                value = (plain - third) + shift_down(plain + third)
                at = 16 * (x - 1)
                s["stro"][at : at + 16] = 0.25 * s["mask"][at : at + 16].astype(F32) * value
            before = now
        for gg in range(top):
            start_if(gx >= 0, s["stro"], s["sti"], SEND_AT["strain"] + gg, RECV_AT["strain"], (gg, gx, gy))

        local("stif").wait()
        stiff = s["stif"][...]
        largest = jnp.max(jnp.max(jnp.abs(stiff), axis=1, keepdims=True), axis=0, keepdims=True)
        s["kap"][...] = jnp.broadcast_to(1.0 / largest, (8, 128))
        high, low = split(stiff / largest)
        line = lax.broadcasted_iota(I32, (64, 24), 0)
        entry = lax.broadcasted_iota(I32, (64, 24), 1)
        pick = jnp.where(((line & 3) < 3) & (3 * (line >> 3) + (line & 3) == entry), 1.0, 0.0).astype(BF16)
        r_half = (lax.broadcasted_iota(I32, (64, 64), 0) >> 2) & 1
        c_half = (lax.broadcasted_iota(I32, (64, 64), 1) >> 2) & 1
        wide = []
        for part in (high, low):
            rows = dot_nn(pick, part).astype(BF16)
            wide.append(jnp.where(r_half == c_half, dot_nt(rows, pick), 0.0).astype(BF16))
        s["kl"][...] = jnp.concatenate([wide[0], wide[0], wide[1]], 1)

        hear(0)
        call_out(1)
        exchange_wait(mw_refs, "mw")
        half = sub_iota() < 4

        def pair_of_rows(arr, x, low):
            return jnp.where(
                half,
                jnp.broadcast_to(arr[x, low : low + 1], (8, 128)),
                jnp.broadcast_to(arr[x, low + 8 : low + 9], (8, 128)),
            )

        def weights(x):
            for j in range(11):
                s["wtile"][x, 8 * j : 8 * j + 8] = pair_of_rows(s["mw"], x + 1, 6 + j)

        loop(7, weights)
        exchange_wait(ue_refs, "ue")
        close_nodes(ue, s["uyl"], s["uyh"])
        kappa = jnp.broadcast_to(largest, (8, 128))

        def initial(x, j, node, product):
            ce[x, 8 * j : 8 * j + 8] = s["bt"][x - 2, 8 * (j - 2) : 8 * (j - 2) + 8] - kappa * product

        operate(ue, (1, 6), (1, 10), initial)
        exchange_start(ce_refs, "ce")
        for turn in range(1, len(rounds)):
            hear(turn)
            if turn + 1 < len(rounds):
                call_out(turn + 1)
        exchange_wait(ce_refs, "ce")
        close_nodes(ce, s["cyl"], s["cyh"])

        for gg in range(top):
            wait_recv_if(gx >= 0, s["cr"].at[gg], RECV_AT["counts"] + gg)
        counts = s["cr"][0]
        for gg in range(1, top):
            counts = counts + s["cr"][gg]
        s["fac"][...] = (0.25 * BIOT) * s["mask"][...].astype(F32) / jnp.maximum(counts, 1.0)
        po[...] = jnp.zeros((64, 128), F32)

        for gg in range(top):
            wait_recv_if(gx >= 0, s["sr"].at[gg], RECV_AT["sums"] + gg)
        sums = s["sr"][0]
        for gg in range(1, top):
            sums = sums + s["sr"][gg]
        value = s["fac"][...] * sums
        for x in range(4):
            s["gr"][x + 3, 8:24] = value[16 * x : 16 * x + 16]
        exchange_start(gr_refs, "gr")
        exchange_wait(gr_refs, "gr")

        def tiles(x):
            for j in range(13):
                s["gt"][x, 8 * j : 8 * j + 8] = pair_of_rows(s["gr"], x, 5 + j)

        loop(9, tiles, True)
        part = sub_iota() & 3
        signs = [jnp.where(part == m, -1.0, 1.0).astype(F32) for m in range(3)]
        rx, qe = s["rx"], s["qe"]

        def force(x):
            okay = x_ok(x)
            last = None
            for j in range(13):
                at = slice(8 * j, 8 * j + 8)
                along_x = s["gt"][x, at] + signs[0] * s["gt"][x + 1, at]
                if last is not None:
                    both = last + signs[1] * along_x
                    node = shift_up(both) + signs[2] * both
                    k = j - 1
                    at = slice(8 * k, 8 * k + 8)
                    rx[x, at] = (ce[x, at] + node) * (y_ok(k) * okay)
                last = along_x

        loop(8, force, True)

        def first(x, j, node, product):
            qe[x, 8 * j : 8 * j + 8] = product * (y_ok(j) * x_ok(x))

        operate(rx, (0, 7), (0, 11), first)
        acc = s["dots"]
        acc[...] = jnp.zeros((8, 128), F32)

        def second(x, j, node, product):
            r = rx[x, 8 * j : 8 * j + 8]
            terms = [r * r, r * node, node * node, node * product]
            rows = [jnp.sum(term, axis=0, keepdims=True) for term in terms]
            acc[0:4] += jnp.concatenate(rows, 0)

        operate(qe, (1, 6), (1, 10), second)
        total = jnp.broadcast_to(jnp.sum(acc[...], axis=1, keepdims=True), (8, 128))
        s["row"][...] = jnp.sum(jnp.where(lane_iota() == sub_iota(), total, 0.0), axis=0, keepdims=True)
        others = [(dx, dy) for dx in range(nx) for dy in range(ny) if (dx, dy) != (0, 0)]
        others.sort(key=lambda d: -(min(d[0], nx - d[0]) + 2 * min(d[1], ny - d[1])))
        for dx, dy in others:
            device = (g, lax.rem(gx + dx, nx), lax.rem(gy + dy, ny))
            start_if(gx >= 0, s["row"], s["ar"].at[dx * ny + dy], SEND_AT["ar"], RECV_AT["ar"], device)

        def to_rows(arr, out):
            for x in range(4):
                for m in range(3):
                    for h in range(2):
                        at = 64 * m + 16 * x + 8 * h
                        out[at : at + 8] = arr[x + 2, pl.ds(16 + 4 * h + m, 8, stride=8), :]

        to_rows(rx, s["rr"])
        to_rows(qe, s["qr"])
        wait_recv_if(gx >= 0, s["ar"].at[1 : nx * ny], RECV_AT["ar"])
        total = s["row"][...] + jnp.sum(s["ar"][1 : nx * ny], axis=0)
        lane = lane_iota((1, 128))
        aa, bb, cc, ee = [
            jnp.broadcast_to(jnp.sum(jnp.where(lane == k, total, 0.0), axis=1, keepdims=True), (8, 128)) for k in range(4)
        ]
        step0 = aa / bb
        new = step0 * step0 * cc - aa
        along = bb - 2.0 * step0 * cc + step0 * step0 * ee
        ratio = new / aa
        step1 = new / (along - ratio * new / step0)
        inverse = s["kap"][...]
        alpha = (step0 + step1 * (1.0 + ratio)) * inverse
        gamma = step1 * step0 * inverse
        for k in range(24):
            at = 8 * k
            m, r = divmod(at, 64)
            do[at : at + 8] = disp[m, r : r + 8] + alpha * s["rr"][at : at + 8] - gamma * s["qr"][at : at + 8]

        for k, (dx, dy, src, _) in enumerate(near):
            wait_send_if(inside(dx, dy), src, SEND_AT["ux"] + k)
        for gg in range(top):
            wait_send_if(gx >= 0, s["stro"], SEND_AT["strain"] + gg)
        for refs_of, name in ((ue_refs, "ue"), (mw_refs, "mw"), (ce_refs, "ce"), (gr_refs, "gr")):
            exchange_done(refs_of, name)
        wait_send_if(gx >= 0, s["ar"].at[1 : nx * ny], SEND_AT["ar"])

    pl.when(jnp.logical_not(mech))(flow)
    pl.when(mech)(mechanics)


def hand_over(p_ref, d_ref, p_out, d_out, sems):
    copies = [pltpu.make_async_copy(p_ref, p_out, sems.at[0]), pltpu.make_async_copy(d_ref, d_out, sems.at[1])]
    for copy in copies:
        copy.start()
    for copy in copies:
        copy.wait()


def local(sizes, *arrays):
    shapes = [(64, 128)] * 5 + [(512, 128), (64, 128), (3, 64, 128), (192, 128), (64, 128), (64, 128), (24, 24)]
    flat = [array.reshape(shape) for array, shape in zip(arrays, shapes)]
    scratch = [pltpu.VMEM(shape, dtype) for shape, dtype in SCRATCH.values()]
    scratch += [
        pltpu.SemaphoreType.DMA((12,)),
        pltpu.SemaphoreType.DMA((N_SEND,)),
        pltpu.SemaphoreType.DMA((N_RECV,)),
        pltpu.SemaphoreType.REGULAR((8,)),
    ]
    pressure, displacement = pl.pallas_call(
        functools.partial(kernel, sizes),
        out_shape=(pltpu.VMEM((64, 128), F32), pltpu.VMEM((192, 128), F32)),
        in_specs=[pl.BlockSpec(memory_space=pl.ANY)] * 12,
        out_specs=(pl.BlockSpec(memory_space=pltpu.VMEM),) * 2,
        scratch_shapes=scratch,
        compiler_params=pltpu.CompilerParams(collective_id=0, has_side_effects=True),
    )(*flat)
    pressure, displacement = pl.pallas_call(
        hand_over,
        out_shape=(jax.ShapeDtypeStruct((64, 128), F32), jax.ShapeDtypeStruct((192, 128), F32)),
        in_specs=[pl.BlockSpec(memory_space=pltpu.VMEM)] * 2,
        out_specs=(pl.BlockSpec(memory_space=pl.ANY),) * 2,
        scratch_shapes=[pltpu.SemaphoreType.DMA((2,))],
    )(pltpu.with_memory_space_constraint(pressure, pltpu.VMEM), pltpu.with_memory_space_constraint(displacement, pltpu.VMEM))
    return pressure.reshape(arrays[0].shape), displacement.reshape(arrays[7].shape)


def solution(mesh):
    cell = P("grp", "gx", "gy", None)
    many = P("grp", None, "gx", "gy", None)
    sizes = (mesh.shape["grp"], mesh.shape["gx"], mesh.shape["gy"])
    return jax.shard_map(
        functools.partial(local, sizes),
        mesh=mesh,
        in_specs=(cell,) * 5 + (many, cell, many, many, cell, cell, P()),
        out_specs=(cell, many),
        check_vma=False,
    )
```

```python
import functools

import jax
import jax.numpy as jnp
from jax import lax
from jax.experimental import pallas as pl
from jax.experimental.pallas import tpu as pltpu
from jax.sharding import PartitionSpec as P

F32 = jnp.float32
BF16 = jnp.bfloat16
I32 = jnp.int32
MESH = pl.DeviceIdType.MESH
NBLK = 64
LANES = 128
ROWS = 64
BIOT = 1.5
RELAX = 0.8
SPRING = 0.5
WELL = 4.0
AROUND = [(-1, -1), (-1, 1), (1, -1), (1, 1), (-1, 0), (1, 0), (0, -1), (0, 1)]

SEND = dict(ux=3, strain=6, ue=8, ce=8, mw=8, gr=8, sums=1, counts=1, halo=18, ar=1)
RECV = dict(ux=3, strain=2, ue=8, ce=8, mw=8, gr=8, sums=3, counts=3, halo=18, ar=1)


def offsets(table):
    at, out = 0, {}
    for name, count in table.items():
        out[name] = at
        at += count
    return out, at


SEND_AT, N_SEND = offsets(SEND)
RECV_AT, N_RECV = offsets(RECV)

SCRATCH = dict(
    pres=((64, 128), F32), srcs=((64, 128), F32), stor=((64, 128), F32), well=((64, 128), I32),
    blk=((64, 128), I32), bas=((512, 128), F32), host=((64, 128), I32),
    disp=((3, 64, 128), F32), body=((192, 128), F32), modl=((64, 128), F32), mask=((64, 128), I32),
    stif=((24, 24), F32),
    p1=((64, 128), F32), p2=((64, 128), F32), diag=((64, 128), F32), frc=((64, 128), F32),
    xh=((6, 16, 128), F32), yh=((6, 8, 128), F32), zh=((6, 8, 128), F32),
    ys=((6, 8, 128), F32), zs=((6, 8, 128), F32),
    sti=((64, 128), F32), ol=((128, 8192), BF16), oh=((64, 8192), BF16), ob=((64, 8192), BF16),
    wt=((64, 8, 128), F32), wr=((16, 8192), BF16), scale=((8, 64), F32),
    chg=((64, 128), F32), lo=((64, 128), F32),
    cnt=((64, 128), F32), sm=((64, 128), F32), rem=((64, 128), F32),
    ux=((3, 16, 128), F32), uy=((16, 128), F32), uc=((8, 128), F32),
    uys=((16, 128), F32), ucs=((8, 128), F32), stro=((64, 128), F32),
    ue=((8, 96, 128), F32), uyl=((8, 16, 128), F32), uyh=((8, 16, 128), F32),
    ce=((8, 96, 128), F32), cyl=((8, 16, 128), F32), cyh=((8, 16, 128), F32),
    mw=((9, 32, 128), F32), gr=((9, 32, 128), F32), wtile=((7, 88, 128), F32),
    sr=((3, 64, 128), F32), cr=((3, 64, 128), F32), fac=((64, 128), F32),
    gt=((9, 104, 128), F32), rx=((8, 96, 128), F32), qe=((8, 96, 128), F32),
    ph=((8, 192, 128), BF16), plo=((8, 192, 128), BF16), vs=((7, 704, 128), F32),
    kl=((64, 192), BF16), pf=((8, 192, 128), F32), gys=((2, 8, 128), F32), gyr=((6, 8, 128), F32), kap=((8, 128), F32), bt=((4, 64, 128), F32),
    rr=((192, 128), F32), qr=((192, 128), F32), dots=((8, 128), F32),
    ar=((64, 1, 128), F32), row=((1, 128), F32),
)


def split(value):
    high = value.astype(BF16)
    return high, (value - high.astype(F32)).astype(BF16)


def dot_nt(a, b):
    return lax.dot_general(a, b, (((1,), (1,)), ((), ())), preferred_element_type=F32)


def dot_nn(a, b):
    return jnp.dot(a, b, preferred_element_type=F32)


def lane_iota(shape=(8, 128)):
    return lax.broadcasted_iota(I32, shape, len(shape) - 1)


def sub_iota(shape=(8, 128)):
    return lax.broadcasted_iota(I32, shape, len(shape) - 2)


def shift_down(value):
    return jnp.where(lane_iota(value.shape) == LANES - 1, 0.0, pltpu.roll(value, LANES - 1, 1))


def shift_up(value):
    return jnp.where(lane_iota(value.shape) == 0, 0.0, pltpu.roll(value, 1, 1))


def loop(count, body, unroll=1):
    def step(i, carry):
        body(i)
        return carry

    lax.fori_loop(0, count, step, 0, unroll=unroll)


def kernel(sizes, *refs):
    groups, nx, ny = sizes
    ins, (po, do), rest = refs[:12], refs[12:14], refs[14:]
    s = dict(zip(SCRATCH, rest))
    in_sems, send_sems, recv_sems, known = rest[len(SCRATCH):]
    g, gx, gy = lax.axis_index("grp"), lax.axis_index("gx"), lax.axis_index("gy")
    top = groups - 1
    mech = g == top
    names = ["pres", "srcs", "stor", "well", "blk", "bas", "host", "disp", "body", "modl", "mask", "stif"]

    def local(name):
        k = names.index(name)
        return pltpu.make_async_copy(ins[k], s[name], in_sems.at[k])

    def inside(dx, dy, dg=0):
        x, y = gx + dx, gy + dy
        ok = (x >= 0) & (x < nx) & (y >= 0) & (y < ny)
        if dg:
            ok = ok & (g + dg >= 0) & (g + dg < top)
        return ok

    def as_int(flag):
        return flag.astype(I32)

    def remote(src, dst, send, recv, device):
        return pltpu.make_async_remote_copy(
            src_ref=src, dst_ref=dst, send_sem=send_sems.at[send], recv_sem=recv_sems.at[recv],
            device_id=device, device_id_type=MESH,
        )

    def start_if(ok, *args):
        @pl.when(ok)
        def _():
            remote(*args).start()

    def wait_recv_if(ok, dst, recv):
        @pl.when(ok)
        def _():
            remote(dst, dst, 0, recv, (g, gx, gy)).wait_recv()

    def wait_send_if(ok, src, send):
        @pl.when(ok)
        def _():
            remote(src, src, send, 0, (g, gx, gy)).wait_send()

    def greet(ok, device):
        @pl.when(ok)
        def _():
            pl.semaphore_signal(pltpu.get_barrier_semaphore(), inc=1, device_id=device, device_id_type=MESH)

    HALO = [(-1, 0, 0), (1, 0, 0), (0, -1, 0), (0, 1, 0), (0, 0, -1), (0, 0, 1)]

    def halo_refs(p, k, way):
        dx, dy, dg = HALO[way]
        if dx:
            src = p.at[0:16] if dx < 0 else p.at[48:64]
            return src, s["xh"].at[2 * k + (1 if dx < 0 else 0)]
        if dy:
            return s["ys"].at[2 * k + (0 if dy < 0 else 1)], s["yh"].at[2 * k + (1 if dy < 0 else 0)]
        return s["zs"].at[2 * k + (0 if dg < 0 else 1)], s["zh"].at[2 * k + (1 if dg < 0 else 0)]

    def stage_halos(p, k):
        lane = lane_iota()
        low = jnp.zeros((8, 128), F32)
        high = jnp.zeros((8, 128), F32)
        for v in range(8):
            tile = p[8 * v : 8 * v + 8]
            low = jnp.where(lane == v, tile if v == 0 else pltpu.roll(tile, v, 1), low)
            high = jnp.where(lane == v, pltpu.roll(tile, v + 1, 1), high)
        s["zs"][2 * k] = low
        s["zs"][2 * k + 1] = high
        for x in range(4):
            s["ys"][2 * k, x : x + 1] = p[16 * x : 16 * x + 1]
            s["ys"][2 * k + 1, x : x + 1] = p[16 * x + 15 : 16 * x + 16]

    def send_halos(p, k):
        for way, (dx, dy, dg) in enumerate(HALO):
            src, dst = halo_refs(p, k, way)
            sem = 6 * k + way
            start_if(inside(dx, dy, dg), src, dst, SEND_AT["halo"] + sem, RECV_AT["halo"] + sem, (g + dg, gx + dx, gy + dy))

    def wait_halos(p, k):
        for way, (dx, dy, dg) in enumerate(HALO):
            _, dst = halo_refs(p, k, way)
            wait_recv_if(inside(-dx, -dy, -dg), dst, RECV_AT["halo"] + 6 * k + way)

    def around(p, k):
        lane = lane_iota()
        value = p[...]
        xlo, xhi = s["xh"][2 * k], s["xh"][2 * k + 1]
        total = jnp.concatenate([xlo, value[:48]], 0) + jnp.concatenate([value[16:], xhi], 0)
        ylo = jnp.concatenate([jnp.broadcast_to(s["yh"][2 * k, x : x + 1], (16, 128)) for x in range(4)], 0)
        yhi = jnp.concatenate([jnp.broadcast_to(s["yh"][2 * k + 1, x : x + 1], (16, 128)) for x in range(4)], 0)
        row = lax.rem(sub_iota((64, 128)), 16)
        total = total + jnp.where(row == 0, ylo, pltpu.roll(value, 1, 0))
        total = total + jnp.where(row == 15, yhi, pltpu.roll(value, 63, 0))
        zlo, zhi = s["zh"][2 * k], s["zh"][2 * k + 1]
        parts = []
        for v in range(8):
            tile = value[8 * v : 8 * v + 8]
            below = zlo if v == 0 else pltpu.roll(zlo, LANES - v, 1)
            above = pltpu.roll(zhi, LANES - 1 - v, 1)
            parts.append(
                jnp.where(lane == 0, below, pltpu.roll(tile, 1, 1))
                + jnp.where(lane == LANES - 1, above, pltpu.roll(tile, LANES - 1, 1))
            )
        return total + jnp.concatenate(parts, 0)

    def cols(i, width=1024):
        return pl.ds(pl.multiple_of(i * width, width), width)

    def rows8(i):
        return pl.ds(pl.multiple_of(i * 8, 8), 8)

    def flow():
        for name in ("pres", "host", "stor", "well", "srcs", "blk", "bas"):
            local(name).start()
        for name in ("xh", "yh", "zh"):
            s[name][...] = jnp.zeros(SCRATCH[name][0], F32)
        count = I32(1)
        greet(gx >= 0, (top, gx, gy))
        for dx, dy, dg in HALO:
            greet(inside(dx, dy, dg), (g + dg, gx + dx, gy + dy))
            count = count + as_int(inside(dx, dy, dg))
        local("pres").wait()
        stage_halos(s["pres"], 0)
        pl.semaphore_wait(pltpu.get_barrier_semaphore(), count)
        send_halos(s["pres"], 0)

        local("host").wait()
        iota_l = sub_iota((128, 128))
        iota_r = sub_iota((64, 128))

        def hosts(i):
            index = s["host"][rows8(i)]
            lanes, rows = index & 127, index >> 7
            left, right = [], []
            for r in range(8):
                left.append((iota_l == lanes[r : r + 1]).astype(F32).astype(BF16))
                right.append((iota_r == rows[r : r + 1]).astype(F32).astype(BF16))
            s["ol"][:, cols(i)] = jnp.concatenate(left, 1)
            s["oh"][:, cols(i)] = jnp.concatenate(right, 1)

        loop(8, hosts)
        for name in ("stor", "well", "srcs", "blk", "bas"):
            local(name).wait()
        s["diag"][...] = 6.0 + s["stor"][...] + WELL * s["well"][...].astype(F32)

        def blocks(i):
            index = s["blk"][rows8(i)]
            diag = s["diag"][rows8(i)]
            parts, highs, lows = [], [], []
            for r in range(8):
                parts.append((iota_r == index[r : r + 1]).astype(F32).astype(BF16))
                weight = s["bas"][pl.ds(i * 8 + r, 8, stride=64), :]
                s["wt"][i * 8 + r] = weight
                term = weight * weight * diag[r : r + 1]
                high = term.astype(BF16).astype(F32)
                highs.append(jnp.concatenate([high, term - high], 0).astype(BF16))
            s["ob"][:, cols(i)] = jnp.concatenate(parts, 1)
            s["wr"][:, cols(i)] = jnp.concatenate(highs, 1)

        loop(8, blocks)
        for half in range(2):
            wait_recv_if(gx >= 0, s["sti"].at[32 * half : 32 * half + 32], RECV_AT["strain"] + half)
            for i in range(8):
                at = slice(8 * i, 8 * i + 8)
                index = s["host"][at]
                lanes, rows = index & 127, index >> 7
                found = s["frc"][at] if half else jnp.zeros((8, 128), F32)
                for r in range(32 * half, 32 * half + 32):
                    row = jnp.broadcast_to(s["sti"][r : r + 1], (8, 128))
                    found = jnp.where(rows == r, jnp.take_along_axis(row, lanes, axis=1), found)
                s["frc"][at] = s["srcs"][at] - BIOT * found if half else found

        def residual(p, k):
            return s["frc"][...] + around(p, k) - s["diag"][...] * p[...]

        wait_halos(s["pres"], 0)
        s["p1"][...] = s["pres"][...] + RELAX * residual(s["pres"], 0) / s["diag"][...]
        stage_halos(s["p1"], 1)
        send_halos(s["p1"], 1)
        norms = dot_nt(s["wr"][...], s["ob"][...])
        s["scale"][...] = 1.0 + norms[0:8] + norms[8:16]
        wait_halos(s["p1"], 1)
        s["p2"][...] = s["p1"][...] + RELAX * residual(s["p1"], 1) / s["diag"][...]
        stage_halos(s["p2"], 2)
        send_halos(s["p2"], 2)
        s["cnt"][...] = dot_nt(s["oh"][...], s["ol"][...])
        start_if(gx >= 0, s["cnt"], s["cr"].at[g], SEND_AT["counts"], RECV_AT["counts"] + g, (top, gx, gy))
        wait_halos(s["p2"], 2)
        s["rem"][...] = residual(s["p2"], 2)

        coarse = jnp.zeros((16, 64), F32)
        for i in range(8):
            rem = s["rem"][8 * i : 8 * i + 8]
            parts = []
            for r in range(8):
                term = s["wt"][8 * i + r] * rem[r : r + 1]
                high = term.astype(BF16).astype(F32)
                parts.append(jnp.concatenate([high, term - high], 0).astype(BF16))
            coarse = coarse + dot_nt(jnp.concatenate(parts, 1), s["ob"][:, 1024 * i : 1024 * i + 1024])
        fixed = (coarse[0:8] + coarse[8:16]) / s["scale"][...]
        table = jnp.concatenate([fixed, fixed], 1)
        both = jnp.zeros((128, 128), F32)
        for i in range(8):
            at = slice(8 * i, 8 * i + 8)
            blocks_of = s["blk"][at]
            parts = []
            for r in range(8):
                back = jnp.take_along_axis(table, jnp.broadcast_to(blocks_of[r : r + 1], (8, 128)), axis=1)
                parts.append(jnp.sum(s["wt"][8 * i + r] * back, axis=0, keepdims=True))
            updated = s["p2"][at] + jnp.concatenate(parts, 0)
            po[at] = updated
            change = updated - s["pres"][at]
            high = change.astype(BF16).astype(F32)
            low = change - high
            tops, lows = [], []
            for r in range(8):
                one = s["oh"][:, 1024 * i + 128 * r : 1024 * i + 128 * r + 128]
                tops.append(one * jnp.broadcast_to(high[r : r + 1], (64, 128)).astype(BF16))
                lows.append(one * jnp.broadcast_to(low[r : r + 1], (64, 128)).astype(BF16))
            scaled = jnp.concatenate([jnp.concatenate(tops, 1), jnp.concatenate(lows, 1)], 0)
            both = both + dot_nt(scaled, s["ol"][:, 1024 * i : 1024 * i + 1024])
        s["sm"][...] = both[0:64] + both[64:128]
        start_if(gx >= 0, s["sm"], s["sr"].at[g], SEND_AT["sums"], RECV_AT["sums"] + g, (top, gx, gy))
        do[...] = jnp.zeros((192, 128), F32)
        for k, p in enumerate((s["pres"], s["p1"], s["p2"])):
            for way, (dx, dy, dg) in enumerate(HALO):
                src, _ = halo_refs(p, k, way)
                wait_send_if(inside(dx, dy, dg), src, SEND_AT["halo"] + 6 * k + way)
        wait_send_if(gx >= 0, s["cnt"], SEND_AT["counts"])
        wait_send_if(gx >= 0, s["sm"], SEND_AT["sums"])

    def x_from(dx, low, high):
        first = low
        if dx == 0:
            return slice(first, first + 4), slice(first, first + 4)
        if dx < 0:
            return slice(first, first + high), slice(first + 4, first + 4 + high)
        return slice(first + 4 - low, first + 4), slice(0, low)

    def node_refs(arr, ylo, yhi, dx, dy):
        xs, xd = x_from(dx, 2, 2)
        if dy == 0:
            return arr.at[xs, 16:80], arr.at[xd, 16:80]
        if dy > 0:
            return arr.at[xs, 64:80], ylo.at[xd]
        return arr.at[xs, 16:32], yhi.at[xd]

    def raw_refs(arr, dx, dy):
        xs, xd = x_from(dx, 3, 2)
        ysrc, ydst = {0: (slice(8, 24), slice(8, 24)), 1: (slice(16, 24), slice(0, 8)), -1: (slice(8, 16), slice(24, 32))}[dy]
        return arr.at[xs, ysrc], arr.at[xd, ydst]

    def pressure_refs(dx, dy):
        if dy:
            return s["gys"].at[0 if dy < 0 else 1], s["gyr"].at[(3 if dy < 0 else 0) + dx + 1]
        src, dst = (slice(3, 5), slice(7, 9)) if dx < 0 else (slice(5, 7), slice(1, 3))
        return s["gr"].at[src, 8:24], s["gr"].at[dst, 8:24]

    def exchange_start(refs_of, name):
        for k, (dx, dy) in enumerate(AROUND):
            src, dst = refs_of(dx, dy)
            start_if(inside(dx, dy), src, dst, SEND_AT[name] + k, RECV_AT[name] + k, (g, gx + dx, gy + dy))

    def exchange_wait(refs_of, name):
        for k, (dx, dy) in enumerate(AROUND):
            _, dst = refs_of(dx, dy)
            wait_recv_if(inside(-dx, -dy), dst, RECV_AT[name] + k)

    def exchange_done(refs_of, name):
        for k, (dx, dy) in enumerate(AROUND):
            src, _ = refs_of(dx, dy)
            wait_send_if(inside(dx, dy), src, SEND_AT[name] + k)

    def close_nodes(arr, ylo, yhi):
        half = sub_iota() < 4

        def plane(x):
            for k in range(2):
                own = arr[x, 64 + 8 * k : 72 + 8 * k]
                arr[x, 8 * k : 8 * k + 8] = pltpu.roll(jnp.where(half, own, ylo[x, 8 * k : 8 * k + 8]), 4, 0)
                own = arr[x, 16 + 8 * k : 24 + 8 * k]
                arr[x, 80 + 8 * k : 88 + 8 * k] = pltpu.roll(jnp.where(half, yhi[x, 8 * k : 8 * k + 8], own), 4, 0)

        loop(8, plane)

    def zero_edges(arr, ylo, yhi):
        @pl.when(gx == 0)
        def _():
            arr[0:2] = jnp.zeros((2,) + arr.shape[1:], F32)
            ylo[0:2] = jnp.zeros((2, 16, 128), F32)
            yhi[0:2] = jnp.zeros((2, 16, 128), F32)

        @pl.when(gx == nx - 1)
        def _():
            arr[6:8] = jnp.zeros((2,) + arr.shape[1:], F32)
            ylo[6:8] = jnp.zeros((2, 16, 128), F32)
            yhi[6:8] = jnp.zeros((2, 16, 128), F32)

        @pl.when(gy == 0)
        def _():
            ylo[...] = jnp.zeros((8, 16, 128), F32)

        @pl.when(gy == ny - 1)
        def _():
            yhi[...] = jnp.zeros((8, 16, 128), F32)

    def zero_raw(arr):
        @pl.when(gx == 0)
        def _():
            arr[0:3] = jnp.zeros((3, 32, 128), F32)

        @pl.when(gx == nx - 1)
        def _():
            arr[7:9] = jnp.zeros((2, 32, 128), F32)

        @pl.when(gy == 0)
        def _():
            arr[:, 0:8] = jnp.zeros((9, 8, 128), F32)

        @pl.when(gy == ny - 1)
        def _():
            arr[:, 24:32] = jnp.zeros((9, 8, 128), F32)

    def x_ok(x):
        bad = ((x < 2) & (gx == 0)) | ((x >= 6) & (gx == nx - 1))
        return jnp.where(bad, 0.0, 1.0).astype(F32)

    def y_ok(j):
        sub = sub_iota()
        mask = jnp.where((sub & 3) < 3, 1.0, 0.0)
        if j < 2:
            mask = jnp.where(sub < 4, mask * jnp.where(gy == 0, 0.0, 1.0), mask)
        if j > 9:
            mask = jnp.where(sub >= 4, mask * jnp.where(gy == ny - 1, 0.0, 1.0), mask)
        return mask

    def stage_nodes(arr, elem_x, elem_j, keep):
        for x in range(elem_x[0], elem_x[1] + 1):
            for j in range(elem_j[0], elem_j[1] + 1):
                value = arr[x, 8 * j : 8 * j + 8]
                pair = jnp.concatenate([value, shift_down(value)], 0)
                if keep:
                    s["pf"][x, 16 * j : 16 * j + 16] = pair
                high, low = split(pair)
                s["ph"][x, 16 * j : 16 * j + 16] = high
                s["plo"][x, 16 * j : 16 * j + 16] = low

    def element_product(x, elem_j):
        columns = []
        for j in range(*elem_j):
            at = slice(16 * j, 16 * j + 32)
            first, second = s["ph"][x, at], s["ph"][x + 1, at]
            columns.append(jnp.concatenate([first, second, s["plo"][x, at], s["plo"][x + 1, at], first, second], 0))
        return dot_nn(s["kl"][...], jnp.concatenate(columns, 1))

    def operate(arr, elem_x, elem_j, use):
        (xa, xb), (ja, jb) = elem_x, elem_j
        vs = s["vs"]
        stage_nodes(arr, elem_x, elem_j, False)
        for x in range(xa, xb):
            product = element_product(x, elem_j)
            for c in range(jb - ja):
                j = ja + c
                weight = s["wtile"][x, 8 * j : 8 * j + 8]
                vs[x, 64 * j : 64 * j + 64] = product[:, 128 * c : 128 * c + 128] * jnp.concatenate([weight] * 8, 0)

        spring = SPRING * s["kap"][...]

        def nodes(k):
            x = xa + 1 + k
            for j in range(ja + 1, jb):
                total = None
                for a in range(2):
                    for b in range(2):
                        at = 64 * (j - b) + 16 * (2 * a + b)
                        part = vs[x - a, at : at + 16]
                        total = part if total is None else total + part
                node = arr[x, 8 * j : 8 * j + 8]
                use(x, j, node, total[0:8] + shift_up(total[8:16]) + spring * node)

        loop(xb - xa - 1, nodes, True)

    def mechanics():
        for name in ("disp", "mask", "modl", "stif", "body"):
            local(name).start()
        s["gyr"][...] = jnp.zeros((6, 8, 128), F32)
        greet_count = I32(top)
        for gg in range(top):
            greet(gx >= 0, (gg, gx, gy))
        for dx, dy in AROUND:
            greet(inside(dx, dy), (g, gx + dx, gy + dy))
            greet_count = greet_count + as_int(inside(dx, dy))
        local("disp").wait()
        disp = s["disp"]
        for m in range(3):
            for x in range(4):
                s["uys"][4 * m + x : 4 * m + x + 1] = disp[m, 16 * x : 16 * x + 1]
            s["ucs"][m : m + 1] = disp[m, 0:1]
        pl.semaphore_wait(pltpu.get_barrier_semaphore(), greet_count)

        near = [
            (-1, -1, s["ucs"], s["uc"]),
            (-1, 0, disp.at[:, 0:16], s["ux"]),
            (0, -1, s["uys"], s["uy"]),
        ]
        for k, (dx, dy, src, dst) in enumerate(near):
            start_if(inside(dx, dy), src, dst, SEND_AT["ux"] + k, RECV_AT["ux"] + k, (g, gx + dx, gy + dy))

        rounds, step = [], 1
        while step < nx:
            rounds.append((1, step))
            step *= 2
        step = 1
        while step < ny:
            rounds.append((2, step))
            step *= 2

        def ends(turn):
            axis, step = rounds[turn]
            coord, size = ((gx, nx), (gy, ny))[axis - 1]
            return coord - step >= 0, coord + step < size

        def call_out(turn):
            axis, step = rounds[turn]
            for ok, move in zip(ends(turn), (-step, step)):
                device = (g, gx + move, gy) if axis == 1 else (g, gx, gy + move)

                @pl.when(ok)
                def _():
                    pl.semaphore_signal(known.at[turn], inc=1, device_id=device, device_id_type=MESH)

        def hear(turn):
            back, ahead = ends(turn)
            pl.semaphore_wait(known.at[turn], as_int(back) + as_int(ahead))

        call_out(0)

        @pl.when(gx == nx - 1)
        def _():
            s["ux"][...] = jnp.zeros((3, 16, 128), F32)
            s["uc"][...] = jnp.zeros((8, 128), F32)

        @pl.when(gy == ny - 1)
        def _():
            s["uy"][...] = jnp.zeros((16, 128), F32)
            s["uc"][...] = jnp.zeros((8, 128), F32)

        ue, ce = s["ue"], s["ce"]
        local("modl").wait()
        local("mask").wait()
        local("body").wait()
        zero = jnp.zeros((64, 128), F32)
        for x in range(4):
            ue[x + 2, 16:80] = zero
            s["bt"][x] = zero
            for m in range(3):
                for h in range(2):
                    at = 16 * x + 8 * h
                    ue[x + 2, pl.ds(16 + 4 * h + m, 8, stride=8), :] = disp[m, at : at + 8]
                    at = 64 * m + at
                    s["bt"][x, pl.ds(4 * h + m, 8, stride=8), :] = s["body"][at : at + 8]
            at = 16 * x
            s["mw"][x + 3, 8:24] = s["modl"][at : at + 16] * s["mask"][at : at + 16].astype(F32)
        ue_refs = functools.partial(node_refs, ue, s["uyl"], s["uyh"])
        ce_refs = functools.partial(node_refs, ce, s["cyl"], s["cyh"])
        mw_refs = functools.partial(raw_refs, s["mw"])
        gr_refs = pressure_refs
        exchange_start(ue_refs, "ue")
        exchange_start(mw_refs, "mw")
        zero_edges(ue, s["uyl"], s["uyh"])
        zero_edges(ce, s["cyl"], s["cyh"])
        zero_raw(s["mw"])
        zero_raw(s["gr"])

        for k, (dx, dy, _, dst) in enumerate(near):
            wait_recv_if(inside(-dx, -dy), dst, RECV_AT["ux"] + k)

        row15 = sub_iota((16, 128)) == 15
        before = None
        for x in range(5):
            sums, diffs = [], []
            for m in range(3):
                plane = disp[m, 16 * x : 16 * x + 16] if x < 4 else s["ux"][m]
                beyond = s["uy"][4 * m + x : 4 * m + x + 1] if x < 4 else s["uc"][m : m + 1]
                up = jnp.where(row15, jnp.broadcast_to(beyond, (16, 128)), pltpu.roll(plane, 15, 0))
                sums.append(up + plane)
                diffs.append(up - plane)
            now = (sums[0], diffs[1], sums[2])
            if before is not None:
                plain = (now[0] - before[0]) + (now[1] + before[1])
                third = now[2] + before[2]
                value = (plain - third) + shift_down(plain + third)
                at = 16 * (x - 1)
                s["stro"][at : at + 16] = 0.25 * s["mask"][at : at + 16].astype(F32) * value
            before = now
        for half in range(2):
            at = slice(32 * half, 32 * half + 32)
            for gg in sorted(range(top), key=lambda gg: -min(top - gg, gg + 1)):
                start_if(gx >= 0, s["stro"].at[at], s["sti"].at[at], SEND_AT["strain"] + 2 * gg + half, RECV_AT["strain"] + half, (gg, gx, gy))

        local("stif").wait()
        stiff = s["stif"][...]
        largest = jnp.max(jnp.max(jnp.abs(stiff), axis=1, keepdims=True), axis=0, keepdims=True)
        s["kap"][...] = jnp.broadcast_to(1.0 / largest, (8, 128))
        high, low = split(stiff / largest)
        line = lax.broadcasted_iota(I32, (64, 24), 0)
        entry = lax.broadcasted_iota(I32, (64, 24), 1)
        pick = jnp.where(((line & 3) < 3) & (3 * (line >> 3) + (line & 3) == entry), 1.0, 0.0).astype(BF16)
        r_half = (lax.broadcasted_iota(I32, (64, 64), 0) >> 2) & 1
        c_half = (lax.broadcasted_iota(I32, (64, 64), 1) >> 2) & 1
        wide = []
        for part in (high, low):
            rows = dot_nn(pick, part).astype(BF16)
            wide.append(jnp.where(r_half == c_half, dot_nt(rows, pick), 0.0).astype(BF16))
        s["kl"][...] = jnp.concatenate([wide[0], wide[0], wide[1]], 1)

        hear(0)
        call_out(1)
        exchange_wait(mw_refs, "mw")
        half = sub_iota() < 4

        def pair_of_rows(arr, x, low):
            return jnp.where(
                half,
                jnp.broadcast_to(arr[x, low : low + 1], (8, 128)),
                jnp.broadcast_to(arr[x, low + 8 : low + 9], (8, 128)),
            )

        def weights(x):
            for j in range(11):
                s["wtile"][x, 8 * j : 8 * j + 8] = pair_of_rows(s["mw"], x + 1, 6 + j)

        loop(7, weights)
        exchange_wait(ue_refs, "ue")
        close_nodes(ue, s["uyl"], s["uyh"])
        kappa = jnp.broadcast_to(largest, (8, 128))

        def initial(x, j, node, product):
            ce[x, 8 * j : 8 * j + 8] = s["bt"][x - 2, 8 * (j - 2) : 8 * (j - 2) + 8] - kappa * product

        operate(ue, (1, 6), (1, 10), initial)
        exchange_start(ce_refs, "ce")
        for turn in range(1, len(rounds)):
            hear(turn)
            if turn + 1 < len(rounds):
                call_out(turn + 1)
        exchange_wait(ce_refs, "ce")
        close_nodes(ce, s["cyl"], s["cyh"])

        for gg in range(top):
            wait_recv_if(gx >= 0, s["cr"].at[gg], RECV_AT["counts"] + gg)
        counts = s["cr"][0]
        for gg in range(1, top):
            counts = counts + s["cr"][gg]
        s["fac"][...] = (0.25 * BIOT) * s["mask"][...].astype(F32) / jnp.maximum(counts, 1.0)
        po[...] = jnp.zeros((64, 128), F32)

        for gg in range(top):
            wait_recv_if(gx >= 0, s["sr"].at[gg], RECV_AT["sums"] + gg)
        sums = s["sr"][0]
        for gg in range(1, top):
            sums = sums + s["sr"][gg]
        value = s["fac"][...] * sums
        for x in range(4):
            s["gr"][x + 3, 8:24] = value[16 * x : 16 * x + 16]
            s["gys"][0, 2 * x : 2 * x + 2] = value[16 * x : 16 * x + 2]
            s["gys"][1, 2 * x : 2 * x + 2] = value[16 * x + 14 : 16 * x + 16]
        exchange_start(gr_refs, "gr")
        exchange_wait(gr_refs, "gr")
        for side in range(2):
            for dx, planes in ((-1, (0, 1)), (0, (0, 1, 2, 3)), (1, (2, 3))):
                for x in planes:
                    to = 24 if side else 6
                    s["gr"][x + 3 - 4 * dx, to : to + 2] = s["gyr"][3 * side + dx + 1, 2 * x : 2 * x + 2]

        def tiles(k):
            for j in range(1, 13):
                s["gt"][k + 1, 8 * j : 8 * j + 8] = pair_of_rows(s["gr"], k + 1, 5 + j)

        loop(8, tiles, True)
        part = sub_iota() & 3
        signs = [jnp.where(part == m, -1.0, 1.0).astype(F32) for m in range(3)]
        rx, qe = s["rx"], s["qe"]

        def force(k):
            x = k + 1
            okay = x_ok(x)
            last = None
            for j in range(1, 13):
                at = slice(8 * j, 8 * j + 8)
                along_x = s["gt"][x, at] + signs[0] * s["gt"][x + 1, at]
                if last is not None:
                    both = last + signs[1] * along_x
                    node = shift_up(both) + signs[2] * both
                    at = slice(8 * j - 8, 8 * j)
                    rx[x, at] = (ce[x, at] + node) * (y_ok(j - 1) * okay)
                last = along_x

        loop(7, force, True)

        def first(x, j, node, product):
            qe[x, 8 * j : 8 * j + 8] = product * (y_ok(j) * x_ok(x))

        operate(rx, (1, 7), (1, 11), first)
        sums = [jnp.zeros((8, 128), F32) for _ in range(4)]
        for x in range(2, 6):
            for j in range(2, 10):
                r, q = rx[x, 8 * j : 8 * j + 8], qe[x, 8 * j : 8 * j + 8]
                for k, term in enumerate((r * r, r * q, q * q)):
                    sums[k] = sums[k] + term
        stage_nodes(qe, (2, 6), (2, 10), True)
        for x in range(2, 6):
            product = element_product(x, (2, 10))
            for c in range(8):
                j = 2 + c
                at = slice(16 * j, 16 * j + 32)
                work = product[:, 128 * c : 128 * c + 128] * jnp.concatenate([s["pf"][x, at], s["pf"][x + 1, at]], 0)
                total = work[0:8]
                for k in range(1, 8):
                    total = total + work[8 * k : 8 * k + 8]
                sums[3] = sums[3] + total * s["wtile"][x, 8 * j : 8 * j + 8]
        acc = s["dots"]
        acc[...] = jnp.concatenate([jnp.sum(term, axis=0, keepdims=True) for term in sums] + [jnp.zeros((4, 128), F32)], 0)
        total = jnp.broadcast_to(jnp.sum(acc[...], axis=1, keepdims=True), (8, 128))
        s["row"][...] = jnp.sum(jnp.where(lane_iota() == sub_iota(), total, 0.0), axis=0, keepdims=True)
        others = [(dx, dy) for dx in range(nx) for dy in range(ny) if (dx, dy) != (0, 0)]
        others.sort(key=lambda d: -(min(d[0], nx - d[0]) + 2 * min(d[1], ny - d[1])))
        for dx, dy in others:
            device = (g, lax.rem(gx + dx, nx), lax.rem(gy + dy, ny))
            start_if(gx >= 0, s["row"], s["ar"].at[dx * ny + dy], SEND_AT["ar"], RECV_AT["ar"], device)

        def to_rows(arr, out):
            for x in range(4):
                for m in range(3):
                    for h in range(2):
                        at = 64 * m + 16 * x + 8 * h
                        out[at : at + 8] = arr[x + 2, pl.ds(16 + 4 * h + m, 8, stride=8), :]

        to_rows(rx, s["rr"])
        to_rows(qe, s["qr"])
        wait_recv_if(gx >= 0, s["ar"].at[1 : nx * ny], RECV_AT["ar"])
        total = s["row"][...] + jnp.sum(s["ar"][1 : nx * ny], axis=0)
        lane = lane_iota((1, 128))
        aa, bb, cc, ee = [
            jnp.broadcast_to(jnp.sum(jnp.where(lane == k, total, 0.0), axis=1, keepdims=True), (8, 128)) for k in range(4)
        ]
        inverse = s["kap"][...]
        ee = ee + SPRING * inverse * cc
        step0 = aa / bb
        new = step0 * step0 * cc - aa
        along = bb - 2.0 * step0 * cc + step0 * step0 * ee
        ratio = new / aa
        step1 = new / (along - ratio * new / step0)
        alpha = (step0 + step1 * (1.0 + ratio)) * inverse
        gamma = step1 * step0 * inverse
        for k in range(24):
            at = 8 * k
            m, r = divmod(at, 64)
            do[at : at + 8] = disp[m, r : r + 8] + alpha * s["rr"][at : at + 8] - gamma * s["qr"][at : at + 8]

        for k, (dx, dy, src, _) in enumerate(near):
            wait_send_if(inside(dx, dy), src, SEND_AT["ux"] + k)
        for k in range(2 * top):
            wait_send_if(gx >= 0, s["stro"].at[0:32], SEND_AT["strain"] + k)
        for refs_of, name in ((ue_refs, "ue"), (mw_refs, "mw"), (ce_refs, "ce"), (gr_refs, "gr")):
            exchange_done(refs_of, name)
        wait_send_if(gx >= 0, s["ar"].at[1 : nx * ny], SEND_AT["ar"])

    pl.when(jnp.logical_not(mech))(flow)
    pl.when(mech)(mechanics)


def hand_over(p_ref, d_ref, p_out, d_out, sems):
    copies = [pltpu.make_async_copy(p_ref, p_out, sems.at[0]), pltpu.make_async_copy(d_ref, d_out, sems.at[1])]
    for copy in copies:
        copy.start()
    for copy in copies:
        copy.wait()


def local(sizes, *arrays):
    shapes = [(64, 128)] * 5 + [(512, 128), (64, 128), (3, 64, 128), (192, 128), (64, 128), (64, 128), (24, 24)]
    flat = [array.reshape(shape) for array, shape in zip(arrays, shapes)]
    scratch = [pltpu.VMEM(shape, dtype) for shape, dtype in SCRATCH.values()]
    scratch += [
        pltpu.SemaphoreType.DMA((12,)),
        pltpu.SemaphoreType.DMA((N_SEND,)),
        pltpu.SemaphoreType.DMA((N_RECV,)),
        pltpu.SemaphoreType.REGULAR((8,)),
    ]
    pressure, displacement = pl.pallas_call(
        functools.partial(kernel, sizes),
        out_shape=(pltpu.VMEM((64, 128), F32), pltpu.VMEM((192, 128), F32)),
        in_specs=[pl.BlockSpec(memory_space=pl.ANY)] * 12,
        out_specs=(pl.BlockSpec(memory_space=pltpu.VMEM),) * 2,
        scratch_shapes=scratch,
        compiler_params=pltpu.CompilerParams(collective_id=0, has_side_effects=True),
    )(*flat)
    pressure, displacement = pl.pallas_call(
        hand_over,
        out_shape=(jax.ShapeDtypeStruct((64, 128), F32), jax.ShapeDtypeStruct((192, 128), F32)),
        in_specs=[pl.BlockSpec(memory_space=pltpu.VMEM)] * 2,
        out_specs=(pl.BlockSpec(memory_space=pl.ANY),) * 2,
        scratch_shapes=[pltpu.SemaphoreType.DMA((2,))],
    )(pltpu.with_memory_space_constraint(pressure, pltpu.VMEM), pltpu.with_memory_space_constraint(displacement, pltpu.VMEM))
    return pressure.reshape(arrays[0].shape), displacement.reshape(arrays[7].shape)


def solution(mesh):
    cell = P("grp", "gx", "gy", None)
    many = P("grp", None, "gx", "gy", None)
    sizes = (mesh.shape["grp"], mesh.shape["gx"], mesh.shape["gy"])
    return jax.shard_map(
        functools.partial(local, sizes),
        mesh=mesh,
        in_specs=(cell,) * 5 + (many, cell, many, many, cell, cell, P()),
        out_specs=(cell, many),
        check_vma=False,
    )
```

```python
import functools

import jax
import jax.numpy as jnp
from jax import lax
from jax.experimental import pallas as pl
from jax.experimental.pallas import tpu as pltpu
from jax.sharding import PartitionSpec as P

F32 = jnp.float32
BF16 = jnp.bfloat16
I32 = jnp.int32
MESH = pl.DeviceIdType.MESH
NBLK = 64
LANES = 128
ROWS = 64
BIOT = 1.5
RELAX = 0.8
SPRING = 0.5
WELL = 4.0
AROUND = [(-1, -1), (-1, 1), (1, -1), (1, 1), (-1, 0), (1, 0), (0, -1), (0, 1)]

SEND = dict(ux=3, strain=6, ue=8, ce=8, mw=8, gr=8, sums=1, counts=1, halo=18, ar=1)
RECV = dict(ux=3, strain=2, ue=8, ce=8, mw=8, gr=8, sums=3, counts=3, halo=18, ar=1)


def offsets(table):
    at, out = 0, {}
    for name, count in table.items():
        out[name] = at
        at += count
    return out, at


SEND_AT, N_SEND = offsets(SEND)
RECV_AT, N_RECV = offsets(RECV)

SCRATCH = dict(
    pres=((64, 128), F32), srcs=((64, 128), F32), stor=((64, 128), F32), well=((64, 128), I32),
    blk=((64, 128), I32), bas=((512, 128), F32), host=((64, 128), I32),
    disp=((3, 64, 128), F32), body=((192, 128), F32), modl=((64, 128), F32), mask=((64, 128), I32),
    stif=((24, 24), F32),
    p1=((64, 128), F32), p2=((64, 128), F32), diag=((64, 128), F32), frc=((64, 128), F32),
    xh=((6, 16, 128), F32), yh=((6, 8, 128), F32), zh=((6, 8, 128), F32),
    ys=((6, 8, 128), F32), zs=((6, 8, 128), F32),
    sti=((64, 128), F32), ol=((128, 8192), BF16), oh=((64, 8192), BF16), ob=((64, 8192), BF16),
    wt=((64, 8, 128), F32), wr=((16, 8192), BF16), scale=((8, 64), F32),
    chg=((64, 128), F32), lo=((64, 128), F32),
    cnt=((64, 128), F32), sm=((64, 128), F32), rem=((64, 128), F32),
    ux=((3, 16, 128), F32), uy=((16, 128), F32), uc=((8, 128), F32),
    uys=((16, 128), F32), ucs=((8, 128), F32), stro=((64, 128), F32),
    ue=((8, 96, 128), F32), uyl=((8, 16, 128), F32), uyh=((8, 16, 128), F32),
    ce=((8, 96, 128), F32), cyl=((8, 16, 128), F32), cyh=((8, 16, 128), F32),
    mw=((9, 32, 128), F32), gr=((9, 32, 128), F32), wtile=((7, 88, 128), F32),
    sr=((3, 64, 128), F32), cr=((3, 64, 128), F32), fac=((64, 128), F32),
    gt=((9, 104, 128), F32), rx=((8, 96, 128), F32), qe=((8, 96, 128), F32),
    ph=((8, 192, 128), BF16), plo=((8, 192, 128), BF16), vs=((7, 704, 128), F32),
    kl=((64, 192), BF16), pf=((8, 192, 128), F32), gys=((2, 8, 128), F32), gyr=((6, 8, 128), F32), kap=((8, 128), F32), bt=((4, 64, 128), F32),
    rr=((192, 128), F32), qr=((192, 128), F32), dots=((8, 128), F32),
    ar=((64, 1, 128), F32), row=((1, 128), F32),
)


STRAIN_PARTS = (slice(0, 48), slice(48, 64))


def split(value):
    high = value.astype(BF16)
    return high, (value - high.astype(F32)).astype(BF16)


def dot_nt(a, b):
    return lax.dot_general(a, b, (((1,), (1,)), ((), ())), preferred_element_type=F32)


def dot_nn(a, b):
    return jnp.dot(a, b, preferred_element_type=F32)


def lane_iota(shape=(8, 128)):
    return lax.broadcasted_iota(I32, shape, len(shape) - 1)


def sub_iota(shape=(8, 128)):
    return lax.broadcasted_iota(I32, shape, len(shape) - 2)


def shift_down(value):
    return jnp.where(lane_iota(value.shape) == LANES - 1, 0.0, pltpu.roll(value, LANES - 1, 1))


def shift_up(value):
    return jnp.where(lane_iota(value.shape) == 0, 0.0, pltpu.roll(value, 1, 1))


def loop(count, body, unroll=1):
    def step(i, carry):
        body(i)
        return carry

    lax.fori_loop(0, count, step, 0, unroll=unroll)


def kernel(sizes, *refs):
    groups, nx, ny = sizes
    ins, (po, do), rest = refs[:12], refs[12:14], refs[14:]
    s = dict(zip(SCRATCH, rest))
    in_sems, send_sems, recv_sems, known = rest[len(SCRATCH):]
    g, gx, gy = lax.axis_index("grp"), lax.axis_index("gx"), lax.axis_index("gy")
    top = groups - 1
    mech = g == top
    names = ["pres", "srcs", "stor", "well", "blk", "bas", "host", "disp", "body", "modl", "mask", "stif"]

    def local(name):
        k = names.index(name)
        return pltpu.make_async_copy(ins[k], s[name], in_sems.at[k])

    def inside(dx, dy, dg=0):
        x, y = gx + dx, gy + dy
        ok = (x >= 0) & (x < nx) & (y >= 0) & (y < ny)
        if dg:
            ok = ok & (g + dg >= 0) & (g + dg < top)
        return ok

    def as_int(flag):
        return flag.astype(I32)

    def remote(src, dst, send, recv, device):
        return pltpu.make_async_remote_copy(
            src_ref=src, dst_ref=dst, send_sem=send_sems.at[send], recv_sem=recv_sems.at[recv],
            device_id=device, device_id_type=MESH,
        )

    def start_if(ok, *args):
        @pl.when(ok)
        def _():
            remote(*args).start()

    def wait_recv_if(ok, dst, recv):
        @pl.when(ok)
        def _():
            remote(dst, dst, 0, recv, (g, gx, gy)).wait_recv()

    def wait_send_if(ok, src, send):
        @pl.when(ok)
        def _():
            remote(src, src, send, 0, (g, gx, gy)).wait_send()

    def greet(ok, device):
        @pl.when(ok)
        def _():
            pl.semaphore_signal(pltpu.get_barrier_semaphore(), inc=1, device_id=device, device_id_type=MESH)

    HALO = [(-1, 0, 0), (1, 0, 0), (0, -1, 0), (0, 1, 0), (0, 0, -1), (0, 0, 1)]

    def halo_refs(p, k, way):
        dx, dy, dg = HALO[way]
        if dx:
            src = p.at[0:16] if dx < 0 else p.at[48:64]
            return src, s["xh"].at[2 * k + (1 if dx < 0 else 0)]
        if dy:
            return s["ys"].at[2 * k + (0 if dy < 0 else 1)], s["yh"].at[2 * k + (1 if dy < 0 else 0)]
        return s["zs"].at[2 * k + (0 if dg < 0 else 1)], s["zh"].at[2 * k + (1 if dg < 0 else 0)]

    def stage_halos(p, k):
        lane = lane_iota()
        low = jnp.zeros((8, 128), F32)
        high = jnp.zeros((8, 128), F32)
        for v in range(8):
            tile = p[8 * v : 8 * v + 8]
            low = jnp.where(lane == v, tile if v == 0 else pltpu.roll(tile, v, 1), low)
            high = jnp.where(lane == v, pltpu.roll(tile, v + 1, 1), high)
        s["zs"][2 * k] = low
        s["zs"][2 * k + 1] = high
        for x in range(4):
            s["ys"][2 * k, x : x + 1] = p[16 * x : 16 * x + 1]
            s["ys"][2 * k + 1, x : x + 1] = p[16 * x + 15 : 16 * x + 16]

    def send_halos(p, k):
        for way, (dx, dy, dg) in enumerate(HALO):
            src, dst = halo_refs(p, k, way)
            sem = 6 * k + way
            start_if(inside(dx, dy, dg), src, dst, SEND_AT["halo"] + sem, RECV_AT["halo"] + sem, (g + dg, gx + dx, gy + dy))

    def wait_halos(p, k):
        for way, (dx, dy, dg) in enumerate(HALO):
            _, dst = halo_refs(p, k, way)
            wait_recv_if(inside(-dx, -dy, -dg), dst, RECV_AT["halo"] + 6 * k + way)

    def around(p, k):
        lane = lane_iota()
        value = p[...]
        xlo, xhi = s["xh"][2 * k], s["xh"][2 * k + 1]
        total = jnp.concatenate([xlo, value[:48]], 0) + jnp.concatenate([value[16:], xhi], 0)
        ylo = jnp.concatenate([jnp.broadcast_to(s["yh"][2 * k, x : x + 1], (16, 128)) for x in range(4)], 0)
        yhi = jnp.concatenate([jnp.broadcast_to(s["yh"][2 * k + 1, x : x + 1], (16, 128)) for x in range(4)], 0)
        row = lax.rem(sub_iota((64, 128)), 16)
        total = total + jnp.where(row == 0, ylo, pltpu.roll(value, 1, 0))
        total = total + jnp.where(row == 15, yhi, pltpu.roll(value, 63, 0))
        zlo, zhi = s["zh"][2 * k], s["zh"][2 * k + 1]
        parts = []
        for v in range(8):
            tile = value[8 * v : 8 * v + 8]
            below = zlo if v == 0 else pltpu.roll(zlo, LANES - v, 1)
            above = pltpu.roll(zhi, LANES - 1 - v, 1)
            parts.append(
                jnp.where(lane == 0, below, pltpu.roll(tile, 1, 1))
                + jnp.where(lane == LANES - 1, above, pltpu.roll(tile, LANES - 1, 1))
            )
        return total + jnp.concatenate(parts, 0)

    def cols(i, width=1024):
        return pl.ds(pl.multiple_of(i * width, width), width)

    def rows8(i):
        return pl.ds(pl.multiple_of(i * 8, 8), 8)

    def flow():
        for name in ("pres", "host", "stor", "well", "srcs", "blk", "bas"):
            local(name).start()
        for name in ("xh", "yh", "zh"):
            s[name][...] = jnp.zeros(SCRATCH[name][0], F32)
        count = I32(1)
        greet(gx >= 0, (top, gx, gy))
        for dx, dy, dg in HALO:
            greet(inside(dx, dy, dg), (g + dg, gx + dx, gy + dy))
            count = count + as_int(inside(dx, dy, dg))
        local("pres").wait()
        stage_halos(s["pres"], 0)
        pl.semaphore_wait(pltpu.get_barrier_semaphore(), count)
        send_halos(s["pres"], 0)

        local("host").wait()
        iota_l = sub_iota((128, 128))
        iota_r = sub_iota((64, 128))

        def hosts(i):
            index = s["host"][rows8(i)]
            lanes, rows = index & 127, index >> 7
            left, right = [], []
            for r in range(8):
                left.append((iota_l == lanes[r : r + 1]).astype(F32).astype(BF16))
                right.append((iota_r == rows[r : r + 1]).astype(F32).astype(BF16))
            s["ol"][:, cols(i)] = jnp.concatenate(left, 1)
            s["oh"][:, cols(i)] = jnp.concatenate(right, 1)

        loop(8, hosts)
        for name in ("stor", "well", "srcs", "blk", "bas"):
            local(name).wait()
        s["diag"][...] = 6.0 + s["stor"][...] + WELL * s["well"][...].astype(F32)

        def blocks(i):
            index = s["blk"][rows8(i)]
            diag = s["diag"][rows8(i)]
            parts, highs, lows = [], [], []
            for r in range(8):
                parts.append((iota_r == index[r : r + 1]).astype(F32).astype(BF16))
                weight = s["bas"][pl.ds(i * 8 + r, 8, stride=64), :]
                s["wt"][i * 8 + r] = weight
                term = weight * weight * diag[r : r + 1]
                high = term.astype(BF16).astype(F32)
                highs.append(jnp.concatenate([high, term - high], 0).astype(BF16))
            s["ob"][:, cols(i)] = jnp.concatenate(parts, 1)
            s["wr"][:, cols(i)] = jnp.concatenate(highs, 1)

        loop(8, blocks)
        for half, part in enumerate(STRAIN_PARTS):
            wait_recv_if(gx >= 0, s["sti"].at[part], RECV_AT["strain"] + half)
            for i in range(8):
                at = slice(8 * i, 8 * i + 8)
                index = s["host"][at]
                lanes, rows = index & 127, index >> 7
                found = s["frc"][at] if half else jnp.zeros((8, 128), F32)
                for r in range(part.start, part.stop):
                    row = jnp.broadcast_to(s["sti"][r : r + 1], (8, 128))
                    found = jnp.where(rows == r, jnp.take_along_axis(row, lanes, axis=1), found)
                s["frc"][at] = s["srcs"][at] - BIOT * found if half else found

        def residual(p, k):
            return s["frc"][...] + around(p, k) - s["diag"][...] * p[...]

        wait_halos(s["pres"], 0)
        s["p1"][...] = s["pres"][...] + RELAX * residual(s["pres"], 0) / s["diag"][...]
        stage_halos(s["p1"], 1)
        send_halos(s["p1"], 1)
        norms = dot_nt(s["wr"][...], s["ob"][...])
        s["scale"][...] = 1.0 + norms[0:8] + norms[8:16]
        wait_halos(s["p1"], 1)
        s["p2"][...] = s["p1"][...] + RELAX * residual(s["p1"], 1) / s["diag"][...]
        stage_halos(s["p2"], 2)
        send_halos(s["p2"], 2)
        s["cnt"][...] = dot_nt(s["oh"][...], s["ol"][...])
        start_if(gx >= 0, s["cnt"], s["cr"].at[g], SEND_AT["counts"], RECV_AT["counts"] + g, (top, gx, gy))
        wait_halos(s["p2"], 2)
        s["rem"][...] = residual(s["p2"], 2)

        coarse = jnp.zeros((16, 64), F32)
        for i in range(8):
            rem = s["rem"][8 * i : 8 * i + 8]
            parts = []
            for r in range(8):
                term = s["wt"][8 * i + r] * rem[r : r + 1]
                high = term.astype(BF16).astype(F32)
                parts.append(jnp.concatenate([high, term - high], 0).astype(BF16))
            coarse = coarse + dot_nt(jnp.concatenate(parts, 1), s["ob"][:, 1024 * i : 1024 * i + 1024])
        fixed = (coarse[0:8] + coarse[8:16]) / s["scale"][...]
        table = jnp.concatenate([fixed, fixed], 1)
        both = jnp.zeros((128, 128), F32)
        for i in range(8):
            at = slice(8 * i, 8 * i + 8)
            blocks_of = s["blk"][at]
            parts = []
            for r in range(8):
                back = jnp.take_along_axis(table, jnp.broadcast_to(blocks_of[r : r + 1], (8, 128)), axis=1)
                parts.append(jnp.sum(s["wt"][8 * i + r] * back, axis=0, keepdims=True))
            updated = s["p2"][at] + jnp.concatenate(parts, 0)
            po[at] = updated
            change = updated - s["pres"][at]
            high = change.astype(BF16).astype(F32)
            low = change - high
            tops, lows = [], []
            for r in range(8):
                one = s["oh"][:, 1024 * i + 128 * r : 1024 * i + 128 * r + 128]
                tops.append(one * jnp.broadcast_to(high[r : r + 1], (64, 128)).astype(BF16))
                lows.append(one * jnp.broadcast_to(low[r : r + 1], (64, 128)).astype(BF16))
            scaled = jnp.concatenate([jnp.concatenate(tops, 1), jnp.concatenate(lows, 1)], 0)
            both = both + dot_nt(scaled, s["ol"][:, 1024 * i : 1024 * i + 1024])
        s["sm"][...] = both[0:64] + both[64:128]
        start_if(gx >= 0, s["sm"], s["sr"].at[g], SEND_AT["sums"], RECV_AT["sums"] + g, (top, gx, gy))
        do[...] = jnp.zeros((192, 128), F32)
        for k, p in enumerate((s["pres"], s["p1"], s["p2"])):
            for way, (dx, dy, dg) in enumerate(HALO):
                src, _ = halo_refs(p, k, way)
                wait_send_if(inside(dx, dy, dg), src, SEND_AT["halo"] + 6 * k + way)
        wait_send_if(gx >= 0, s["cnt"], SEND_AT["counts"])
        wait_send_if(gx >= 0, s["sm"], SEND_AT["sums"])

    def x_from(dx, low, high):
        first = low
        if dx == 0:
            return slice(first, first + 4), slice(first, first + 4)
        if dx < 0:
            return slice(first, first + high), slice(first + 4, first + 4 + high)
        return slice(first + 4 - low, first + 4), slice(0, low)

    def node_refs(arr, ylo, yhi, dx, dy):
        xs, xd = x_from(dx, 2, 2)
        if dy == 0:
            return arr.at[xs, 16:80], arr.at[xd, 16:80]
        if dy > 0:
            return arr.at[xs, 64:80], ylo.at[xd]
        return arr.at[xs, 16:32], yhi.at[xd]

    def raw_refs(arr, dx, dy):
        xs, xd = x_from(dx, 3, 2)
        ysrc, ydst = {0: (slice(8, 24), slice(8, 24)), 1: (slice(16, 24), slice(0, 8)), -1: (slice(8, 16), slice(24, 32))}[dy]
        return arr.at[xs, ysrc], arr.at[xd, ydst]

    def pressure_refs(dx, dy):
        if dy:
            return s["gys"].at[0 if dy < 0 else 1], s["gyr"].at[(3 if dy < 0 else 0) + dx + 1]
        src, dst = (slice(3, 5), slice(7, 9)) if dx < 0 else (slice(5, 7), slice(1, 3))
        return s["gr"].at[src, 8:24], s["gr"].at[dst, 8:24]

    def exchange_start(refs_of, name):
        for k, (dx, dy) in enumerate(AROUND):
            src, dst = refs_of(dx, dy)
            start_if(inside(dx, dy), src, dst, SEND_AT[name] + k, RECV_AT[name] + k, (g, gx + dx, gy + dy))

    def exchange_wait(refs_of, name):
        for k, (dx, dy) in enumerate(AROUND):
            _, dst = refs_of(dx, dy)
            wait_recv_if(inside(-dx, -dy), dst, RECV_AT[name] + k)

    def exchange_done(refs_of, name):
        for k, (dx, dy) in enumerate(AROUND):
            src, _ = refs_of(dx, dy)
            wait_send_if(inside(dx, dy), src, SEND_AT[name] + k)

    def close_nodes(arr, ylo, yhi):
        half = sub_iota() < 4

        def plane(x):
            for k in range(2):
                own = arr[x, 64 + 8 * k : 72 + 8 * k]
                arr[x, 8 * k : 8 * k + 8] = pltpu.roll(jnp.where(half, own, ylo[x, 8 * k : 8 * k + 8]), 4, 0)
                own = arr[x, 16 + 8 * k : 24 + 8 * k]
                arr[x, 80 + 8 * k : 88 + 8 * k] = pltpu.roll(jnp.where(half, yhi[x, 8 * k : 8 * k + 8], own), 4, 0)

        loop(8, plane)

    def zero_edges(arr, ylo, yhi):
        @pl.when(gx == 0)
        def _():
            arr[0:2] = jnp.zeros((2,) + arr.shape[1:], F32)
            ylo[0:2] = jnp.zeros((2, 16, 128), F32)
            yhi[0:2] = jnp.zeros((2, 16, 128), F32)

        @pl.when(gx == nx - 1)
        def _():
            arr[6:8] = jnp.zeros((2,) + arr.shape[1:], F32)
            ylo[6:8] = jnp.zeros((2, 16, 128), F32)
            yhi[6:8] = jnp.zeros((2, 16, 128), F32)

        @pl.when(gy == 0)
        def _():
            ylo[...] = jnp.zeros((8, 16, 128), F32)

        @pl.when(gy == ny - 1)
        def _():
            yhi[...] = jnp.zeros((8, 16, 128), F32)

    def zero_raw(arr):
        @pl.when(gx == 0)
        def _():
            arr[0:3] = jnp.zeros((3, 32, 128), F32)

        @pl.when(gx == nx - 1)
        def _():
            arr[7:9] = jnp.zeros((2, 32, 128), F32)

        @pl.when(gy == 0)
        def _():
            arr[:, 0:8] = jnp.zeros((9, 8, 128), F32)

        @pl.when(gy == ny - 1)
        def _():
            arr[:, 24:32] = jnp.zeros((9, 8, 128), F32)

    def x_ok(x):
        bad = ((x < 2) & (gx == 0)) | ((x >= 6) & (gx == nx - 1))
        return jnp.where(bad, 0.0, 1.0).astype(F32)

    def y_ok(j):
        sub = sub_iota()
        mask = jnp.where((sub & 3) < 3, 1.0, 0.0)
        if j < 2:
            mask = jnp.where(sub < 4, mask * jnp.where(gy == 0, 0.0, 1.0), mask)
        if j > 9:
            mask = jnp.where(sub >= 4, mask * jnp.where(gy == ny - 1, 0.0, 1.0), mask)
        return mask

    def stage_nodes(arr, elem_x, elem_j, keep):
        for x in range(elem_x[0], elem_x[1] + 1):
            for j in range(elem_j[0], elem_j[1] + 1):
                value = arr[x, 8 * j : 8 * j + 8]
                pair = jnp.concatenate([value, shift_down(value)], 0)
                if keep:
                    s["pf"][x, 16 * j : 16 * j + 16] = pair
                high, low = split(pair)
                s["ph"][x, 16 * j : 16 * j + 16] = high
                s["plo"][x, 16 * j : 16 * j + 16] = low

    def element_product(x, elem_j):
        columns = []
        for j in range(*elem_j):
            at = slice(16 * j, 16 * j + 32)
            first, second = s["ph"][x, at], s["ph"][x + 1, at]
            columns.append(jnp.concatenate([first, second, s["plo"][x, at], s["plo"][x + 1, at], first, second], 0))
        return dot_nn(s["kl"][...], jnp.concatenate(columns, 1))

    def operate(arr, elem_x, elem_j, use):
        (xa, xb), (ja, jb) = elem_x, elem_j
        vs = s["vs"]
        stage_nodes(arr, elem_x, elem_j, False)
        for x in range(xa, xb):
            product = element_product(x, elem_j)
            for c in range(jb - ja):
                j = ja + c
                weight = s["wtile"][x, 8 * j : 8 * j + 8]
                vs[x, 64 * j : 64 * j + 64] = product[:, 128 * c : 128 * c + 128] * jnp.concatenate([weight] * 8, 0)

        spring = SPRING * s["kap"][...]

        def nodes(k):
            x = xa + 1 + k
            for j in range(ja + 1, jb):
                total = None
                for a in range(2):
                    for b in range(2):
                        at = 64 * (j - b) + 16 * (2 * a + b)
                        part = vs[x - a, at : at + 16]
                        total = part if total is None else total + part
                node = arr[x, 8 * j : 8 * j + 8]
                use(x, j, node, total[0:8] + shift_up(total[8:16]) + spring * node)

        loop(xb - xa - 1, nodes, True)

    def mechanics():
        for name in ("disp", "mask", "modl", "stif", "body"):
            local(name).start()
        s["gyr"][...] = jnp.zeros((6, 8, 128), F32)
        greet_count = I32(top)
        for gg in range(top):
            greet(gx >= 0, (gg, gx, gy))
        for dx, dy in AROUND:
            greet(inside(dx, dy), (g, gx + dx, gy + dy))
            greet_count = greet_count + as_int(inside(dx, dy))
        local("disp").wait()
        disp = s["disp"]
        for m in range(3):
            for x in range(4):
                s["uys"][4 * m + x : 4 * m + x + 1] = disp[m, 16 * x : 16 * x + 1]
            s["ucs"][m : m + 1] = disp[m, 0:1]
        pl.semaphore_wait(pltpu.get_barrier_semaphore(), greet_count)

        near = [
            (-1, -1, s["ucs"], s["uc"]),
            (-1, 0, disp.at[:, 0:16], s["ux"]),
            (0, -1, s["uys"], s["uy"]),
        ]
        for k, (dx, dy, src, dst) in enumerate(near):
            start_if(inside(dx, dy), src, dst, SEND_AT["ux"] + k, RECV_AT["ux"] + k, (g, gx + dx, gy + dy))

        rounds, step = [], 1
        while step < nx:
            rounds.append((1, step))
            step *= 2
        step = 1
        while step < ny:
            rounds.append((2, step))
            step *= 2

        def ends(turn):
            axis, step = rounds[turn]
            coord, size = ((gx, nx), (gy, ny))[axis - 1]
            return coord - step >= 0, coord + step < size

        def call_out(turn):
            axis, step = rounds[turn]
            for ok, move in zip(ends(turn), (-step, step)):
                device = (g, gx + move, gy) if axis == 1 else (g, gx, gy + move)

                @pl.when(ok)
                def _():
                    pl.semaphore_signal(known.at[turn], inc=1, device_id=device, device_id_type=MESH)

        def hear(turn):
            back, ahead = ends(turn)
            pl.semaphore_wait(known.at[turn], as_int(back) + as_int(ahead))

        call_out(0)

        @pl.when(gx == nx - 1)
        def _():
            s["ux"][...] = jnp.zeros((3, 16, 128), F32)
            s["uc"][...] = jnp.zeros((8, 128), F32)

        @pl.when(gy == ny - 1)
        def _():
            s["uy"][...] = jnp.zeros((16, 128), F32)
            s["uc"][...] = jnp.zeros((8, 128), F32)

        ue, ce = s["ue"], s["ce"]
        local("modl").wait()
        local("mask").wait()
        local("body").wait()
        zero = jnp.zeros((64, 128), F32)
        for x in range(4):
            ue[x + 2, 16:80] = zero
            s["bt"][x] = zero
            for m in range(3):
                for h in range(2):
                    at = 16 * x + 8 * h
                    ue[x + 2, pl.ds(16 + 4 * h + m, 8, stride=8), :] = disp[m, at : at + 8]
                    at = 64 * m + at
                    s["bt"][x, pl.ds(4 * h + m, 8, stride=8), :] = s["body"][at : at + 8]
            at = 16 * x
            s["mw"][x + 3, 8:24] = s["modl"][at : at + 16] * s["mask"][at : at + 16].astype(F32)
        ue_refs = functools.partial(node_refs, ue, s["uyl"], s["uyh"])
        ce_refs = functools.partial(node_refs, ce, s["cyl"], s["cyh"])
        mw_refs = functools.partial(raw_refs, s["mw"])
        gr_refs = pressure_refs
        exchange_start(ue_refs, "ue")
        exchange_start(mw_refs, "mw")
        zero_edges(ue, s["uyl"], s["uyh"])
        zero_edges(ce, s["cyl"], s["cyh"])
        zero_raw(s["mw"])
        zero_raw(s["gr"])

        def await_near(*which):
            for k in which:
                dx, dy, _, dst = near[k]
                wait_recv_if(inside(-dx, -dy), dst, RECV_AT["ux"] + k)

        def send_strain(half):
            part = STRAIN_PARTS[half]
            for gg in sorted(range(top), key=lambda gg: -min(top - gg, gg + 1)):
                start_if(gx >= 0, s["stro"].at[part], s["sti"].at[part], SEND_AT["strain"] + 2 * gg + half, RECV_AT["strain"] + half, (gg, gx, gy))

        await_near(2)
        row15 = sub_iota((16, 128)) == 15
        before = None
        for x in range(5):
            if x == 4:
                send_strain(0)
                await_near(0, 1)
            sums, diffs = [], []
            for m in range(3):
                plane = disp[m, 16 * x : 16 * x + 16] if x < 4 else s["ux"][m]
                beyond = s["uy"][4 * m + x : 4 * m + x + 1] if x < 4 else s["uc"][m : m + 1]
                up = jnp.where(row15, jnp.broadcast_to(beyond, (16, 128)), pltpu.roll(plane, 15, 0))
                sums.append(up + plane)
                diffs.append(up - plane)
            now = (sums[0], diffs[1], sums[2])
            if before is not None:
                plain = (now[0] - before[0]) + (now[1] + before[1])
                third = now[2] + before[2]
                value = (plain - third) + shift_down(plain + third)
                at = 16 * (x - 1)
                s["stro"][at : at + 16] = 0.25 * s["mask"][at : at + 16].astype(F32) * value
            before = now
        send_strain(1)
        local("stif").wait()
        stiff = s["stif"][...]
        largest = jnp.max(jnp.max(jnp.abs(stiff), axis=1, keepdims=True), axis=0, keepdims=True)
        s["kap"][...] = jnp.broadcast_to(1.0 / largest, (8, 128))
        high, low = split(stiff / largest)
        line = lax.broadcasted_iota(I32, (64, 24), 0)
        entry = lax.broadcasted_iota(I32, (64, 24), 1)
        pick = jnp.where(((line & 3) < 3) & (3 * (line >> 3) + (line & 3) == entry), 1.0, 0.0).astype(BF16)
        r_half = (lax.broadcasted_iota(I32, (64, 64), 0) >> 2) & 1
        c_half = (lax.broadcasted_iota(I32, (64, 64), 1) >> 2) & 1
        wide = []
        for part in (high, low):
            rows = dot_nn(pick, part).astype(BF16)
            wide.append(jnp.where(r_half == c_half, dot_nt(rows, pick), 0.0).astype(BF16))
        s["kl"][...] = jnp.concatenate([wide[0], wide[0], wide[1]], 1)

        hear(0)
        call_out(1)
        exchange_wait(mw_refs, "mw")
        half = sub_iota() < 4

        def pair_of_rows(arr, x, low):
            return jnp.where(
                half,
                jnp.broadcast_to(arr[x, low : low + 1], (8, 128)),
                jnp.broadcast_to(arr[x, low + 8 : low + 9], (8, 128)),
            )

        def weights(x):
            for j in range(11):
                s["wtile"][x, 8 * j : 8 * j + 8] = pair_of_rows(s["mw"], x + 1, 6 + j)

        loop(7, weights)
        exchange_wait(ue_refs, "ue")
        close_nodes(ue, s["uyl"], s["uyh"])
        kappa = jnp.broadcast_to(largest, (8, 128))

        def initial(x, j, node, product):
            ce[x, 8 * j : 8 * j + 8] = s["bt"][x - 2, 8 * (j - 2) : 8 * (j - 2) + 8] - kappa * product

        operate(ue, (1, 6), (1, 10), initial)
        exchange_start(ce_refs, "ce")
        for turn in range(1, len(rounds)):
            hear(turn)
            if turn + 1 < len(rounds):
                call_out(turn + 1)
        exchange_wait(ce_refs, "ce")
        close_nodes(ce, s["cyl"], s["cyh"])

        for gg in range(top):
            wait_recv_if(gx >= 0, s["cr"].at[gg], RECV_AT["counts"] + gg)
        counts = s["cr"][0]
        for gg in range(1, top):
            counts = counts + s["cr"][gg]
        s["fac"][...] = (0.25 * BIOT) * s["mask"][...].astype(F32) / jnp.maximum(counts, 1.0)
        po[...] = jnp.zeros((64, 128), F32)

        for gg in range(top):
            wait_recv_if(gx >= 0, s["sr"].at[gg], RECV_AT["sums"] + gg)
        sums = s["sr"][0]
        for gg in range(1, top):
            sums = sums + s["sr"][gg]
        value = s["fac"][...] * sums
        for x in range(4):
            s["gr"][x + 3, 8:24] = value[16 * x : 16 * x + 16]
            s["gys"][0, 2 * x : 2 * x + 2] = value[16 * x : 16 * x + 2]
            s["gys"][1, 2 * x : 2 * x + 2] = value[16 * x + 14 : 16 * x + 16]
        exchange_start(gr_refs, "gr")
        exchange_wait(gr_refs, "gr")
        for side in range(2):
            for dx, planes in ((-1, (0, 1)), (0, (0, 1, 2, 3)), (1, (2, 3))):
                for x in planes:
                    to = 24 if side else 6
                    s["gr"][x + 3 - 4 * dx, to : to + 2] = s["gyr"][3 * side + dx + 1, 2 * x : 2 * x + 2]

        def tiles(k):
            for j in range(1, 13):
                s["gt"][k + 1, 8 * j : 8 * j + 8] = pair_of_rows(s["gr"], k + 1, 5 + j)

        loop(8, tiles, True)
        part = sub_iota() & 3
        signs = [jnp.where(part == m, -1.0, 1.0).astype(F32) for m in range(3)]
        rx, qe = s["rx"], s["qe"]

        def force(k):
            x = k + 1
            okay = x_ok(x)
            last = None
            for j in range(1, 13):
                at = slice(8 * j, 8 * j + 8)
                along_x = s["gt"][x, at] + signs[0] * s["gt"][x + 1, at]
                if last is not None:
                    both = last + signs[1] * along_x
                    node = shift_up(both) + signs[2] * both
                    at = slice(8 * j - 8, 8 * j)
                    rx[x, at] = (ce[x, at] + node) * (y_ok(j - 1) * okay)
                last = along_x

        loop(7, force, True)

        def first(x, j, node, product):
            qe[x, 8 * j : 8 * j + 8] = product * (y_ok(j) * x_ok(x))

        operate(rx, (1, 7), (1, 11), first)
        sums = [jnp.zeros((8, 128), F32) for _ in range(4)]
        for x in range(2, 6):
            for j in range(2, 10):
                r, q = rx[x, 8 * j : 8 * j + 8], qe[x, 8 * j : 8 * j + 8]
                for k, term in enumerate((r * r, r * q, q * q)):
                    sums[k] = sums[k] + term
        stage_nodes(qe, (2, 6), (2, 10), True)
        for x in range(2, 6):
            product = element_product(x, (2, 10))
            for c in range(8):
                j = 2 + c
                at = slice(16 * j, 16 * j + 32)
                work = product[:, 128 * c : 128 * c + 128] * jnp.concatenate([s["pf"][x, at], s["pf"][x + 1, at]], 0)
                total = work[0:8]
                for k in range(1, 8):
                    total = total + work[8 * k : 8 * k + 8]
                sums[3] = sums[3] + total * s["wtile"][x, 8 * j : 8 * j + 8]
        acc = s["dots"]
        acc[...] = jnp.concatenate([jnp.sum(term, axis=0, keepdims=True) for term in sums] + [jnp.zeros((4, 128), F32)], 0)
        total = jnp.broadcast_to(jnp.sum(acc[...], axis=1, keepdims=True), (8, 128))
        s["row"][...] = jnp.sum(jnp.where(lane_iota() == sub_iota(), total, 0.0), axis=0, keepdims=True)
        others = [(dx, dy) for dx in range(nx) for dy in range(ny) if (dx, dy) != (0, 0)]
        others.sort(key=lambda d: -(min(d[0], nx - d[0]) + 2 * min(d[1], ny - d[1])))
        for dx, dy in others:
            device = (g, lax.rem(gx + dx, nx), lax.rem(gy + dy, ny))
            start_if(gx >= 0, s["row"], s["ar"].at[dx * ny + dy], SEND_AT["ar"], RECV_AT["ar"], device)

        def to_rows(arr, out):
            for x in range(4):
                for m in range(3):
                    for h in range(2):
                        at = 64 * m + 16 * x + 8 * h
                        out[at : at + 8] = arr[x + 2, pl.ds(16 + 4 * h + m, 8, stride=8), :]

        to_rows(rx, s["rr"])
        to_rows(qe, s["qr"])
        wait_recv_if(gx >= 0, s["ar"].at[1 : nx * ny], RECV_AT["ar"])
        total = s["row"][...] + jnp.sum(s["ar"][1 : nx * ny], axis=0)
        lane = lane_iota((1, 128))
        aa, bb, cc, ee = [
            jnp.broadcast_to(jnp.sum(jnp.where(lane == k, total, 0.0), axis=1, keepdims=True), (8, 128)) for k in range(4)
        ]
        inverse = s["kap"][...]
        ee = ee + SPRING * inverse * cc
        step0 = aa / bb
        new = step0 * step0 * cc - aa
        along = bb - 2.0 * step0 * cc + step0 * step0 * ee
        ratio = new / aa
        step1 = new / (along - ratio * new / step0)
        alpha = (step0 + step1 * (1.0 + ratio)) * inverse
        gamma = step1 * step0 * inverse
        for k in range(24):
            at = 8 * k
            m, r = divmod(at, 64)
            do[at : at + 8] = disp[m, r : r + 8] + alpha * s["rr"][at : at + 8] - gamma * s["qr"][at : at + 8]

        for k, (dx, dy, src, _) in enumerate(near):
            wait_send_if(inside(dx, dy), src, SEND_AT["ux"] + k)
        for half, part in enumerate(STRAIN_PARTS):
            for gg in range(top):
                wait_send_if(gx >= 0, s["stro"].at[part], SEND_AT["strain"] + 2 * gg + half)
        for refs_of, name in ((ue_refs, "ue"), (mw_refs, "mw"), (ce_refs, "ce"), (gr_refs, "gr")):
            exchange_done(refs_of, name)
        wait_send_if(gx >= 0, s["ar"].at[1 : nx * ny], SEND_AT["ar"])

    pl.when(jnp.logical_not(mech))(flow)
    pl.when(mech)(mechanics)


def hand_over(p_ref, d_ref, p_out, d_out, sems):
    copies = [pltpu.make_async_copy(p_ref, p_out, sems.at[0]), pltpu.make_async_copy(d_ref, d_out, sems.at[1])]
    for copy in copies:
        copy.start()
    for copy in copies:
        copy.wait()


def local(sizes, *arrays):
    shapes = [(64, 128)] * 5 + [(512, 128), (64, 128), (3, 64, 128), (192, 128), (64, 128), (64, 128), (24, 24)]
    flat = [array.reshape(shape) for array, shape in zip(arrays, shapes)]
    scratch = [pltpu.VMEM(shape, dtype) for shape, dtype in SCRATCH.values()]
    scratch += [
        pltpu.SemaphoreType.DMA((12,)),
        pltpu.SemaphoreType.DMA((N_SEND,)),
        pltpu.SemaphoreType.DMA((N_RECV,)),
        pltpu.SemaphoreType.REGULAR((8,)),
    ]
    pressure, displacement = pl.pallas_call(
        functools.partial(kernel, sizes),
        out_shape=(pltpu.VMEM((64, 128), F32), pltpu.VMEM((192, 128), F32)),
        in_specs=[pl.BlockSpec(memory_space=pl.ANY)] * 12,
        out_specs=(pl.BlockSpec(memory_space=pltpu.VMEM),) * 2,
        scratch_shapes=scratch,
        compiler_params=pltpu.CompilerParams(collective_id=0, has_side_effects=True),
    )(*flat)
    pressure, displacement = pl.pallas_call(
        hand_over,
        out_shape=(jax.ShapeDtypeStruct((64, 128), F32), jax.ShapeDtypeStruct((192, 128), F32)),
        in_specs=[pl.BlockSpec(memory_space=pltpu.VMEM)] * 2,
        out_specs=(pl.BlockSpec(memory_space=pl.ANY),) * 2,
        scratch_shapes=[pltpu.SemaphoreType.DMA((2,))],
    )(pltpu.with_memory_space_constraint(pressure, pltpu.VMEM), pltpu.with_memory_space_constraint(displacement, pltpu.VMEM))
    return pressure.reshape(arrays[0].shape), displacement.reshape(arrays[7].shape)


def solution(mesh):
    cell = P("grp", "gx", "gy", None)
    many = P("grp", None, "gx", "gy", None)
    sizes = (mesh.shape["grp"], mesh.shape["gx"], mesh.shape["gy"])
    return jax.shard_map(
        functools.partial(local, sizes),
        mesh=mesh,
        in_specs=(cell,) * 5 + (many, cell, many, many, cell, cell, P()),
        out_specs=(cell, many),
        check_vma=False,
    )
```
